32 devices in a mesh: ctx: 2 (over x), tp: 4 (over y, core), dp: 4 (over z).
Axes of the slice: x: 2, y: 2, z: 4, core: 2. Of those that a mesh axis runs over, the one named last changes fastest.
Arguments:
- hidden: bfloat16 [4, 1024, 4096], P('dp', 'ctx', 'tp'), may hold values from -6 to 6
- target: bfloat16 [4, 1024, 4096], P('dp', 'ctx', 'tp'), may hold values from -24 to 24
- gain: float32 [4096], replicated, may hold values from 0.5 to 1.5
- w_query: bfloat16 [4096, 2048], P(('ctx', 'dp'), 'tp'), may hold values from -2.15625 to 2.15625
- w_key: bfloat16 [4096, 512], P(('ctx', 'dp'), 'tp'), may hold values from -0.09375 to 0.09375
- value_matrix: bfloat16 [4096, 512], P(('ctx', 'dp'), 'tp'), may hold values from -0.09375 to 0.09375
- w_out: bfloat16 [2048, 4096], P('tp', ('ctx', 'dp')), may hold values from -0.125 to 0.125
- block_order: int32 [4], replicated, may hold values from 0 to 3, each once
Outputs:
- branch: bfloat16 [4, 1024, 4096], P('dp', 'ctx', 'tp')
- loss: float32 [], replicated
The draws below stay inside these ranges and needn't reach their ends.
Inputs may be any that keep to these rules, and one draw needn't show every extreme that they name: block_order is a permutation of 0 to 3.
All inputs are finite; a program needn't handle non-finite values.
Results may differ from the reference program's by a relative error of at most 0.013.
The reference program's roundings to bfloat16 on the way (of `normed` and `attn`) count: a program that leaves them out, or rounds other values in their place, can miss the bound.
Values may be sent and summed in bfloat16 or wider, within the bound.
A program may use at most 128 MiB of HBM per device.

```python
import math
import jax
import jax.numpy as jnp
from jax import lax

MODEL_WIDTH = 4096
QUERY_HEADS = 16
KEY_VALUE_HEADS = 4
HEAD_SIZE = 128
CH = 256
SEQUENCE_LENGTH = 1024
SEQS = 4
N_CTX = 2
N_TP = 4


def key_weights(key):
    random_jitter = jax.random.normal(jax.random.fold_in(key, 11), (MODEL_WIDTH, KEY_VALUE_HEADS * HEAD_SIZE), jnp.float32)
    return jnp.clip(random_jitter, -6.0, 6.0) / MODEL_WIDTH ** 0.5


def draw_w_key(key, part):
    return key_weights(key).astype(jnp.bfloat16)


def draw_w_query(key, part):
    random_jitter = jax.random.normal(jax.random.fold_in(key, 23), (MODEL_WIDTH, QUERY_HEADS * HEAD_SIZE), jnp.float32)
    base = jnp.clip(random_jitter, -6.0, 6.0) * (3.0 / MODEL_WIDTH ** 0.5)
    return base.astype(jnp.bfloat16)


def draw_hidden(key, part):
    base = jnp.clip(jax.random.normal(jax.random.fold_in(key, 41), (SEQS, SEQUENCE_LENGTH, MODEL_WIDTH), jnp.float32), -6.0, 6.0)
    return base.astype(jnp.bfloat16)


def draw_target(key, part):
    fraction = jnp.arange(SEQUENCE_LENGTH, dtype=jnp.float32) / (SEQUENCE_LENGTH - 1)
    scale = jnp.exp(fraction * jnp.log(6.0))
    noise = jnp.clip(jax.random.normal(jax.random.fold_in(key, 67), (SEQS, SEQUENCE_LENGTH, MODEL_WIDTH), jnp.float32), -4.0, 4.0)
    return jnp.clip(noise * scale[None, :, None], -24.0, 24.0).astype(jnp.bfloat16)


def shard_levels(rng, extent, cuts, least, largest):
    def one(dim, shards_of):
        steps = jax.random.uniform(jax.random.fold_in(jax.random.fold_in(rng, 6), dim), (shards_of,), jnp.float32, least / len(cuts), largest / len(cuts))
        return jnp.repeat(jnp.exp(steps), extent[dim] // shards_of).reshape((-1,) + (1,) * (len(extent) - dim - 1))

    factor_of = one(*cuts[0])
    for cut in cuts[1:]:
        factor_of = factor_of * one(*cut)
    return factor_of


def normal_values(own_key, extent, scale, bound, shards=(), kind=jnp.bfloat16):
    values = scale * jax.random.normal(own_key, extent, jnp.float32)
    if shards:
        values = values * shard_levels(own_key, extent, shards, -0.22, 0.18)
    return jnp.clip(values, -bound, bound).astype(kind)


def setup_inputs(seed: int = 0) -> dict:
    seeds = jax.random.split(jax.random.key(seed), 9)
    hidden = draw_hidden(jax.random.fold_in(seeds[8], 71), 0)
    target = draw_target(jax.random.fold_in(seeds[8], 71), 0)
    gain = jnp.clip(1.0 + 0.1 * jax.random.normal(seeds[2], (MODEL_WIDTH,), jnp.float32), 0.5, 1.5)
    w_query = draw_w_query(jax.random.fold_in(seeds[8], 71), 0)
    w_key = draw_w_key(jax.random.fold_in(seeds[8], 71), 0)
    value_matrix = normal_values(seeds[5], (MODEL_WIDTH, KEY_VALUE_HEADS * HEAD_SIZE), MODEL_WIDTH ** -0.5, 0.09375, ((0, 8), (1, 4)))
    w_out = normal_values(seeds[6], (QUERY_HEADS * HEAD_SIZE, MODEL_WIDTH), (QUERY_HEADS * HEAD_SIZE) ** -0.5, 0.125, ((0, 4), (1, 8)))
    block_order = jax.random.permutation(seeds[7], 2 * N_CTX).astype(jnp.int32)
    return {"hidden": hidden, "target": target, "gain": gain, "w_query": w_query, "w_key": w_key, "value_matrix": value_matrix, "w_out": w_out, "block_order": block_order}


rope_base = 500000.0

def apply_rotary(values, token_places):
    half = values.shape[-1] // 2
    freqs = rope_base ** (-(jnp.arange(half, dtype=jnp.float32) * 2.0) / values.shape[-1])
    angles = token_places.astype(jnp.float32)[:, None] * freqs[None, :]
    cosine = jnp.cos(angles)[:, None, :]
    sine = jnp.sin(angles)[:, None, :]
    first = values[..., :half]
    second = values[..., half:]
    return jnp.concatenate([first * cosine - second * sine, second * cosine + first * sine], axis=-1)

def one_sequence(states, gain, w_query, w_key, value_matrix, w_out, token_places):
    query_group = QUERY_HEADS // KEY_VALUE_HEADS
    wide = states.astype(jnp.float32)
    normed = (wide * lax.rsqrt(lax.optimization_barrier(jnp.mean(wide * wide, axis=1, keepdims=True)) + 1e-05) * gain[None, :]).astype(jnp.bfloat16)
    query_rows = jnp.dot(normed, w_query, preferred_element_type=jnp.float32)
    key = jnp.dot(normed, w_key, preferred_element_type=jnp.float32)
    value_rows = jnp.dot(normed, value_matrix, preferred_element_type=jnp.float32)
    query_rows = apply_rotary(query_rows.reshape(SEQUENCE_LENGTH, QUERY_HEADS, HEAD_SIZE), token_places).astype(jnp.bfloat16).reshape(SEQUENCE_LENGTH, KEY_VALUE_HEADS, query_group, HEAD_SIZE)
    key = apply_rotary(key.reshape(SEQUENCE_LENGTH, KEY_VALUE_HEADS, HEAD_SIZE), token_places).astype(jnp.bfloat16)
    value_rows = value_rows.astype(jnp.bfloat16).reshape(SEQUENCE_LENGTH, KEY_VALUE_HEADS, HEAD_SIZE)
    scale = 1.0 / HEAD_SIZE ** 0.5
    block_rows = math.gcd(SEQUENCE_LENGTH, 1024)

    def head_split(index):
        qhead = lax.dynamic_index_in_dim(query_rows, index, 1, False)
        khead = lax.dynamic_index_in_dim(key, index, 1, False).astype(jnp.float32)
        vhead = lax.dynamic_index_in_dim(value_rows, index, 1, False).astype(jnp.float32)

        def per_block(number):
            first_row = (number * block_rows).astype(jnp.int32)
            qpart = lax.dynamic_slice_in_dim(qhead, first_row, block_rows, 0).astype(jnp.float32)
            qplaces = lax.dynamic_slice_in_dim(token_places, first_row, block_rows, 0)
            allowed = qplaces[:, None] >= token_places[None, :]
            scores = jnp.einsum('qgd,kd->gqk', qpart, khead) * scale
            scores = jnp.where(allowed[None], scores, -1e+30)
            peak = lax.optimization_barrier(jnp.max(scores, axis=-1, keepdims=True))
            weights = jnp.where(allowed[None], jnp.exp(scores - peak), 0.0)
            total = lax.optimization_barrier(jnp.sum(weights, axis=-1))
            rounded = weights.astype(jnp.bfloat16).astype(jnp.float32)
            mixed = jnp.einsum('gqk,kd->qgd', rounded, vhead)
            return (mixed / jnp.transpose(total)[:, :, None]).astype(jnp.bfloat16)
        pieces = lax.map(per_block, jnp.arange(SEQUENCE_LENGTH // block_rows, dtype=jnp.int32))
        return pieces.reshape(SEQUENCE_LENGTH, query_group, HEAD_SIZE)
    head_list = lax.map(head_split, jnp.arange(KEY_VALUE_HEADS, dtype=jnp.int32))
    attn = jnp.transpose(head_list, (1, 0, 2, 3)).reshape(SEQUENCE_LENGTH, QUERY_HEADS * HEAD_SIZE)
    width = QUERY_HEADS * HEAD_SIZE // N_TP
    summed = jnp.zeros((SEQUENCE_LENGTH, MODEL_WIDTH), jnp.float32)
    for part in range(N_TP):
        partial_term = jnp.dot(attn[:, part * width:(part + 1) * width], w_out[part * width:(part + 1) * width], preferred_element_type=jnp.float32)
        summed = summed + partial_term.astype(jnp.bfloat16).astype(jnp.float32)
    return summed.astype(jnp.bfloat16)

def reference(hidden, target, gain, w_query, w_key, value_matrix, w_out, block_order):
    rows = jnp.arange(SEQUENCE_LENGTH, dtype=jnp.int32)
    token_places = (jnp.take(block_order, rows // CH).astype(jnp.int32) * CH + rows % CH).astype(jnp.int32)
    outputs = []
    squares = jnp.zeros((), jnp.float32)
    for index in range(SEQS):
        result = one_sequence(hidden[index], gain, w_query, w_key, value_matrix, w_out, token_places)
        outputs.append(result)
        resid = hidden[index].astype(jnp.float32) + result.astype(jnp.float32) - target[index].astype(jnp.float32)
        squares = squares + jnp.sum(resid * resid)
    loss = squares / (SEQS * SEQUENCE_LENGTH * MODEL_WIDTH)
    return (jnp.stack(outputs), loss)
```

```python
import functools

import jax
import jax.numpy as jnp
from jax import lax
from jax.experimental import pallas as pl
from jax.experimental.pallas import tpu as pltpu
from jax.sharding import PartitionSpec as P

MODEL_WIDTH = 4096
QUERY_HEADS = 16
KEY_VALUE_HEADS = 4
HEAD_SIZE = 128


rope_base = 500000.0


def shifted(value, axis, by):
    peers = lax.axis_size(axis)
    return lax.ppermute(value, axis, [(i, (i + by) % peers) for i in range(peers)])


def positions(order, start, rows, half):
    index = start + lax.iota(jnp.int32, rows)
    block = index // half
    slots = lax.iota(jnp.int32, order.shape[0])
    chosen = jnp.sum(jnp.where(block[:, None] == slots[None, :], order[None, :], 0), axis=1)
    return chosen * half + index % half


def apply_rotary(values, token_places):
    half = values.shape[-1] // 2
    freqs = rope_base ** (-(jnp.arange(half, dtype=jnp.float32) * 2.0) / values.shape[-1])
    angles = token_places.astype(jnp.float32)[:, None] * freqs[None, :]
    cosine = jnp.cos(angles)[:, None, :]
    sine = jnp.sin(angles)[:, None, :]
    first = values[..., :half]
    second = values[..., half:]
    return jnp.concatenate(
        [first * cosine - second * sine, second * cosine + first * sine], axis=-1
    )


def attend(state, query_rows, qpos, piece, kpos):
    peak, total, accum = state
    rows = piece.shape[1]
    local_heads = query_rows.shape[1]
    pair = piece.reshape(2, rows, local_heads, HEAD_SIZE)
    scores = jnp.einsum(
        "qcgd,kcd->cgqk", query_rows, pair[0], preferred_element_type=jnp.float32
    ) * (1.0 / HEAD_SIZE**0.5)
    allowed = (qpos[:, None] >= kpos[None, :])[None, None]
    scores = jnp.where(allowed, scores, -1e30)
    new_peak = jnp.maximum(peak, jnp.max(scores, axis=-1))
    weights = jnp.where(allowed, jnp.exp(scores - new_peak[..., None]), 0.0)
    factor = jnp.exp(peak - new_peak)
    total = total * factor + jnp.sum(weights, axis=-1)
    update = jnp.einsum(
        "cgqk,kcd->qcgd", weights.astype(jnp.bfloat16), pair[1], preferred_element_type=jnp.float32
    )
    accum = accum * jnp.transpose(factor, (2, 0, 1))[..., None] + update
    return (new_peak, total, accum)


def on_device(hidden, target, gain, w_query, w_key, value_matrix, w_out, block_order):
    rows = hidden.shape[1]
    half = rows // 2
    local = hidden[0]
    whole = lax.all_gather(local, "tp", axis=1, tiled=True)
    wide = whole.astype(jnp.float32)
    normed = (
        wide * lax.rsqrt(jnp.mean(wide * wide, axis=1, keepdims=True) + 1e-05) * gain[None, :]
    ).astype(jnp.bfloat16)
    pieces = (
        lax.all_gather(w_query, ("ctx", "dp"), axis=0, tiled=True),
        lax.all_gather(w_key, ("ctx", "dp"), axis=0, tiled=True),
        lax.all_gather(value_matrix, ("ctx", "dp"), axis=0, tiled=True),
    )
    query_rows, key, value_rows = tuple(
        (jnp.dot(normed, piece, preferred_element_type=jnp.float32) for piece in pieces)
    )
    shard = lax.axis_index("ctx")
    qpos = positions(block_order, shard * rows, rows, half)
    local_heads = w_key.shape[1] // HEAD_SIZE
    query_group = QUERY_HEADS // KEY_VALUE_HEADS
    query_rows = (
        apply_rotary(query_rows.reshape(rows, local_heads * query_group, HEAD_SIZE), qpos)
        .astype(jnp.bfloat16)
        .reshape(rows, local_heads, query_group, HEAD_SIZE)
    )
    key = (
        apply_rotary(key.reshape(rows, local_heads, HEAD_SIZE), qpos)
        .astype(jnp.bfloat16)
        .reshape(rows, local_heads * HEAD_SIZE)
    )
    pair = jnp.stack([key, value_rows.astype(jnp.bfloat16)])
    state = (
        jnp.full((local_heads, query_group, rows), -1e30, jnp.float32),
        jnp.zeros((local_heads, query_group, rows), jnp.float32),
        jnp.zeros((rows, local_heads, query_group, HEAD_SIZE), jnp.float32),
    )
    count = lax.axis_size("ctx")
    state = attend(state, query_rows, qpos, pair, qpos)

    def turn(step, carry):
        moved, inner = carry
        moved = shifted(moved, "ctx", 1)
        source = (shard - step) % count
        return (
            moved,
            attend(
                inner, query_rows, qpos, moved, positions(block_order, source * rows, rows, half)
            ),
        )

    moved_end, state = lax.fori_loop(1, count, turn, (pair, state))
    peak, total, accum = state
    attn = (
        (accum / jnp.transpose(total, (2, 0, 1))[..., None])
        .astype(jnp.bfloat16)
        .reshape(rows, local_heads * query_group * HEAD_SIZE)
    )
    terms = jnp.dot(
        attn,
        lax.all_gather(w_out, ("ctx", "dp"), axis=1, tiled=True),
        preferred_element_type=jnp.float32,
    )
    summed = lax.psum_scatter(terms.astype(jnp.bfloat16), "tp", scatter_dimension=1, tiled=True)
    resid = local.astype(jnp.float32) + summed.astype(jnp.float32) - target[0].astype(jnp.float32)
    squares = lax.psum(jnp.sum(resid * resid), ("ctx", "tp", "dp"))
    loss = squares / (lax.axis_size("dp") * lax.axis_size("ctx") * rows * MODEL_WIDTH)
    return (summed[None], loss)


MESH = pl.DeviceIdType.MESH
F32 = jnp.float32
BF16 = jnp.bfloat16


def layer(
    nd,
    order,
    hidden,
    target,
    gain,
    freqs,
    w_query,
    w_key,
    value_matrix,
    w_out,
    out,
    loss,
    ga,
    stage,
    go,
    ostage,
    mine,
    xs,
    goal,
    normed,
    acc,
    trig,
    query,
    kv,
    attn,
    made,
    arrived,
    tile,
    sums_plane,
    sums_line,
    load_sem,
    x_send,
    a_send,
    a_recv,
    oy_send,
    oy_recv,
    o_send,
    o_recv,
    h_send,
    h_recv,
    kv_send,
    kv_recv,
    at_send,
    at_recv,
    r_send,
    r_recv,
    p_send,
    p_recv,
    l_send,
    l_recv,
):
    c, t, d = lax.axis_index("ctx"), lax.axis_index("tp"), lax.axis_index("dp")
    y, k = t // 2, t % 2
    sibling = y * 2 + (1 - k)
    across = (1 - y) * 2 + k
    rows, wide = hidden.shape
    deep, qcols = w_query.shape
    half = rows // 2
    n_heads = qcols // HEAD_SIZE
    tp = 4
    plane = 2 * tp
    owner = c == k
    up, down = d < nd - 1, d > 0

    def load(i, src, dst):
        return pltpu.make_async_copy(src, dst, load_sem.at[i])

    def weight_loads(dst):
        return (
            load(0, w_query, dst.at[:, pl.ds(0, qcols)]),
            load(1, w_key, dst.at[:, pl.ds(qcols, HEAD_SIZE)]),
            load(2, value_matrix, dst.at[:, pl.ds(qcols + HEAD_SIZE, HEAD_SIZE)]),
        )

    hc = w_out.shape[1] // 2
    own_loads = weight_loads(ga.at[k * nd + d])
    stage_loads = weight_loads(stage)
    mine_load = load(3, hidden, mine)
    keep_load = load(4, w_out.at[:, pl.ds(pl.multiple_of(y * hc, hc), hc)], go.at[d, k, y])
    give_load = load(5, w_out.at[:, pl.ds(pl.multiple_of((1 - y) * hc, hc), hc)], ostage)
    local_load = load(6, hidden, xs.at[t])
    goal_load = load(7, target, goal)

    @pl.when(owner)
    def _():
        for copy in own_loads:
            copy.start()

    @pl.when(jnp.logical_not(owner))
    def _():
        for copy in stage_loads:
            copy.start()

    mine_load.start()
    give_load.start()
    keep_load.start()

    @pl.when(owner)
    def _():
        local_load.start()

    goal_load.start()

    barrier = pltpu.get_barrier_semaphore()
    seat = c * tp + t
    for s in range(1, plane):
        p = (seat + s) % plane
        pl.semaphore_signal(
            barrier, inc=1, device_id={"ctx": p // tp, "tp": p % tp}, device_id_type=MESH
        )
    for s in range(1, nd):
        pl.semaphore_signal(barrier, inc=1, device_id={"dp": (d + s) % nd}, device_id_type=MESH)
    pl.semaphore_wait(barrier, plane - 1 + nd - 1)

    def remote(src, dst, ssem, rsem, where):
        return pltpu.make_async_remote_copy(
            src_ref=src, dst_ref=dst, send_sem=ssem, recv_sem=rsem,
            device_id=where, device_id_type=MESH,
        )

    UP, DOWN, SIB = 0, 1, 2

    def target_of(way):
        return {
            UP: {"dp": jnp.minimum(d + 1, nd - 1)},
            DOWN: {"dp": jnp.maximum(d - 1, 0)},
            SIB: {"tp": sibling},
        }[way]

    def a_copy(i, way, lane=k):
        ref = ga.at[lane * nd + i]
        return remote(ref, ref, a_send.at[way, i], a_recv.at[lane * nd + i], target_of(way))

    def o_copy(i, way, lane=k):
        ref = go.at[i, lane]
        return remote(ref, ref, o_send.at[way, i], o_recv.at[lane * nd + i], target_of(way))

    def spread(copy, i, ways):
        copy_up = lambda: copy(i, UP).start()
        copy_down = lambda: copy(i, DOWN).start()
        if UP in ways:
            pl.when(up)(copy_up)
        if DOWN in ways:
            pl.when(down)(copy_down)
        copy(i, SIB).start()

    def relay(copy, s):
        @pl.when(d >= s)
        def _():
            copy(d - s, UP).wait_recv()
            spread(copy, d - s, (UP,))

        @pl.when(d + s < nd)
        def _():
            copy(d + s, DOWN).wait_recv()
            spread(copy, d + s, (DOWN,))

    x_slot = ga.at[c * nd + d]
    x_copy = remote(
        stage, x_slot, x_send.at[0], a_recv.at[c * nd + d], {"ctx": k, "tp": y * 2 + c}
    )

    @pl.when(owner)
    def _():
        for copy in own_loads:
            copy.wait()
        spread(a_copy, d, (UP, DOWN))

    @pl.when(jnp.logical_not(owner))
    def _():
        for copy in stage_loads:
            copy.wait()
        x_copy.start()

    mine_load.wait()
    h_y = remote(mine, xs.at[t], h_send.at[0], h_recv.at[t], {"tp": (1 - y) * 2 + c})
    h_x = remote(mine, xs.at[t], h_send.at[1], h_recv.at[t], {"ctx": 1 - c, "tp": y * 2 + c})
    h_sib = remote(mine, xs.at[t], h_send.at[2], h_recv.at[t], {"tp": sibling})
    h_y.start()
    h_x.start()

    @pl.when(jnp.logical_not(owner))
    def _():
        h_sib.start()

    give_load.wait()
    oy_copy = remote(ostage, go.at[d, k, y], oy_send.at[0], oy_recv.at[0], {"tp": across})
    oy_copy.start()

    def positions_of(shard, index):
        low = order[2 * shard] * half
        high = order[2 * shard + 1] * half
        return jnp.where(index < half, low + index, high + index - half)

    place = positions_of(k, lax.broadcasted_iota(jnp.int32, (rows, HEAD_SIZE), 0)).astype(F32)
    angle = place * freqs[...]
    lane_of = lax.broadcasted_iota(jnp.int32, (rows, HEAD_SIZE), 1)
    trig[0] = jnp.cos(angle)
    sine = jnp.sin(angle)
    trig[1] = jnp.where(lane_of < HEAD_SIZE // 2, -sine, sine)

    @pl.when(jnp.logical_not(owner))
    def _():
        a_copy(d, UP).wait_recv()
        spread(a_copy, d, (UP, DOWN))

    for s in range(1, min(2, nd - 1)):
        relay(a_copy, s)

    def h_wait(slot):
        remote(mine, xs.at[slot], h_send.at[0], h_recv.at[slot], {"tp": across}).wait_recv()

    far = (1 - y) * 2
    h_relay_x = remote(
        xs.at[far + 1], xs.at[far + 1], h_send.at[3], h_recv.at[far + 1], {"ctx": 1 - c}
    )
    h_relay_y = remote(
        xs.at[y * 2], xs.at[y * 2], h_send.at[3], h_recv.at[y * 2], {"tp": across}
    )

    @pl.when(owner)
    def _():
        h_wait(far + 1)
        h_relay_x.start()

    @pl.when(jnp.logical_not(owner))
    def _():
        h_wait(y * 2)
        h_relay_y.start()

    for s in range(2, nd - 1):
        relay(a_copy, s)

    keep_load.wait()
    remote(
        ostage, go.at[d, k, 1 - y], oy_send.at[0], oy_recv.at[0], {"tp": across}
    ).wait_recv()
    spread(o_copy, d, (UP, DOWN))

    @pl.when(owner)
    def _():
        local_load.wait()
        h_wait(sibling)
        h_wait(far)

    @pl.when(jnp.logical_not(owner))
    def _():
        h_wait(y * 2 + 1)
        h_wait(far)
        h_wait(far + 1)

    chunk = min(64, rows)
    per = wide // deep

    def norm_rows(i, carry):
        r = pl.multiple_of(i * chunk, chunk)
        total = jnp.zeros((chunk, 1), F32)
        for j in range(tp):
            v = xs[j, pl.ds(r, chunk), :].astype(F32)
            total = total + jnp.sum(v * v, axis=1, keepdims=True)
        scale = lax.rsqrt(total * (1.0 / (tp * wide)) + 1e-05)
        for j in range(tp):
            for m in range(per):
                v = xs[j, pl.ds(r, chunk), m * deep : (m + 1) * deep].astype(F32)
                g = gain[:, j * wide + m * deep : j * wide + (m + 1) * deep]
                normed[j * per + m, pl.ds(r, chunk), :] = (v * scale * g).astype(BF16)
        return carry

    lax.fori_loop(0, rows // chunk, norm_rows, 0)
    acc[...] = jnp.zeros_like(acc)

    def nearest(i):
        return jnp.where(d < nd // 2, i, nd - 1 - i)

    def project(i):
        b = k * nd + i
        acc[...] += jnp.dot(normed[b], ga[b], preferred_element_type=F32)
        a_copy(i, SIB, 1 - k).wait_recv()
        b = (1 - k) * nd + i
        acc[...] += jnp.dot(normed[b], ga[b], preferred_element_type=F32)

    def project_step(i, carry):
        @pl.when(i == nd - 1)
        def _():
            relay(a_copy, nd - 1)

        project(nearest(i))
        return carry

    lax.fori_loop(0, nd, project_step, 0)

    def rotated(v):
        return (v * trig[0] + pltpu.roll(v, HEAD_SIZE // 2, 1) * trig[1]).astype(BF16)

    kv[k, :, 0:HEAD_SIZE] = rotated(acc[:, qcols : qcols + HEAD_SIZE])
    kv[k, :, HEAD_SIZE:] = acc[:, qcols + HEAD_SIZE :].astype(BF16)
    kv_copy = remote(kv.at[k], kv.at[k], kv_send.at[0], kv_recv.at[0], {"tp": sibling})
    kv_copy.start()
    for h in range(n_heads):
        part = slice(h * HEAD_SIZE, (h + 1) * HEAD_SIZE)
        query[h] = rotated(acc[:, part])
    for s in range(1, min(2, nd - 1)):
        relay(o_copy, s)

    remote(kv.at[1 - k], kv.at[1 - k], kv_send.at[0], kv_recv.at[0], {"tp": sibling}).wait_recv()
    qrows = min(256, rows)
    dims = (((1,), (1,)), ((), ()))
    group = y * 2 + c
    spots = ({"ctx": 1 - c}, {"tp": across}, {"ctx": 1 - c, "tp": across})

    def at_copy(h, way):
        ref = attn.at[group * n_heads + h]
        return remote(
            ref, ref, at_send.at[way, h], at_recv.at[group * n_heads + h], spots[way]
        )

    def attend_head(h, carry):
        def attend_block(i, inner):
            r = pl.multiple_of(i * qrows, qrows)
            q = query[h, pl.ds(r, qrows), :]
            qpos = positions_of(k, r + lax.broadcasted_iota(jnp.int32, (qrows, rows), 0))
            scores = []
            for n in range(2):
                kpos = positions_of(n, lax.broadcasted_iota(jnp.int32, (qrows, rows), 1))
                sc = lax.dot_general(
                    q, kv[n, :, 0:HEAD_SIZE], dims, preferred_element_type=F32
                ) * (1.0 / HEAD_SIZE**0.5)
                scores.append(jnp.where(qpos >= kpos, sc, -1e30))
            peak = jnp.maximum(
                jnp.max(scores[0], axis=1, keepdims=True),
                jnp.max(scores[1], axis=1, keepdims=True),
            )
            total = jnp.zeros((qrows, 1), F32)
            value = jnp.zeros((qrows, HEAD_SIZE), F32)
            for n in range(2):
                p = jnp.exp(scores[n] - peak)
                total = total + jnp.sum(p, axis=1, keepdims=True)
                value = value + jnp.dot(
                    p.astype(BF16), kv[n, :, HEAD_SIZE:], preferred_element_type=F32
                )
            attn[group * n_heads + h, pl.ds(r, qrows), :] = (value / total).astype(BF16)
            return inner

        lax.fori_loop(0, rows // qrows, attend_block, 0)
        for way in (2, 0, 1):
            at_copy(h, way).start()
        return carry

    lax.fori_loop(0, n_heads, attend_head, 0)

    for s in range(2, nd - 1):
        relay(o_copy, s)

    def at_wait(i, carry):
        g = (group + 1 + i // n_heads) % tp
        ref = attn.at[g * n_heads + i % n_heads]
        remote(
            ref, ref, at_send.at[0, 0], at_recv.at[g * n_heads + i % n_heads], spots[0]
        ).wait_recv()
        return carry

    lax.fori_loop(0, (tp - 1) * n_heads, at_wait, 0)

    js = nd // 2
    orow = min(256, rows)

    def made_copy(i):
        slot = (i % js) * 2 + y
        where = {"ctx": k, "tp": c * 2 + i // js}
        return remote(made.at[i], arrived.at[slot], r_send.at[i], r_recv.at[slot], where)

    def stays(i):
        return (k == c) & (y == c) & (i // js == k)

    def out_step(n, carry):
        @pl.when(n == nd - 1)
        def _():
            relay(o_copy, nd - 1)

        i = nearest(n)
        o_copy(i, SIB, 1 - k).wait_recv()

        def out_rows(m, inner):
            rr = pl.ds(pl.multiple_of(m * orow, orow), orow)
            total = jnp.zeros((orow, hc), F32)
            for g in range(tp):
                full = jnp.concatenate(
                    [attn[g * n_heads + h, rr, :] for h in range(n_heads)], axis=1
                )
                term = jnp.dot(full, go[i, g % 2, g // 2], preferred_element_type=F32)
                total = total + term.astype(BF16).astype(F32)
            made[i, rr, :] = total.astype(BF16)
            return inner

        lax.fori_loop(0, rows // orow, out_rows, 0)

        @pl.when(jnp.logical_not(stays(i)))
        def _():
            made_copy(i).start()

        @pl.when(stays(i))
        def _():
            arrived[(i % js) * 2 + y] = made[i]

        return carry

    lax.fori_loop(0, nd, out_step, 0)
    goal_load.wait()
    tile[...] = jnp.zeros_like(tile)

    def finish_block(n, carry):
        j = jnp.where(d < nd // 2, n // 2, js - 1 - n // 2)
        side = n % 2
        slot = j * 2 + side

        @pl.when(jnp.logical_not((y == c) & (side == y) & (c == k)))
        def _():
            remote(
                made.at[0], arrived.at[slot], r_send.at[0], r_recv.at[slot], {"tp": sibling}
            ).wait_recv()

        place = pl.ds(pl.multiple_of(slot * hc, hc), hc)

        def finish(i, inner):
            rr = pl.ds(pl.multiple_of(i * chunk, chunk), chunk)
            result = arrived[slot, rr, :]
            out[rr, place] = result
            resid = mine[rr, place].astype(F32) + result.astype(F32)
            resid = resid - goal[rr, place].astype(F32)
            sq = jnp.sum((resid * resid).reshape(chunk // 8, 8, hc), axis=0)
            part = sq[:, 0:128]
            for m in range(1, hc // 128):
                part = part + sq[:, m * 128 : (m + 1) * 128]
            tile[...] += part
            return inner

        lax.fori_loop(0, rows // chunk, finish, 0)
        return carry

    lax.fori_loop(0, 2 * js, finish_block, 0)

    def p_copy(s, slot):
        p = (seat + s) % plane
        return remote(
            sums_plane.at[slot], sums_plane.at[slot], p_send.at[s], p_recv.at[slot],
            {"ctx": p // tp, "tp": p % tp},
        )

    sums_plane[seat] = tile[...]
    for s in range(1, plane):
        p_copy(s, seat).start()
    for s in range(1, plane):
        p_copy(s, (seat + s) % plane).wait_recv()
    whole = sums_plane[0]
    for b in range(1, plane):
        whole = whole + sums_plane[b]
    sums_line[d] = whole

    def l_copy(s, slot):
        return remote(
            sums_line.at[slot], sums_line.at[slot], l_send.at[s], l_recv.at[slot],
            {"dp": (d + s) % nd},
        )

    for s in range(1, nd):
        l_copy(s, d).start()
    for s in range(1, nd):
        l_copy(s, (d + s) % nd).wait_recv()
    whole = sums_line[0]
    for b in range(1, nd):
        whole = whole + sums_line[b]
    count = plane * nd * rows * wide
    loss[0, 0] = jnp.sum(whole) / count

    @pl.when(jnp.logical_not(owner))
    def _():
        x_copy.wait_send()
        h_sib.wait_send()

    h_y.wait_send()
    h_x.wait_send()
    h_relay_x.wait_send()
    oy_copy.wait_send()
    kv_copy.wait_send()

    def drain_heads(h, carry):
        for way in range(3):
            at_copy(h, way).wait_send()
        return carry

    lax.fori_loop(0, n_heads, drain_heads, 0)

    def drain_line(i, carry):
        a_copy(i, SIB).wait_send()
        o_copy(i, SIB).wait_send()

        @pl.when(up & (i <= d))
        def _():
            a_copy(i, UP).wait_send()
            o_copy(i, UP).wait_send()

        @pl.when(down & (i >= d))
        def _():
            a_copy(i, DOWN).wait_send()
            o_copy(i, DOWN).wait_send()

        @pl.when(jnp.logical_not(stays(i)))
        def _():
            made_copy(i).wait_send()

        return carry

    lax.fori_loop(0, nd, drain_line, 0)
    for s in range(1, plane):
        p_copy(s, seat).wait_send()
    for s in range(1, nd):
        l_copy(s, d).wait_send()


def fused(nd, hidden, target, gain, w_query, w_key, value_matrix, w_out, block_order):
    rows, wide = hidden.shape[1:]
    nb = 2 * nd
    tp = 4
    plane = 2 * tp
    deep, qcols = w_query.shape
    all_cols = qcols + w_key.shape[1] + value_matrix.shape[1]
    orows, ocols = w_out.shape
    hc = ocols // 2
    half = HEAD_SIZE // 2
    freqs = rope_base ** (-(jnp.arange(half, dtype=F32) * 2.0) / HEAD_SIZE)
    freqs = jnp.concatenate([freqs, freqs])[None, :]
    heads = qcols // HEAD_SIZE
    js = nd // 2
    vmem = pl.BlockSpec(memory_space=pltpu.VMEM)
    anyspace = pl.BlockSpec(memory_space=pl.ANY)
    dma = pltpu.SemaphoreType.DMA
    branch, loss = pl.pallas_call(
        functools.partial(layer, nd),
        out_shape=(
            jax.ShapeDtypeStruct((rows, wide), BF16),
            jax.ShapeDtypeStruct((1, 1), F32),
        ),
        in_specs=[
            pl.BlockSpec(memory_space=pltpu.SMEM),
            anyspace,
            anyspace,
            vmem,
            vmem,
            anyspace,
            anyspace,
            anyspace,
            anyspace,
        ],
        out_specs=(vmem, pl.BlockSpec(memory_space=pltpu.SMEM)),
        scratch_shapes=[
            pltpu.VMEM((nb, deep, all_cols), BF16),
            pltpu.VMEM((deep, all_cols), BF16),
            pltpu.VMEM((nd, 2, 2, orows, hc), BF16),
            pltpu.VMEM((orows, hc), BF16),
            pltpu.VMEM((rows, wide), BF16),
            pltpu.VMEM((tp, rows, wide), BF16),
            pltpu.VMEM((rows, wide), BF16),
            pltpu.VMEM((nb, rows, deep), BF16),
            pltpu.VMEM((rows, all_cols), F32),
            pltpu.VMEM((2, rows, HEAD_SIZE), F32),
            pltpu.VMEM((heads, rows, HEAD_SIZE), BF16),
            pltpu.VMEM((2, rows, 2 * HEAD_SIZE), BF16),
            pltpu.VMEM((tp * heads, rows, HEAD_SIZE), BF16),
            pltpu.VMEM((nd, rows, hc), BF16),
            pltpu.VMEM((2 * js, rows, hc), BF16),
            pltpu.VMEM((8, 128), F32),
            pltpu.VMEM((plane, 8, 128), F32),
            pltpu.VMEM((nd, 8, 128), F32),
            dma((8,)),
            dma((1,)),
            dma((3, nd)),
            dma((nb,)),
            dma((1,)),
            dma((1,)),
            dma((3, nd)),
            dma((nb,)),
            dma((4,)),
            dma((tp,)),
            dma((1,)),
            dma((1,)),
            dma((3, heads)),
            dma((tp * heads,)),
            dma((nd,)),
            dma((2 * js,)),
            dma((plane,)),
            dma((plane,)),
            dma((nd,)),
            dma((nd,)),
        ],
        compiler_params=pltpu.CompilerParams(
            collective_id=1, has_side_effects=True, vmem_limit_bytes=60 * 1024 * 1024
        ),
    )(
        block_order,
        hidden[0],
        target[0],
        gain[None, :],
        freqs,
        w_query,
        w_key,
        value_matrix,
        w_out,
    )
    return (branch[None], loss.reshape(()))


def solution(mesh):
    in_specs = (
        P("dp", "ctx", "tp"),
        P("dp", "ctx", "tp"),
        P(),
        P(("ctx", "dp"), "tp"),
        P(("ctx", "dp"), "tp"),
        P(("ctx", "dp"), "tp"),
        P("tp", ("ctx", "dp")),
        P(),
    )
    out_specs = (P("dp", "ctx", "tp"), P())
    sizes = mesh.shape
    fits = sizes["ctx"] == 2 and sizes["tp"] == 4 and sizes["dp"] % 2 == 0
    body = functools.partial(fused, sizes["dp"]) if fits else on_device
    return jax.shard_map(
        body, mesh=mesh, in_specs=in_specs, out_specs=out_specs, check_vma=False
    )
```

```python
import functools

import jax
import numpy as np
import jax.numpy as jnp
from jax import lax
from jax.experimental import pallas as pl
from jax.experimental.pallas import tpu as pltpu
from jax.sharding import PartitionSpec as P

MODEL_WIDTH = 4096
QUERY_HEADS = 16
KEY_VALUE_HEADS = 4
HEAD_SIZE = 128


rope_base = 500000.0


def shifted(value, axis, by):
    peers = lax.axis_size(axis)
    return lax.ppermute(value, axis, [(i, (i + by) % peers) for i in range(peers)])


def positions(order, start, rows, half):
    index = start + lax.iota(jnp.int32, rows)
    block = index // half
    slots = lax.iota(jnp.int32, order.shape[0])
    chosen = jnp.sum(jnp.where(block[:, None] == slots[None, :], order[None, :], 0), axis=1)
    return chosen * half + index % half


def apply_rotary(values, token_places):
    half = values.shape[-1] // 2
    freqs = rope_base ** (-(jnp.arange(half, dtype=jnp.float32) * 2.0) / values.shape[-1])
    angles = token_places.astype(jnp.float32)[:, None] * freqs[None, :]
    cosine = jnp.cos(angles)[:, None, :]
    sine = jnp.sin(angles)[:, None, :]
    first = values[..., :half]
    second = values[..., half:]
    return jnp.concatenate(
        [first * cosine - second * sine, second * cosine + first * sine], axis=-1
    )


def attend(state, query_rows, qpos, piece, kpos):
    peak, total, accum = state
    rows = piece.shape[1]
    local_heads = query_rows.shape[1]
    pair = piece.reshape(2, rows, local_heads, HEAD_SIZE)
    scores = jnp.einsum(
        "qcgd,kcd->cgqk", query_rows, pair[0], preferred_element_type=jnp.float32
    ) * (1.0 / HEAD_SIZE**0.5)
    allowed = (qpos[:, None] >= kpos[None, :])[None, None]
    scores = jnp.where(allowed, scores, -1e30)
    new_peak = jnp.maximum(peak, jnp.max(scores, axis=-1))
    weights = jnp.where(allowed, jnp.exp(scores - new_peak[..., None]), 0.0)
    factor = jnp.exp(peak - new_peak)
    total = total * factor + jnp.sum(weights, axis=-1)
    update = jnp.einsum(
        "cgqk,kcd->qcgd", weights.astype(jnp.bfloat16), pair[1], preferred_element_type=jnp.float32
    )
    accum = accum * jnp.transpose(factor, (2, 0, 1))[..., None] + update
    return (new_peak, total, accum)


def on_device(hidden, target, gain, w_query, w_key, value_matrix, w_out, block_order):
    rows = hidden.shape[1]
    half = rows // 2
    local = hidden[0]
    whole = lax.all_gather(local, "tp", axis=1, tiled=True)
    wide = whole.astype(jnp.float32)
    normed = (
        wide * lax.rsqrt(jnp.mean(wide * wide, axis=1, keepdims=True) + 1e-05) * gain[None, :]
    ).astype(jnp.bfloat16)
    pieces = (
        lax.all_gather(w_query, ("ctx", "dp"), axis=0, tiled=True),
        lax.all_gather(w_key, ("ctx", "dp"), axis=0, tiled=True),
        lax.all_gather(value_matrix, ("ctx", "dp"), axis=0, tiled=True),
    )
    query_rows, key, value_rows = tuple(
        (jnp.dot(normed, piece, preferred_element_type=jnp.float32) for piece in pieces)
    )
    shard = lax.axis_index("ctx")
    qpos = positions(block_order, shard * rows, rows, half)
    local_heads = w_key.shape[1] // HEAD_SIZE
    query_group = QUERY_HEADS // KEY_VALUE_HEADS
    query_rows = (
        apply_rotary(query_rows.reshape(rows, local_heads * query_group, HEAD_SIZE), qpos)
        .astype(jnp.bfloat16)
        .reshape(rows, local_heads, query_group, HEAD_SIZE)
    )
    key = (
        apply_rotary(key.reshape(rows, local_heads, HEAD_SIZE), qpos)
        .astype(jnp.bfloat16)
        .reshape(rows, local_heads * HEAD_SIZE)
    )
    pair = jnp.stack([key, value_rows.astype(jnp.bfloat16)])
    state = (
        jnp.full((local_heads, query_group, rows), -1e30, jnp.float32),
        jnp.zeros((local_heads, query_group, rows), jnp.float32),
        jnp.zeros((rows, local_heads, query_group, HEAD_SIZE), jnp.float32),
    )
    count = lax.axis_size("ctx")
    state = attend(state, query_rows, qpos, pair, qpos)

    def turn(step, carry):
        moved, inner = carry
        moved = shifted(moved, "ctx", 1)
        source = (shard - step) % count
        return (
            moved,
            attend(
                inner, query_rows, qpos, moved, positions(block_order, source * rows, rows, half)
            ),
        )

    moved_end, state = lax.fori_loop(1, count, turn, (pair, state))
    peak, total, accum = state
    attn = (
        (accum / jnp.transpose(total, (2, 0, 1))[..., None])
        .astype(jnp.bfloat16)
        .reshape(rows, local_heads * query_group * HEAD_SIZE)
    )
    terms = jnp.dot(
        attn,
        lax.all_gather(w_out, ("ctx", "dp"), axis=1, tiled=True),
        preferred_element_type=jnp.float32,
    )
    summed = lax.psum_scatter(terms.astype(jnp.bfloat16), "tp", scatter_dimension=1, tiled=True)
    resid = local.astype(jnp.float32) + summed.astype(jnp.float32) - target[0].astype(jnp.float32)
    squares = lax.psum(jnp.sum(resid * resid), ("ctx", "tp", "dp"))
    loss = squares / (lax.axis_size("dp") * lax.axis_size("ctx") * rows * MODEL_WIDTH)
    return (summed[None], loss)


MESH = pl.DeviceIdType.MESH
F32 = jnp.float32
BF16 = jnp.bfloat16


def layer(
    nd,
    order,
    hidden,
    target,
    gain,
    freqs,
    w_query,
    w_key,
    value_matrix,
    w_out,
    out,
    loss,
    ga,
    stage,
    go,
    ostage,
    mine,
    xs,
    goal,
    normed,
    acc,
    trig,
    query,
    kv,
    attn,
    made,
    arrived,
    tile,
    sums,
    gains,
    turns,
    load_sem,
    out_sem,
    x_send,
    a_send,
    a_recv,
    oy_send,
    oy_recv,
    o_send,
    o_recv,
    h_send,
    h_recv,
    kv_send,
    kv_recv,
    at_send,
    at_recv,
    r_send,
    r_recv,
    l_send,
    l_recv,
):
    c, t, d = lax.axis_index("ctx"), lax.axis_index("tp"), lax.axis_index("dp")
    y, k = t // 2, t % 2
    sibling = y * 2 + (1 - k)
    across = (1 - y) * 2 + k
    rows, wide = hidden.shape
    deep, qcols = w_query.shape
    half = rows // 2
    n_heads = qcols // HEAD_SIZE
    tp = 4
    plane = 2 * tp
    owner = c == k
    up, down = d < nd - 1, d > 0

    def load(i, src, dst):
        return pltpu.make_async_copy(src, dst, load_sem.at[i])

    hd = deep // 2

    def weight_loads(dst):
        copies = []
        for h in range(2):
            part, first = dst.at[h], pl.ds(h * hd, hd)
            for src, start in (
                (w_query, 0),
                (w_key, qcols),
                (value_matrix, qcols + HEAD_SIZE),
            ):
                there = part.at[:, pl.ds(start, src.shape[1])]
                copies.append(load(len(copies), src.at[first], there))
        return copies

    hc = w_out.shape[1] // 2
    own_loads = weight_loads(ga.at[c * nd + d])
    stage_loads = weight_loads(stage)
    mine_load = load(6, hidden, mine)
    keep_load = load(7, w_out.at[:, pl.ds(pl.multiple_of(y * hc, hc), hc)], go.at[d, k, y])
    give_load = load(8, w_out.at[:, pl.ds(pl.multiple_of((1 - y) * hc, hc), hc)], ostage)
    local_load = load(9, hidden, xs.at[t])
    goal_load = load(10, target, goal)
    gain_load = load(11, gain, gains)
    turn_load = load(12, freqs, turns)

    @pl.when(owner)
    def _():
        for copy in own_loads:
            copy.start()

    @pl.when(jnp.logical_not(owner))
    def _():
        for copy in stage_loads:
            copy.start()

    mine_load.start()
    turn_load.start()
    give_load.start()
    keep_load.start()

    @pl.when(owner)
    def _():
        local_load.start()

    goal_load.start()
    gain_load.start()

    barrier = pltpu.get_barrier_semaphore()
    seat = c * tp + t
    for s in range(1, plane):
        p = (seat + s) % plane
        pl.semaphore_signal(
            barrier, inc=1, device_id={"ctx": p // tp, "tp": p % tp}, device_id_type=MESH
        )
    for there, step in ((up, 1), (down, -1)):

        @pl.when(there)
        def _():
            pl.semaphore_signal(barrier, inc=1, device_id={"dp": d + step}, device_id_type=MESH)

    pl.semaphore_wait(barrier, plane - 1 + up.astype(jnp.int32) + down.astype(jnp.int32))

    def remote(src, dst, ssem, rsem, where):
        return pltpu.make_async_remote_copy(
            src_ref=src, dst_ref=dst, send_sem=ssem, recv_sem=rsem,
            device_id=where, device_id_type=MESH,
        )

    UP, DOWN, SIB = 0, 1, 2

    def target_of(way):
        return {
            UP: {"dp": jnp.minimum(d + 1, nd - 1)},
            DOWN: {"dp": jnp.maximum(d - 1, 0)},
            SIB: {"tp": sibling},
        }[way]

    def a_copy(line, i, way, piece=k):
        b = line * nd + i
        ref = ga.at[b, piece]
        return remote(ref, ref, a_send.at[way, b], a_recv.at[b, piece], target_of(way))

    def o_copy(i, way, lane=k):
        ref = go.at[i, lane]
        return remote(ref, ref, o_send.at[way, i], o_recv.at[lane * nd + i], target_of(way))

    def spread(copy, i, ways):
        copy_up = lambda: copy(i, UP).start()
        copy_down = lambda: copy(i, DOWN).start()
        if UP in ways:
            pl.when(up)(copy_up)
        if DOWN in ways:
            pl.when(down)(copy_down)
        if SIB in ways:
            copy(i, SIB).start()

    def relay(copy, s):
        @pl.when(d >= s)
        def _():
            copy(d - s, UP).wait_recv()
            spread(copy, d - s, (UP, SIB))

        @pl.when(d + s < nd)
        def _():
            copy(d + s, DOWN).wait_recv()
            spread(copy, d + s, (DOWN, SIB))

    near_copy = functools.partial(a_copy, c)
    far_copy = functools.partial(a_copy, 1 - c)
    b_own = c * nd + d
    half_copy = remote(
        ga.at[b_own, 1 - k],
        ga.at[b_own, 1 - k],
        x_send.at[2],
        a_recv.at[b_own, 1 - k],
        {"tp": sibling},
    )
    x_copies = [
        remote(
            stage.at[h],
            ga.at[b_own, h],
            x_send.at[h],
            a_recv.at[b_own, h],
            {"ctx": 1 - c, "tp": y * 2 + h},
        )
        for h in range(2)
    ]

    @pl.when(owner)
    def _():
        for copy in own_loads:
            copy.wait()
        half_copy.start()
        spread(near_copy, d, (UP, DOWN, SIB))

    @pl.when(jnp.logical_not(owner))
    def _():
        for copy in stage_loads:
            copy.wait()
        for copy in x_copies:
            copy.start()

    mine_load.wait()
    h_y = remote(mine, xs.at[t], h_send.at[0], h_recv.at[t], {"tp": (1 - y) * 2 + c})
    h_x = remote(mine, xs.at[t], h_send.at[1], h_recv.at[t], {"ctx": 1 - c, "tp": y * 2 + c})
    h_sib = remote(mine, xs.at[t], h_send.at[2], h_recv.at[t], {"tp": sibling})
    h_y.start()

    @pl.when(jnp.logical_not(owner) & (k == 0))
    def _():
        h_x.start()

    @pl.when(jnp.logical_not(owner))
    def _():
        h_sib.start()
        near_copy(d, UP).wait_recv()
        spread(near_copy, d, (UP, DOWN))

    give_load.wait()
    oy_copy = remote(ostage, go.at[d, k, y], oy_send.at[0], oy_recv.at[0], {"tp": across})
    oy_copy.start()

    def positions_of(shard, index):
        low = order[2 * shard] * half
        high = order[2 * shard + 1] * half
        return jnp.where(index < half, low + index, high + index - half)

    turn_load.wait()
    place = positions_of(k, lax.broadcasted_iota(jnp.int32, (rows, HEAD_SIZE), 0)).astype(F32)
    angle = place * turns[...]
    lane_of = lax.broadcasted_iota(jnp.int32, (rows, HEAD_SIZE), 1)
    trig[0] = jnp.cos(angle)
    sine = jnp.sin(angle)
    trig[1] = jnp.where(lane_of < HEAD_SIZE // 2, -sine, sine)

    for s in range(1, min(2, nd - 1)):
        relay(near_copy, s)

    @pl.when(owner & (k == 0))
    def _():
        h_x.start()

    far_copy(d, UP).wait_recv()
    spread(far_copy, d, (UP, DOWN, SIB))

    for s in range(2, nd - 1):
        relay(near_copy, s)

    @pl.when(k == 1)
    def _():
        h_x.start()

    def h_wait(slot):
        remote(mine, xs.at[slot], h_send.at[0], h_recv.at[slot], {"tp": across}).wait_recv()

    far = (1 - y) * 2
    h_relay_x = remote(
        xs.at[far + 1], xs.at[far + 1], h_send.at[3], h_recv.at[far + 1], {"ctx": 1 - c}
    )
    h_relay_y = remote(
        xs.at[y * 2], xs.at[y * 2], h_send.at[3], h_recv.at[y * 2], {"tp": across}
    )

    @pl.when(owner)
    def _():
        h_wait(far + 1)
        h_relay_x.start()

    @pl.when(jnp.logical_not(owner))
    def _():
        h_wait(y * 2)
        h_relay_y.start()

    for s in range(1, min(2, nd - 1)):
        relay(far_copy, s)

    for s in range(2, nd - 1):
        relay(far_copy, s)

    keep_load.wait()
    remote(
        ostage, go.at[d, k, 1 - y], oy_send.at[0], oy_recv.at[0], {"tp": across}
    ).wait_recv()
    spread(o_copy, d, (UP, DOWN, SIB))

    @pl.when(owner)
    def _():
        local_load.wait()
        h_wait(sibling)
        h_wait(far)

    @pl.when(jnp.logical_not(owner))
    def _():
        h_wait(y * 2 + 1)
        h_wait(far)
        h_wait(far + 1)

    gain_load.wait()
    chunk = min(64, rows)
    per = wide // deep

    def norm_rows(i, carry):
        r = pl.multiple_of(i * chunk, chunk)
        total = jnp.zeros((chunk, 1), F32)
        for j in range(tp):
            v = xs[j, pl.ds(r, chunk), :].astype(F32)
            total = total + jnp.sum(v * v, axis=1, keepdims=True)
        scale = lax.rsqrt(total * (1.0 / (tp * wide)) + 1e-05)
        for j in range(tp):
            for m in range(per):
                v = xs[j, pl.ds(r, chunk), m * deep : (m + 1) * deep].astype(F32)
                g = gains[:, j * wide + m * deep : j * wide + (m + 1) * deep]
                normed[j * per + m, pl.ds(r, chunk), :] = (v * scale * g).astype(BF16)
        return carry

    lax.fori_loop(0, rows // chunk, norm_rows, 0)
    acc[...] = jnp.zeros_like(acc)

    def nearest(i):
        return jnp.where(d < nd // 2, i, nd - 1 - i)

    def project(i, line):
        b = line * nd + i

        @pl.when(jnp.logical_not(owner & (b == b_own)))
        def _():
            a_copy(line, i, SIB, 1 - k).wait_recv()

        weights = ga[b].reshape(deep, ga.shape[3])
        acc[...] += jnp.dot(normed[b], weights, preferred_element_type=F32)

    def project_step(i, carry):
        @pl.when(i == nd - 1)
        def _():
            relay(near_copy, nd - 1)

        project(nearest(i), c)

        @pl.when(i == nd - 1)
        def _():
            relay(far_copy, nd - 1)

        project(nearest(i), 1 - c)
        return carry

    lax.fori_loop(0, nd, project_step, 0)

    def rotated(v):
        return (v * trig[0] + pltpu.roll(v, HEAD_SIZE // 2, 1) * trig[1]).astype(BF16)

    kv[k, :, 0:HEAD_SIZE] = rotated(acc[:, qcols : qcols + HEAD_SIZE])
    kv[k, :, HEAD_SIZE:] = acc[:, qcols + HEAD_SIZE :].astype(BF16)
    kv_copy = remote(kv.at[k], kv.at[k], kv_send.at[0], kv_recv.at[0], {"tp": sibling})
    kv_copy.start()
    for h in range(n_heads):
        part = slice(h * HEAD_SIZE, (h + 1) * HEAD_SIZE)
        query[h] = rotated(acc[:, part])
    remote(kv.at[1 - k], kv.at[1 - k], kv_send.at[0], kv_recv.at[0], {"tp": sibling}).wait_recv()
    qrows = min(256, rows)
    dims = (((1,), (1,)), ((), ()))
    group = y * 2 + c
    spots = ({"ctx": 1 - c}, {"tp": across})
    x_group, y_group = y * 2 + 1 - c, (1 - y) * 2 + c

    def at_copy(h, way, source=group):
        b = source * n_heads + h
        ref = attn.at[b]
        sem = at_send.at[way, jnp.where(source == group, 0, n_heads) + h]
        return remote(ref, ref, sem, at_recv.at[b], spots[way])

    def attend_head(h, carry):
        def attend_block(i, inner):
            r = pl.multiple_of(i * qrows, qrows)
            q = query[h, pl.ds(r, qrows), :]
            qpos = positions_of(k, r + lax.broadcasted_iota(jnp.int32, (qrows, rows), 0))
            scores = []
            for n in range(2):
                kpos = positions_of(n, lax.broadcasted_iota(jnp.int32, (qrows, rows), 1))
                sc = lax.dot_general(
                    q, kv[n, :, 0:HEAD_SIZE], dims, preferred_element_type=F32
                ) * (1.0 / HEAD_SIZE**0.5)
                scores.append(jnp.where(qpos >= kpos, sc, -1e30))
            peak = jnp.maximum(
                jnp.max(scores[0], axis=1, keepdims=True),
                jnp.max(scores[1], axis=1, keepdims=True),
            )
            total = jnp.zeros((qrows, 1), F32)
            value = jnp.zeros((qrows, HEAD_SIZE), F32)
            for n in range(2):
                p = jnp.exp(scores[n] - peak)
                total = total + jnp.sum(p, axis=1, keepdims=True)
                value = value + jnp.dot(
                    p.astype(BF16), kv[n, :, HEAD_SIZE:], preferred_element_type=F32
                )
            attn[group * n_heads + h, pl.ds(r, qrows), :] = (value / total).astype(BF16)
            return inner

        lax.fori_loop(0, rows // qrows, attend_block, 0)
        for way in range(2):
            at_copy(h, way).start()
        return carry

    lax.fori_loop(0, n_heads, attend_head, 0)

    for s in range(1, min(2, nd - 1)):
        relay(o_copy, s)

    early = n_heads // 2

    def at_relay(h, carry):
        at_copy(h, 0, x_group).wait_recv()
        at_copy(h, 1, x_group).start()
        at_copy(early + h, 1, y_group).wait_recv()
        at_copy(early + h, 0, y_group).start()
        return carry

    lax.fori_loop(0, early, at_relay, 0)

    for s in range(2, nd - 1):
        relay(o_copy, s)


    def at_wait(h, carry):
        at_copy(early + h, 0, x_group).wait_recv()
        at_copy(h, 1, y_group).wait_recv()
        return carry

    lax.fori_loop(0, early, at_wait, 0)
    z_group = (1 - y) * 2 + 1 - c

    def far_wait(h, carry):
        at_copy(h, 1, z_group).wait_recv()
        return carry

    lax.fori_loop(0, n_heads, far_wait, 0)

    js = nd // 2
    orow = min(256, rows)

    def made_copy(i):
        slot = (i % js) * 2 + y
        where = {"ctx": k, "tp": c * 2 + i // js}
        return remote(made.at[i], arrived.at[slot], r_send.at[i], r_recv.at[slot], where)

    def stays(i):
        return (k == c) & (y == c) & (i // js == k)

    def out_step(n, carry):
        @pl.when(n == nd - 1)
        def _():
            relay(o_copy, nd - 1)

        i = nearest(n)
        o_copy(i, SIB, 1 - k).wait_recv()

        def out_rows(m, inner):
            rr = pl.ds(pl.multiple_of(m * orow, orow), orow)
            total = jnp.zeros((orow, hc), F32)
            for g in range(tp):
                full = jnp.concatenate(
                    [attn[g * n_heads + h, rr, :] for h in range(n_heads)], axis=1
                )
                term = jnp.dot(full, go[i, g % 2, g // 2], preferred_element_type=F32)
                total = total + term.astype(BF16).astype(F32)
            made[i, rr, :] = total.astype(BF16)
            return inner

        lax.fori_loop(0, rows // orow, out_rows, 0)

        @pl.when(jnp.logical_not(stays(i)))
        def _():
            made_copy(i).start()

        @pl.when(stays(i))
        def _():
            arrived[(i % js) * 2 + y] = made[i]

        return carry

    lax.fori_loop(0, nd, out_step, 0)
    goal_load.wait()
    tile[...] = jnp.zeros_like(tile)

    def out_copy(slot):
        place = pl.ds(pl.multiple_of(slot * hc, hc), hc)
        return pltpu.make_async_copy(arrived.at[slot], out.at[:, place], out_sem.at[slot])

    def finish_block(n, carry):
        j = jnp.where(d < nd // 2, n // 2, js - 1 - n // 2)
        side = n % 2
        slot = j * 2 + side

        @pl.when(jnp.logical_not((y == c) & (side == y) & (c == k)))
        def _():
            remote(
                made.at[0], arrived.at[slot], r_send.at[0], r_recv.at[slot], {"tp": sibling}
            ).wait_recv()

        out_copy(slot).start()
        place = pl.ds(pl.multiple_of(slot * hc, hc), hc)

        def finish(i, inner):
            rr = pl.ds(pl.multiple_of(i * chunk, chunk), chunk)
            result = arrived[slot, rr, :]
            resid = mine[rr, place].astype(F32) + result.astype(F32)
            resid = resid - goal[rr, place].astype(F32)
            sq = jnp.sum((resid * resid).reshape(chunk // 8, 8, hc), axis=0)
            part = sq[:, 0:128]
            for m in range(1, hc // 128):
                part = part + sq[:, m * 128 : (m + 1) * 128]
            tile[...] += part
            return inner

        lax.fori_loop(0, rows // chunk, finish, 0)
        return carry

    lax.fori_loop(0, 2 * js, finish_block, 0)

    everyone = plane * nd
    number = d * plane + seat

    def l_copy(s, slot):
        p = (number + s) % everyone
        return remote(
            sums.at[slot], sums.at[slot], l_send.at[s], l_recv.at[slot],
            {"ctx": p % plane // tp, "tp": p % tp, "dp": p // plane},
        )

    sums[number] = tile[...]

    def share(s, carry):
        l_copy(s, number).start()
        return carry

    lax.fori_loop(1, everyone, share, 0)

    def collect(s, carry):
        l_copy(s, (number + s) % everyone).wait_recv()
        return carry

    lax.fori_loop(1, everyone, collect, 0)
    whole = sums[0]
    for b in range(1, everyone):
        whole = whole + sums[b]
    count = plane * nd * rows * wide
    loss[0, 0] = jnp.sum(whole) / count

    @pl.when(owner)
    def _():
        half_copy.wait_send()

    @pl.when(jnp.logical_not(owner))
    def _():
        for copy in x_copies:
            copy.wait_send()
        h_sib.wait_send()

    for slot in range(2 * js):
        out_copy(slot).wait()
    h_y.wait_send()
    h_x.wait_send()
    h_relay_x.wait_send()
    oy_copy.wait_send()
    kv_copy.wait_send()

    def drain_heads(h, carry):
        for way in range(2):
            at_copy(h, way).wait_send()
        return carry

    lax.fori_loop(0, n_heads, drain_heads, 0)

    def drain_relays(h, carry):
        at_copy(h, 1, x_group).wait_send()
        at_copy(early + h, 0, y_group).wait_send()
        return carry

    lax.fori_loop(0, early, drain_relays, 0)

    def drain_line(i, carry):
        @pl.when(owner | (i != d))
        def _():
            near_copy(i, SIB).wait_send()

        far_copy(i, SIB).wait_send()
        o_copy(i, SIB).wait_send()
        for copy in (near_copy, far_copy, o_copy):

            @pl.when(up & (i <= d))
            def _():
                copy(i, UP).wait_send()

            @pl.when(down & (i >= d))
            def _():
                copy(i, DOWN).wait_send()

        @pl.when(jnp.logical_not(stays(i)))
        def _():
            made_copy(i).wait_send()

        return carry

    lax.fori_loop(0, nd, drain_line, 0)
    def drain_sums(s, carry):
        l_copy(s, number).wait_send()
        return carry

    lax.fori_loop(1, everyone, drain_sums, 0)


def fused(nd, hidden, target, gain, w_query, w_key, value_matrix, w_out, block_order):
    rows, wide = hidden.shape[1:]
    nb = 2 * nd
    tp = 4
    plane = 2 * tp
    deep, qcols = w_query.shape
    all_cols = qcols + w_key.shape[1] + value_matrix.shape[1]
    orows, ocols = w_out.shape
    hc = ocols // 2
    half = HEAD_SIZE // 2
    freqs = np.float64(rope_base) ** (-np.arange(half) * 2.0 / HEAD_SIZE)
    freqs = jnp.asarray(np.concatenate([freqs, freqs])[None, :].astype(np.float32))
    heads = qcols // HEAD_SIZE
    js = nd // 2
    anyspace = pl.BlockSpec(memory_space=pl.ANY)
    dma = pltpu.SemaphoreType.DMA
    branch, loss = pl.pallas_call(
        functools.partial(layer, nd),
        out_shape=(
            jax.ShapeDtypeStruct((rows, wide), BF16),
            jax.ShapeDtypeStruct((1, 1), F32),
        ),
        in_specs=[
            pl.BlockSpec(memory_space=pltpu.SMEM),
            anyspace,
            anyspace,
            anyspace,
            anyspace,
            anyspace,
            anyspace,
            anyspace,
            anyspace,
        ],
        out_specs=(anyspace, pl.BlockSpec(memory_space=pltpu.SMEM)),
        scratch_shapes=[
            pltpu.VMEM((nb, 2, deep // 2, all_cols), BF16),
            pltpu.VMEM((2, deep // 2, all_cols), BF16),
            pltpu.VMEM((nd, 2, 2, orows, hc), BF16),
            pltpu.VMEM((orows, hc), BF16),
            pltpu.VMEM((rows, wide), BF16),
            pltpu.VMEM((tp, rows, wide), BF16),
            pltpu.VMEM((rows, wide), BF16),
            pltpu.VMEM((nb, rows, deep), BF16),
            pltpu.VMEM((rows, all_cols), F32),
            pltpu.VMEM((2, rows, HEAD_SIZE), F32),
            pltpu.VMEM((heads, rows, HEAD_SIZE), BF16),
            pltpu.VMEM((2, rows, 2 * HEAD_SIZE), BF16),
            pltpu.VMEM((tp * heads, rows, HEAD_SIZE), BF16),
            pltpu.VMEM((nd, rows, hc), BF16),
            pltpu.VMEM((2 * js, rows, hc), BF16),
            pltpu.VMEM((8, 128), F32),
            pltpu.VMEM((plane * nd, 8, 128), F32),
            pltpu.VMEM((1, tp * wide), F32),
            pltpu.VMEM((1, HEAD_SIZE), F32),
            dma((13,)),
            dma((2 * js,)),
            dma((3,)),
            dma((3, nb)),
            dma((nb, 2)),
            dma((1,)),
            dma((1,)),
            dma((3, nd)),
            dma((nb,)),
            dma((4,)),
            dma((tp,)),
            dma((1,)),
            dma((1,)),
            dma((2, 2 * heads)),
            dma((tp * heads,)),
            dma((nd,)),
            dma((2 * js,)),
            dma((plane * nd,)),
            dma((plane * nd,)),
        ],
        compiler_params=pltpu.CompilerParams(
            collective_id=1, has_side_effects=True, vmem_limit_bytes=60 * 1024 * 1024
        ),
    )(
        block_order,
        hidden[0],
        target[0],
        gain[None, :],
        freqs,
        w_query,
        w_key,
        value_matrix,
        w_out,
    )
    return (branch[None], loss.reshape(()))


def solution(mesh):
    in_specs = (
        P("dp", "ctx", "tp"),
        P("dp", "ctx", "tp"),
        P(),
        P(("ctx", "dp"), "tp"),
        P(("ctx", "dp"), "tp"),
        P(("ctx", "dp"), "tp"),
        P("tp", ("ctx", "dp")),
        P(),
    )
    out_specs = (P("dp", "ctx", "tp"), P())
    sizes = mesh.shape
    fits = sizes["ctx"] == 2 and sizes["tp"] == 4 and sizes["dp"] % 2 == 0
    body = functools.partial(fused, sizes["dp"]) if fits else on_device
    return jax.shard_map(
        body, mesh=mesh, in_specs=in_specs, out_specs=out_specs, check_vma=False
    )
```

```python
import functools

import jax
import numpy as np
import jax.numpy as jnp
from jax import lax
from jax.experimental import pallas as pl
from jax.experimental.pallas import tpu as pltpu
from jax.sharding import PartitionSpec as P

MODEL_WIDTH = 4096
QUERY_HEADS = 16
KEY_VALUE_HEADS = 4
HEAD_SIZE = 128


rope_base = 500000.0


def shifted(value, axis, by):
    peers = lax.axis_size(axis)
    return lax.ppermute(value, axis, [(i, (i + by) % peers) for i in range(peers)])


def positions(order, start, rows, half):
    index = start + lax.iota(jnp.int32, rows)
    block = index // half
    slots = lax.iota(jnp.int32, order.shape[0])
    chosen = jnp.sum(jnp.where(block[:, None] == slots[None, :], order[None, :], 0), axis=1)
    return chosen * half + index % half


def apply_rotary(values, token_places):
    half = values.shape[-1] // 2
    freqs = rope_base ** (-(jnp.arange(half, dtype=jnp.float32) * 2.0) / values.shape[-1])
    angles = token_places.astype(jnp.float32)[:, None] * freqs[None, :]
    cosine = jnp.cos(angles)[:, None, :]
    sine = jnp.sin(angles)[:, None, :]
    first = values[..., :half]
    second = values[..., half:]
    return jnp.concatenate(
        [first * cosine - second * sine, second * cosine + first * sine], axis=-1
    )


def attend(state, query_rows, qpos, piece, kpos):
    peak, total, accum = state
    rows = piece.shape[1]
    local_heads = query_rows.shape[1]
    pair = piece.reshape(2, rows, local_heads, HEAD_SIZE)
    scores = jnp.einsum(
        "qcgd,kcd->cgqk", query_rows, pair[0], preferred_element_type=jnp.float32
    ) * (1.0 / HEAD_SIZE**0.5)
    allowed = (qpos[:, None] >= kpos[None, :])[None, None]
    scores = jnp.where(allowed, scores, -1e30)
    new_peak = jnp.maximum(peak, jnp.max(scores, axis=-1))
    weights = jnp.where(allowed, jnp.exp(scores - new_peak[..., None]), 0.0)
    factor = jnp.exp(peak - new_peak)
    total = total * factor + jnp.sum(weights, axis=-1)
    update = jnp.einsum(
        "cgqk,kcd->qcgd", weights.astype(jnp.bfloat16), pair[1], preferred_element_type=jnp.float32
    )
    accum = accum * jnp.transpose(factor, (2, 0, 1))[..., None] + update
    return (new_peak, total, accum)


def on_device(hidden, target, gain, w_query, w_key, value_matrix, w_out, block_order):
    rows = hidden.shape[1]
    half = rows // 2
    local = hidden[0]
    whole = lax.all_gather(local, "tp", axis=1, tiled=True)
    wide = whole.astype(jnp.float32)
    normed = (
        wide * lax.rsqrt(jnp.mean(wide * wide, axis=1, keepdims=True) + 1e-05) * gain[None, :]
    ).astype(jnp.bfloat16)
    pieces = (
        lax.all_gather(w_query, ("ctx", "dp"), axis=0, tiled=True),
        lax.all_gather(w_key, ("ctx", "dp"), axis=0, tiled=True),
        lax.all_gather(value_matrix, ("ctx", "dp"), axis=0, tiled=True),
    )
    query_rows, key, value_rows = tuple(
        (jnp.dot(normed, piece, preferred_element_type=jnp.float32) for piece in pieces)
    )
    shard = lax.axis_index("ctx")
    qpos = positions(block_order, shard * rows, rows, half)
    local_heads = w_key.shape[1] // HEAD_SIZE
    query_group = QUERY_HEADS // KEY_VALUE_HEADS
    query_rows = (
        apply_rotary(query_rows.reshape(rows, local_heads * query_group, HEAD_SIZE), qpos)
        .astype(jnp.bfloat16)
        .reshape(rows, local_heads, query_group, HEAD_SIZE)
    )
    key = (
        apply_rotary(key.reshape(rows, local_heads, HEAD_SIZE), qpos)
        .astype(jnp.bfloat16)
        .reshape(rows, local_heads * HEAD_SIZE)
    )
    pair = jnp.stack([key, value_rows.astype(jnp.bfloat16)])
    state = (
        jnp.full((local_heads, query_group, rows), -1e30, jnp.float32),
        jnp.zeros((local_heads, query_group, rows), jnp.float32),
        jnp.zeros((rows, local_heads, query_group, HEAD_SIZE), jnp.float32),
    )
    count = lax.axis_size("ctx")
    state = attend(state, query_rows, qpos, pair, qpos)

    def turn(step, carry):
        moved, inner = carry
        moved = shifted(moved, "ctx", 1)
        source = (shard - step) % count
        return (
            moved,
            attend(
                inner, query_rows, qpos, moved, positions(block_order, source * rows, rows, half)
            ),
        )

    moved_end, state = lax.fori_loop(1, count, turn, (pair, state))
    peak, total, accum = state
    attn = (
        (accum / jnp.transpose(total, (2, 0, 1))[..., None])
        .astype(jnp.bfloat16)
        .reshape(rows, local_heads * query_group * HEAD_SIZE)
    )
    terms = jnp.dot(
        attn,
        lax.all_gather(w_out, ("ctx", "dp"), axis=1, tiled=True),
        preferred_element_type=jnp.float32,
    )
    summed = lax.psum_scatter(terms.astype(jnp.bfloat16), "tp", scatter_dimension=1, tiled=True)
    resid = local.astype(jnp.float32) + summed.astype(jnp.float32) - target[0].astype(jnp.float32)
    squares = lax.psum(jnp.sum(resid * resid), ("ctx", "tp", "dp"))
    loss = squares / (lax.axis_size("dp") * lax.axis_size("ctx") * rows * MODEL_WIDTH)
    return (summed[None], loss)


MESH = pl.DeviceIdType.MESH
F32 = jnp.float32
BF16 = jnp.bfloat16


def layer(
    nd,
    order_in,
    hidden,
    target,
    gain,
    freqs,
    w_query,
    w_key,
    value_matrix,
    w_out,
    out,
    loss,
    ga,
    stage,
    go,
    ostage,
    mine,
    xs,
    goal,
    normed,
    acc,
    trig,
    query,
    kv,
    attn,
    made,
    arrived,
    tile,
    sums,
    gains,
    turns,
    order,
    load_sem,
    x_send,
    a_send,
    a_recv,
    oy_send,
    oy_recv,
    o_send,
    o_recv,
    h_send,
    h_recv,
    kv_send,
    kv_recv,
    at_send,
    at_recv,
    r_send,
    r_recv,
    l_send,
    l_recv,
):
    c, t, d = lax.axis_index("ctx"), lax.axis_index("tp"), lax.axis_index("dp")
    y, k = t // 2, t % 2
    sibling = y * 2 + (1 - k)
    across = (1 - y) * 2 + k
    rows, wide = hidden.shape
    deep, qcols = w_query.shape
    half = rows // 2
    n_heads = qcols // HEAD_SIZE
    tp = 4
    plane = 2 * tp
    owner = c == k
    up, down = d < nd - 1, d > 0

    def load(i, src, dst):
        return pltpu.make_async_copy(src, dst, load_sem.at[i])

    quarter = deep // 4

    def rows_of(piece):
        return pl.ds(pl.multiple_of(piece * quarter, quarter), quarter)

    def weight_loads(dst):
        return (
            load(0, w_query, dst.at[:, pl.ds(0, qcols)]),
            load(1, w_key, dst.at[:, pl.ds(qcols, HEAD_SIZE)]),
            load(2, value_matrix, dst.at[:, pl.ds(qcols + HEAD_SIZE, HEAD_SIZE)]),
        )

    hc = w_out.shape[1] // 2
    hq = hc // 2
    own_loads = weight_loads(ga.at[c * nd + d])
    stage_loads = weight_loads(stage)
    mine_load = load(3, hidden, mine)

    def columns_of(half_of, part):
        return pl.ds(pl.multiple_of(half_of * hc + part * hq, hq), hq)

    keep_loads = [
        load(4 + e, w_out.at[:, columns_of(y, e)], go.at[d, k, e, y]) for e in range(2)
    ]
    give_loads = [
        load(6 + e, w_out.at[:, columns_of(1 - y, e)], ostage.at[e]) for e in range(2)
    ]
    local_load = load(8, hidden, xs.at[t])
    goal_load = load(9, target, goal)
    gain_load = load(10, gain, gains)
    turn_load = load(11, freqs, turns)
    order_load = load(12, order_in, order)

    @pl.when(owner)
    def _():
        for copy in own_loads:
            copy.start()

    @pl.when(jnp.logical_not(owner))
    def _():
        for copy in stage_loads:
            copy.start()

    mine_load.start()
    order_load.start()
    turn_load.start()
    for copy in give_loads + keep_loads:
        copy.start()

    @pl.when(owner)
    def _():
        local_load.start()

    goal_load.start()
    gain_load.start()

    barrier = pltpu.get_barrier_semaphore()
    seat = c * tp + t
    for s in range(1, plane):
        p = (seat + s) % plane
        pl.semaphore_signal(
            barrier, inc=1, device_id={"ctx": p // tp, "tp": p % tp}, device_id_type=MESH
        )
    for there, step in ((up, 1), (down, -1)):

        @pl.when(there)
        def _():
            pl.semaphore_signal(barrier, inc=1, device_id={"dp": d + step}, device_id_type=MESH)

    pl.semaphore_wait(barrier, plane - 1 + up.astype(jnp.int32) + down.astype(jnp.int32))

    def remote(src, dst, ssem, rsem, where):
        return pltpu.make_async_remote_copy(
            src_ref=src, dst_ref=dst, send_sem=ssem, recv_sem=rsem,
            device_id=where, device_id_type=MESH,
        )

    UP, DOWN, SIB = 0, 1, 2

    def target_of(way):
        return {
            UP: {"dp": jnp.minimum(d + 1, nd - 1)},
            DOWN: {"dp": jnp.maximum(d - 1, 0)},
            SIB: {"tp": sibling},
        }[way]

    def a_copy(line, i, way, e, core=k):
        b, piece = line * nd + i, 2 * core + e
        ref = ga.at[b, rows_of(piece)]
        return remote(ref, ref, a_send.at[way, b, e], a_recv.at[b, piece], target_of(way))

    def o_copy(i, way, e, core=k):
        ref = go.at[i, core, e]
        return remote(
            ref, ref, o_send.at[way, i, e], o_recv.at[core * nd + i, e], target_of(way)
        )

    def spread(copy, i, ways, e):
        copy_up = lambda: copy(i, UP, e).start()
        copy_down = lambda: copy(i, DOWN, e).start()
        if UP in ways:
            pl.when(up)(copy_up)
        if DOWN in ways:
            pl.when(down)(copy_down)
        if SIB in ways:
            copy(i, SIB, e).start()

    def relay(copy, s, parts=(0, 1)):
        for e in parts:

            @pl.when(d >= s)
            def _():
                copy(d - s, UP, e).wait_recv()
                spread(copy, d - s, (UP, SIB), e)

            @pl.when(d + s < nd)
            def _():
                copy(d + s, DOWN, e).wait_recv()
                spread(copy, d + s, (DOWN, SIB), e)

    near_copy = functools.partial(a_copy, c)
    far_copy = functools.partial(a_copy, 1 - c)
    b_own = c * nd + d
    half_copies = []
    x_copies = []
    for e in range(2):
        ref = ga.at[b_own, rows_of(2 * (1 - k) + e)]
        half_copies.append(
            remote(
                ref, ref, x_send.at[4 + e], a_recv.at[b_own, 2 * (1 - k) + e], {"tp": sibling}
            )
        )
        for h in range(2):
            piece = 2 * h + e
            x_copies.append(
                remote(
                    stage.at[rows_of(piece)],
                    ga.at[b_own, rows_of(piece)],
                    x_send.at[piece],
                    a_recv.at[b_own, piece],
                    {"ctx": 1 - c, "tp": y * 2 + h},
                )
            )

    @pl.when(owner)
    def _():
        for copy in own_loads:
            copy.wait()
        for e in range(2):
            half_copies[e].start()
            spread(near_copy, d, (UP, DOWN), e)
        for e in range(2):
            spread(near_copy, d, (SIB,), e)

    @pl.when(jnp.logical_not(owner))
    def _():
        for copy in stage_loads:
            copy.wait()
        for copy in x_copies:
            copy.start()

    mine_load.wait()
    h_y = remote(mine, xs.at[t], h_send.at[0], h_recv.at[t], {"tp": (1 - y) * 2 + c})
    h_x = remote(mine, xs.at[t], h_send.at[1], h_recv.at[t], {"ctx": 1 - c, "tp": y * 2 + c})
    h_sib = remote(mine, xs.at[t], h_send.at[2], h_recv.at[t], {"tp": sibling})
    h_y.start()

    @pl.when(jnp.logical_not(owner) & (k == 0))
    def _():
        h_x.start()

    @pl.when(jnp.logical_not(owner))
    def _():
        h_sib.start()
        for e in range(2):
            near_copy(d, UP, e).wait_recv()
            spread(near_copy, d, (UP, DOWN), e)

    oy_copies = []
    for e in range(2):
        give_loads[e].wait()
        oy_copies.append(
            remote(
                ostage.at[e], go.at[d, k, e, y], oy_send.at[e], oy_recv.at[e], {"tp": across}
            )
        )
        oy_copies[e].start()

    def positions_of(shard, index):
        low = order[2 * shard] * half
        high = order[2 * shard + 1] * half
        return jnp.where(index < half, low + index, high + index - half)

    order_load.wait()
    turn_load.wait()
    place = positions_of(k, lax.broadcasted_iota(jnp.int32, (rows, HEAD_SIZE), 0)).astype(F32)
    angle = place * turns[...]
    lane_of = lax.broadcasted_iota(jnp.int32, (rows, HEAD_SIZE), 1)
    trig[0] = jnp.cos(angle)
    sine = jnp.sin(angle)
    trig[1] = jnp.where(lane_of < HEAD_SIZE // 2, -sine, sine)

    for s in range(1, min(2, nd - 1)):
        relay(near_copy, s)

    @pl.when(owner & (k == 0))
    def _():
        h_x.start()

    for e in range(2):
        far_copy(d, UP, e).wait_recv()
        spread(far_copy, d, (UP, DOWN, SIB), e)

    for s in range(2, nd - 1):
        relay(near_copy, s)

    @pl.when(k == 1)
    def _():
        h_x.start()

    def h_wait(slot):
        remote(mine, xs.at[slot], h_send.at[0], h_recv.at[slot], {"tp": across}).wait_recv()

    far = (1 - y) * 2
    h_relay_x = remote(
        xs.at[far + 1], xs.at[far + 1], h_send.at[3], h_recv.at[far + 1], {"ctx": 1 - c}
    )
    h_relay_y = remote(
        xs.at[y * 2], xs.at[y * 2], h_send.at[3], h_recv.at[y * 2], {"tp": across}
    )

    @pl.when(owner)
    def _():
        h_wait(far + 1)
        h_relay_x.start()

    @pl.when(jnp.logical_not(owner))
    def _():
        h_wait(y * 2)
        h_relay_y.start()

    for s in range(1, min(2, nd - 1)):
        relay(far_copy, s)

    for s in range(2, nd - 1):
        relay(far_copy, s)

    for e in range(2):
        keep_loads[e].wait()
        remote(
            ostage.at[e], go.at[d, k, e, 1 - y], oy_send.at[e], oy_recv.at[e], {"tp": across}
        ).wait_recv()
        spread(o_copy, d, (UP, DOWN, SIB), e)

    @pl.when(owner)
    def _():
        local_load.wait()
        h_wait(sibling)
        h_wait(far)

    @pl.when(jnp.logical_not(owner))
    def _():
        h_wait(y * 2 + 1)
        h_wait(far)
        h_wait(far + 1)

    gain_load.wait()
    chunk = min(64, rows)
    per = wide // deep

    def norm_rows(i, carry):
        r = pl.multiple_of(i * chunk, chunk)
        total = jnp.zeros((chunk, 1), F32)
        for j in range(tp):
            v = xs[j, pl.ds(r, chunk), :].astype(F32)
            total = total + jnp.sum(v * v, axis=1, keepdims=True)
        scale = lax.rsqrt(total * (1.0 / (tp * wide)) + 1e-05)
        for j in range(tp):
            for m in range(per):
                v = xs[j, pl.ds(r, chunk), m * deep : (m + 1) * deep].astype(F32)
                g = gains[:, j * wide + m * deep : j * wide + (m + 1) * deep]
                normed[j * per + m, pl.ds(r, chunk), :] = (v * scale * g).astype(BF16)
        return carry

    lax.fori_loop(0, rows // chunk, norm_rows, 0)
    acc[...] = jnp.zeros_like(acc)

    def nearest(i):
        return jnp.where(d < nd // 2, i, nd - 1 - i)

    def project(i, line):
        b = line * nd + i

        @pl.when(jnp.logical_not(owner & (b == b_own)))
        def _():
            for e in range(2):
                a_copy(line, i, SIB, e, 1 - k).wait_recv()

        acc[...] += jnp.dot(normed[b], ga[b], preferred_element_type=F32)

    def project_step(i, carry):
        @pl.when(i == nd - 1)
        def _():
            relay(near_copy, nd - 1)

        project(nearest(i), c)

        @pl.when(i == nd - 1)
        def _():
            relay(far_copy, nd - 1)

        project(nearest(i), 1 - c)
        return carry

    lax.fori_loop(0, nd, project_step, 0)

    def rotated(v):
        return (v * trig[0] + pltpu.roll(v, HEAD_SIZE // 2, 1) * trig[1]).astype(BF16)

    kv[k, :, 0:HEAD_SIZE] = rotated(acc[:, qcols : qcols + HEAD_SIZE])
    kv[k, :, HEAD_SIZE:] = acc[:, qcols + HEAD_SIZE :].astype(BF16)
    kv_copy = remote(kv.at[k], kv.at[k], kv_send.at[0], kv_recv.at[0], {"tp": sibling})
    kv_copy.start()
    for h in range(n_heads):
        part = slice(h * HEAD_SIZE, (h + 1) * HEAD_SIZE)
        query[h] = rotated(acc[:, part])
    remote(kv.at[1 - k], kv.at[1 - k], kv_send.at[0], kv_recv.at[0], {"tp": sibling}).wait_recv()
    qrows = min(256, rows)
    dims = (((1,), (1,)), ((), ()))
    group = y * 2 + c
    spots = ({"ctx": 1 - c}, {"tp": across})
    x_group, y_group = y * 2 + 1 - c, (1 - y) * 2 + c

    def at_copy(h, way, source=group):
        b = source * n_heads + h
        ref = attn.at[b]
        sem = at_send.at[way, jnp.where(source == group, 0, n_heads) + h]
        return remote(ref, ref, sem, at_recv.at[b], spots[way])

    def attend_head(h, carry):
        def attend_block(i, inner):
            r = pl.multiple_of(i * qrows, qrows)
            q = query[h, pl.ds(r, qrows), :]
            qpos = positions_of(k, r + lax.broadcasted_iota(jnp.int32, (qrows, rows), 0))
            scores = []
            for n in range(2):
                kpos = positions_of(n, lax.broadcasted_iota(jnp.int32, (qrows, rows), 1))
                sc = lax.dot_general(
                    q, kv[n, :, 0:HEAD_SIZE], dims, preferred_element_type=F32
                ) * (1.0 / HEAD_SIZE**0.5)
                scores.append(jnp.where(qpos >= kpos, sc, -1e30))
            peak = jnp.maximum(
                jnp.max(scores[0], axis=1, keepdims=True),
                jnp.max(scores[1], axis=1, keepdims=True),
            )
            total = jnp.zeros((qrows, 1), F32)
            value = jnp.zeros((qrows, HEAD_SIZE), F32)
            for n in range(2):
                p = jnp.exp(scores[n] - peak)
                total = total + jnp.sum(p, axis=1, keepdims=True)
                value = value + jnp.dot(
                    p.astype(BF16), kv[n, :, HEAD_SIZE:], preferred_element_type=F32
                )
            attn[group * n_heads + h, pl.ds(r, qrows), :] = (value / total).astype(BF16)
            return inner

        lax.fori_loop(0, rows // qrows, attend_block, 0)
        for way in range(2):
            at_copy(h, way).start()
        return carry

    lax.fori_loop(0, n_heads, attend_head, 0)

    for s in range(1, min(2, nd - 1)):
        relay(o_copy, s)

    early = n_heads // 2

    def at_relay(h, carry):
        at_copy(h, 0, x_group).wait_recv()
        at_copy(h, 1, x_group).start()
        at_copy(early + h, 1, y_group).wait_recv()
        at_copy(early + h, 0, y_group).start()
        return carry

    lax.fori_loop(0, early, at_relay, 0)

    for s in range(2, nd - 1):
        relay(o_copy, s)


    def at_wait(h, carry):
        at_copy(early + h, 0, x_group).wait_recv()
        at_copy(h, 1, y_group).wait_recv()
        return carry

    lax.fori_loop(0, early, at_wait, 0)
    z_group = (1 - y) * 2 + 1 - c

    def far_wait(h, carry):
        at_copy(h, 1, z_group).wait_recv()
        return carry

    lax.fori_loop(0, n_heads, far_wait, 0)

    js = nd // 2
    orow = min(256, rows)

    def made_copy(i, e):
        slot = (i % js) * 2 + y
        where = {"ctx": k, "tp": c * 2 + i // js}
        return remote(
            made.at[i, e], arrived.at[slot, e], r_send.at[i, e], r_recv.at[slot, e], where
        )

    def stays(i):
        return (k == c) & (y == c) & (i // js == k)

    def out_step(n, carry):
        i, e = nearest(n // 2), n % 2

        @pl.when(n >= 2 * (nd - 1))
        def _():
            relay(o_copy, nd - 1, (e,))

        o_copy(i, SIB, e, 1 - k).wait_recv()

        def out_rows(m, inner):
            rr = pl.ds(pl.multiple_of(m * orow, orow), orow)
            total = jnp.zeros((orow, hq), F32)
            for g in range(tp):
                full = jnp.concatenate(
                    [attn[g * n_heads + h, rr, :] for h in range(n_heads)], axis=1
                )
                term = jnp.dot(full, go[i, g % 2, e, g // 2], preferred_element_type=F32)
                total = total + term.astype(BF16).astype(F32)
            made[i, e, rr, :] = total.astype(BF16)
            return inner

        lax.fori_loop(0, rows // orow, out_rows, 0)

        @pl.when(jnp.logical_not(stays(i)))
        def _():
            made_copy(i, e).start()

        @pl.when(stays(i))
        def _():
            arrived[(i % js) * 2 + y, e] = made[i, e]

        return carry

    lax.fori_loop(0, 2 * nd, out_step, 0)
    goal_load.wait()
    tile[...] = jnp.zeros_like(tile)

    last = min(256, rows)

    def finish_block(n, carry):
        j = jnp.where(d < nd // 2, n // 4, js - 1 - n // 4)
        e, side = n // 2 % 2, n % 2
        slot = j * 2 + side

        @pl.when(jnp.logical_not((y == c) & (side == y) & (c == k)))
        def _():
            remote(
                made.at[0, 0], arrived.at[slot, e], r_send.at[0, 0], r_recv.at[slot, e],
                {"tp": sibling},
            ).wait_recv()

        place = pl.ds(pl.multiple_of(slot * hc + e * hq, hq), hq)

        def finish(i, inner):
            rr = pl.ds(pl.multiple_of(i * last, last), last)
            result = arrived[slot, e, rr, :]
            out[rr, place] = result
            resid = mine[rr, place].astype(F32) + result.astype(F32)
            resid = resid - goal[rr, place].astype(F32)
            tile[...] += jnp.sum((resid * resid).reshape(last // 8, 8, hq), axis=0)
            return inner

        lax.fori_loop(0, rows // last, finish, 0)
        return carry

    lax.fori_loop(0, 4 * js, finish_block, 0)

    everyone = plane * nd
    number = d * plane + seat

    def l_copy(s):
        p = (number + s) % everyone
        return remote(
            sums.at[number], sums.at[number], l_send.at[0], l_recv.at[0],
            {"ctx": p % plane // tp, "tp": p % tp, "dp": p // plane},
        )

    others = sums.at[pl.ds(0, everyone - 1)]
    l_all = remote(others, others, l_send.at[0], l_recv.at[0], {"tp": sibling})
    sums[number] = tile[...]

    def share(s, carry):
        l_copy(s).start()
        return carry

    lax.fori_loop(1, everyone, share, 0)
    l_all.wait_recv()
    whole = sums[0]
    for b in range(1, everyone):
        whole = whole + sums[b]
    count = plane * nd * rows * wide
    loss[...] = jnp.full(loss.shape, jnp.sum(whole) / count, F32)

    @pl.when(owner)
    def _():
        for copy in half_copies:
            copy.wait_send()

    @pl.when(jnp.logical_not(owner))
    def _():
        for copy in x_copies:
            copy.wait_send()
        h_sib.wait_send()

    h_y.wait_send()
    h_x.wait_send()
    h_relay_x.wait_send()
    for copy in oy_copies:
        copy.wait_send()
    kv_copy.wait_send()

    def drain_heads(h, carry):
        for way in range(2):
            at_copy(h, way).wait_send()
        return carry

    lax.fori_loop(0, n_heads, drain_heads, 0)

    def drain_relays(h, carry):
        at_copy(h, 1, x_group).wait_send()
        at_copy(early + h, 0, y_group).wait_send()
        return carry

    lax.fori_loop(0, early, drain_relays, 0)

    def drain_line(n, carry):
        i, e = n // 2, n % 2

        @pl.when(owner | (i != d))
        def _():
            near_copy(i, SIB, e).wait_send()

        far_copy(i, SIB, e).wait_send()
        o_copy(i, SIB, e).wait_send()
        for copy in (near_copy, far_copy, o_copy):

            @pl.when(up & (i <= d))
            def _():
                copy(i, UP, e).wait_send()

            @pl.when(down & (i >= d))
            def _():
                copy(i, DOWN, e).wait_send()

        @pl.when(jnp.logical_not(stays(i)))
        def _():
            made_copy(i, e).wait_send()

        return carry

    lax.fori_loop(0, 2 * nd, drain_line, 0)
    l_all.wait_send()


def fused(nd, hidden, target, gain, w_query, w_key, value_matrix, w_out, block_order):
    rows, wide = hidden.shape[1:]
    nb = 2 * nd
    tp = 4
    plane = 2 * tp
    deep, qcols = w_query.shape
    all_cols = qcols + w_key.shape[1] + value_matrix.shape[1]
    orows, ocols = w_out.shape
    hc = ocols // 2
    order_shape = block_order.shape
    half = HEAD_SIZE // 2
    freqs = np.float64(rope_base) ** (-np.arange(half) * 2.0 / HEAD_SIZE)
    freqs = jnp.asarray(np.concatenate([freqs, freqs])[None, :].astype(np.float32))
    heads = qcols // HEAD_SIZE
    js = nd // 2
    anyspace = pl.BlockSpec(memory_space=pltpu.HBM)
    vmem = pl.BlockSpec(memory_space=pltpu.VMEM)
    dma = pltpu.SemaphoreType.DMA
    branch, loss = pl.pallas_call(
        functools.partial(layer, nd),
        out_shape=(
            jax.ShapeDtypeStruct((rows, wide), BF16),
            jax.ShapeDtypeStruct((1, 128), F32),
        ),
        in_specs=[
            anyspace,
            anyspace,
            anyspace,
            anyspace,
            anyspace,
            anyspace,
            anyspace,
            anyspace,
            anyspace,
        ],
        out_specs=(vmem, vmem),
        scratch_shapes=[
            pltpu.VMEM((nb, deep, all_cols), BF16),
            pltpu.VMEM((deep, all_cols), BF16),
            pltpu.VMEM((nd, 2, 2, 2, orows, hc // 2), BF16),
            pltpu.VMEM((2, orows, hc // 2), BF16),
            pltpu.VMEM((rows, wide), BF16),
            pltpu.VMEM((tp, rows, wide), BF16),
            pltpu.VMEM((rows, wide), BF16),
            pltpu.VMEM((nb, rows, deep), BF16),
            pltpu.VMEM((rows, all_cols), F32),
            pltpu.VMEM((2, rows, HEAD_SIZE), F32),
            pltpu.VMEM((heads, rows, HEAD_SIZE), BF16),
            pltpu.VMEM((2, rows, 2 * HEAD_SIZE), BF16),
            pltpu.VMEM((tp * heads, rows, HEAD_SIZE), BF16),
            pltpu.VMEM((nd, 2, rows, hc // 2), BF16),
            pltpu.VMEM((2 * js, 2, rows, hc // 2), BF16),
            pltpu.VMEM((8, hc // 2), F32),
            pltpu.VMEM((plane * nd, 8, hc // 2), F32),
            pltpu.VMEM((1, tp * wide), F32),
            pltpu.VMEM((1, HEAD_SIZE), F32),
            pltpu.SMEM(order_shape, jnp.int32),
            dma((13,)),
            dma((6,)),
            dma((3, nb, 2)),
            dma((nb, 4)),
            dma((2,)),
            dma((2,)),
            dma((3, nd, 2)),
            dma((nb, 2)),
            dma((4,)),
            dma((tp,)),
            dma((1,)),
            dma((1,)),
            dma((2, 2 * heads)),
            dma((tp * heads,)),
            dma((nd, 2)),
            dma((2 * js, 2)),
            dma((1,)),
            dma((1,)),
        ],
        compiler_params=pltpu.CompilerParams(
            collective_id=1, has_side_effects=True, vmem_limit_bytes=36 * 1024 * 1024
        ),
    )(
        *(
            pltpu.with_memory_space_constraint(v, pltpu.HBM)
            for v in (
                block_order,
                hidden[0],
                target[0],
                gain[None, :],
                freqs,
                w_query,
                w_key,
                value_matrix,
                w_out,
            )
        )
    )
    return (branch[None], loss[0, 0])


def solution(mesh):
    in_specs = (
        P("dp", "ctx", "tp"),
        P("dp", "ctx", "tp"),
        P(),
        P(("ctx", "dp"), "tp"),
        P(("ctx", "dp"), "tp"),
        P(("ctx", "dp"), "tp"),
        P("tp", ("ctx", "dp")),
        P(),
    )
    out_specs = (P("dp", "ctx", "tp"), P())
    sizes = mesh.shape
    fits = sizes["ctx"] == 2 and sizes["tp"] == 4 and sizes["dp"] % 2 == 0
    body = functools.partial(fused, sizes["dp"]) if fits else on_device
    return jax.shard_map(
        body, mesh=mesh, in_specs=in_specs, out_specs=out_specs, check_vma=False
    )
```

```python
import functools

import jax
import numpy as np
import jax.numpy as jnp
from jax import lax
from jax.experimental import pallas as pl
from jax.experimental.pallas import tpu as pltpu
from jax.sharding import PartitionSpec as P

MODEL_WIDTH = 4096
QUERY_HEADS = 16
KEY_VALUE_HEADS = 4
HEAD_SIZE = 128


rope_base = 500000.0


def shifted(value, axis, by):
    peers = lax.axis_size(axis)
    return lax.ppermute(value, axis, [(i, (i + by) % peers) for i in range(peers)])


def positions(order, start, rows, half):
    index = start + lax.iota(jnp.int32, rows)
    block = index // half
    slots = lax.iota(jnp.int32, order.shape[0])
    chosen = jnp.sum(jnp.where(block[:, None] == slots[None, :], order[None, :], 0), axis=1)
    return chosen * half + index % half


def apply_rotary(values, token_places):
    half = values.shape[-1] // 2
    freqs = rope_base ** (-(jnp.arange(half, dtype=jnp.float32) * 2.0) / values.shape[-1])
    angles = token_places.astype(jnp.float32)[:, None] * freqs[None, :]
    cosine = jnp.cos(angles)[:, None, :]
    sine = jnp.sin(angles)[:, None, :]
    first = values[..., :half]
    second = values[..., half:]
    return jnp.concatenate(
        [first * cosine - second * sine, second * cosine + first * sine], axis=-1
    )


def attend(state, query_rows, qpos, piece, kpos):
    peak, total, accum = state
    rows = piece.shape[1]
    local_heads = query_rows.shape[1]
    pair = piece.reshape(2, rows, local_heads, HEAD_SIZE)
    scores = jnp.einsum(
        "qcgd,kcd->cgqk", query_rows, pair[0], preferred_element_type=jnp.float32
    ) * (1.0 / HEAD_SIZE**0.5)
    allowed = (qpos[:, None] >= kpos[None, :])[None, None]
    scores = jnp.where(allowed, scores, -1e30)
    new_peak = jnp.maximum(peak, jnp.max(scores, axis=-1))
    weights = jnp.where(allowed, jnp.exp(scores - new_peak[..., None]), 0.0)
    factor = jnp.exp(peak - new_peak)
    total = total * factor + jnp.sum(weights, axis=-1)
    update = jnp.einsum(
        "cgqk,kcd->qcgd", weights.astype(jnp.bfloat16), pair[1], preferred_element_type=jnp.float32
    )
    accum = accum * jnp.transpose(factor, (2, 0, 1))[..., None] + update
    return (new_peak, total, accum)


def on_device(hidden, target, gain, w_query, w_key, value_matrix, w_out, block_order):
    rows = hidden.shape[1]
    half = rows // 2
    local = hidden[0]
    whole = lax.all_gather(local, "tp", axis=1, tiled=True)
    wide = whole.astype(jnp.float32)
    normed = (
        wide * lax.rsqrt(jnp.mean(wide * wide, axis=1, keepdims=True) + 1e-05) * gain[None, :]
    ).astype(jnp.bfloat16)
    pieces = (
        lax.all_gather(w_query, ("ctx", "dp"), axis=0, tiled=True),
        lax.all_gather(w_key, ("ctx", "dp"), axis=0, tiled=True),
        lax.all_gather(value_matrix, ("ctx", "dp"), axis=0, tiled=True),
    )
    query_rows, key, value_rows = tuple(
        (jnp.dot(normed, piece, preferred_element_type=jnp.float32) for piece in pieces)
    )
    shard = lax.axis_index("ctx")
    qpos = positions(block_order, shard * rows, rows, half)
    local_heads = w_key.shape[1] // HEAD_SIZE
    query_group = QUERY_HEADS // KEY_VALUE_HEADS
    query_rows = (
        apply_rotary(query_rows.reshape(rows, local_heads * query_group, HEAD_SIZE), qpos)
        .astype(jnp.bfloat16)
        .reshape(rows, local_heads, query_group, HEAD_SIZE)
    )
    key = (
        apply_rotary(key.reshape(rows, local_heads, HEAD_SIZE), qpos)
        .astype(jnp.bfloat16)
        .reshape(rows, local_heads * HEAD_SIZE)
    )
    pair = jnp.stack([key, value_rows.astype(jnp.bfloat16)])
    state = (
        jnp.full((local_heads, query_group, rows), -1e30, jnp.float32),
        jnp.zeros((local_heads, query_group, rows), jnp.float32),
        jnp.zeros((rows, local_heads, query_group, HEAD_SIZE), jnp.float32),
    )
    count = lax.axis_size("ctx")
    state = attend(state, query_rows, qpos, pair, qpos)

    def turn(step, carry):
        moved, inner = carry
        moved = shifted(moved, "ctx", 1)
        source = (shard - step) % count
        return (
            moved,
            attend(
                inner, query_rows, qpos, moved, positions(block_order, source * rows, rows, half)
            ),
        )

    moved_end, state = lax.fori_loop(1, count, turn, (pair, state))
    peak, total, accum = state
    attn = (
        (accum / jnp.transpose(total, (2, 0, 1))[..., None])
        .astype(jnp.bfloat16)
        .reshape(rows, local_heads * query_group * HEAD_SIZE)
    )
    terms = jnp.dot(
        attn,
        lax.all_gather(w_out, ("ctx", "dp"), axis=1, tiled=True),
        preferred_element_type=jnp.float32,
    )
    summed = lax.psum_scatter(terms.astype(jnp.bfloat16), "tp", scatter_dimension=1, tiled=True)
    resid = local.astype(jnp.float32) + summed.astype(jnp.float32) - target[0].astype(jnp.float32)
    squares = lax.psum(jnp.sum(resid * resid), ("ctx", "tp", "dp"))
    loss = squares / (lax.axis_size("dp") * lax.axis_size("ctx") * rows * MODEL_WIDTH)
    return (summed[None], loss)


MESH = pl.DeviceIdType.MESH
F32 = jnp.float32
BF16 = jnp.bfloat16


def layer(
    nd,
    order_in,
    hidden,
    target,
    gain,
    freqs,
    w_query,
    w_key,
    value_matrix,
    w_out,
    out,
    loss,
    ga,
    stage,
    go,
    ostage,
    mine,
    xs,
    goal,
    normed,
    acc,
    trig,
    query,
    kv,
    attn,
    made,
    arrived,
    want,
    tile,
    sums,
    gains,
    turns,
    order,
    load_sem,
    x_send,
    a_send,
    a_recv,
    sib_recv,
    oy_send,
    oy_recv,
    o_send,
    o_recv,
    h_send,
    h_recv,
    kv_send,
    kv_recv,
    at_send,
    at_recv,
    r_send,
    r_recv,
    w_send,
    w_recv,
    l_send,
    l_recv,
):
    c, t, d = lax.axis_index("ctx"), lax.axis_index("tp"), lax.axis_index("dp")
    y, k = t // 2, t % 2
    sibling = y * 2 + (1 - k)
    across = (1 - y) * 2 + k
    rows, wide = hidden.shape
    deep, qcols = w_query.shape
    half = rows // 2
    n_heads = qcols // HEAD_SIZE
    tp = 4
    plane = 2 * tp
    owner = c == k
    up, down = d < nd - 1, d > 0

    def load(i, src, dst):
        return pltpu.make_async_copy(src, dst, load_sem.at[i])

    quarter = deep // 4

    def rows_of(piece):
        return pl.ds(pl.multiple_of(piece * quarter, quarter), quarter)

    def weight_loads(dst):
        return (
            load(0, w_query, dst.at[:, pl.ds(0, qcols)]),
            load(1, w_key, dst.at[:, pl.ds(qcols, HEAD_SIZE)]),
            load(2, value_matrix, dst.at[:, pl.ds(qcols + HEAD_SIZE, HEAD_SIZE)]),
        )

    hc = w_out.shape[1] // 2
    hq = hc // 2
    own_loads = weight_loads(ga.at[c * nd + d])
    stage_loads = weight_loads(stage)
    mine_load = load(3, hidden, mine)

    def columns_of(half_of, part):
        return pl.ds(pl.multiple_of(half_of * hc + part * hq, hq), hq)

    keep_loads = [
        load(4 + e, w_out.at[:, columns_of(y, e)], go.at[d * 2 + k, e, y]) for e in range(2)
    ]
    give_loads = [
        load(6 + e, w_out.at[:, columns_of(1 - y, e)], ostage.at[e]) for e in range(2)
    ]
    local_load = load(8, hidden, xs.at[t])
    goal_load = load(9, target, goal)
    gain_load = load(10, gain, gains)
    turn_load = load(11, freqs, turns)
    order_load = load(12, order_in, order)

    @pl.when(owner)
    def _():
        for copy in own_loads:
            copy.start()

    @pl.when(jnp.logical_not(owner))
    def _():
        for copy in stage_loads:
            copy.start()

    mine_load.start()
    order_load.start()
    turn_load.start()
    for copy in give_loads + keep_loads:
        copy.start()

    @pl.when(owner)
    def _():
        local_load.start()

    goal_load.start()
    gain_load.start()

    barrier = pltpu.get_barrier_semaphore()
    seat = c * tp + t
    for s in range(1, plane):
        p = (seat + s) % plane
        pl.semaphore_signal(
            barrier, inc=1, device_id={"ctx": p // tp, "tp": p % tp}, device_id_type=MESH
        )
    for there, step in ((up, 1), (down, -1)):

        @pl.when(there)
        def _():
            pl.semaphore_signal(barrier, inc=1, device_id={"dp": d + step}, device_id_type=MESH)

    pl.semaphore_wait(barrier, plane - 1 + up.astype(jnp.int32) + down.astype(jnp.int32))

    def remote(src, dst, ssem, rsem, where):
        return pltpu.make_async_remote_copy(
            src_ref=src, dst_ref=dst, send_sem=ssem, recv_sem=rsem,
            device_id=where, device_id_type=MESH,
        )

    UP, DOWN, SIB = 0, 1, 2

    def target_of(way):
        return {
            UP: {"dp": jnp.minimum(d + 1, nd - 1)},
            DOWN: {"dp": jnp.maximum(d - 1, 0)},
            SIB: {"tp": sibling},
        }[way]

    def a_copy(line, i, way, e, core=k):
        b = line * nd + i
        ref = ga.at[b, rows_of(2 * core + e)]
        there = sib_recv.at[b] if way == SIB else a_recv.at[b, e]
        return remote(ref, ref, a_send.at[int(way == SIB)], there, target_of(way))

    def o_copy(i, way, e, core=k):
        ref = go.at[i * 2 + core, e]
        there = o_recv.at[core * nd + i, e]
        return remote(ref, ref, o_send.at[int(way == SIB)], there, target_of(way))

    def spread(copy, i, ways, e):
        copy_up = lambda: copy(i, UP, e).start()
        copy_down = lambda: copy(i, DOWN, e).start()
        if UP in ways:
            pl.when(up)(copy_up)
        if DOWN in ways:
            pl.when(down)(copy_down)
        if SIB in ways:
            copy(i, SIB, e).start()

    def relay(copy, s, parts=(0, 1)):
        for e in parts:

            @pl.when(d >= s)
            def _():
                copy(d - s, UP, e).wait_recv()
                spread(copy, d - s, (UP, SIB), e)

            @pl.when(d + s < nd)
            def _():
                copy(d + s, DOWN, e).wait_recv()
                spread(copy, d + s, (DOWN, SIB), e)

    near_copy = functools.partial(a_copy, c)
    far_copy = functools.partial(a_copy, 1 - c)
    b_own = c * nd + d
    half_copies = []
    x_copies = []
    for e in range(2):
        ref = ga.at[b_own, rows_of(2 * (1 - k) + e)]
        half_copies.append(
            remote(
                ref, ref, x_send.at[0], a_recv.at[b_own, e], {"tp": sibling}
            )
        )
        for h in range(2):
            piece = 2 * h + e
            x_copies.append(
                remote(
                    stage.at[rows_of(piece)],
                    ga.at[b_own, rows_of(piece)],
                    x_send.at[0],
                    a_recv.at[b_own, e],
                    {"ctx": 1 - c, "tp": y * 2 + h},
                )
            )

    @pl.when(owner)
    def _():
        for copy in own_loads:
            copy.wait()
        for e in range(2):
            half_copies[e].start()
            spread(near_copy, d, (UP, DOWN), e)
        for e in range(2):
            spread(near_copy, d, (SIB,), e)

    @pl.when(jnp.logical_not(owner))
    def _():
        for copy in stage_loads:
            copy.wait()
        for copy in x_copies:
            copy.start()

    mine_load.wait()
    h_y = remote(mine, xs.at[t], h_send.at[0], h_recv.at[t], {"tp": (1 - y) * 2 + c})
    h_x = remote(mine, xs.at[t], h_send.at[1], h_recv.at[t], {"ctx": 1 - c, "tp": y * 2 + c})
    h_sib = remote(mine, xs.at[t], h_send.at[2], h_recv.at[t], {"tp": sibling})
    h_y.start()

    @pl.when(jnp.logical_not(owner) & (k == 0))
    def _():
        h_x.start()

    @pl.when(jnp.logical_not(owner))
    def _():
        h_sib.start()
        for e in range(2):
            near_copy(d, UP, e).wait_recv()
            spread(near_copy, d, (UP, DOWN), e)

    oy_copies = []
    for e in range(2):
        give_loads[e].wait()
        oy_copies.append(
            remote(
                ostage.at[e], go.at[d * 2 + k, e, y], oy_send.at[0], oy_recv.at[e], {"tp": across}
            )
        )
        oy_copies[e].start()

    def positions_of(shard, index):
        low = order[2 * shard] * half
        high = order[2 * shard + 1] * half
        return jnp.where(index < half, low + index, high + index - half)

    order_load.wait()
    turn_load.wait()
    place = positions_of(k, lax.broadcasted_iota(jnp.int32, (rows, HEAD_SIZE), 0)).astype(F32)
    angle = place * turns[...]
    lane_of = lax.broadcasted_iota(jnp.int32, (rows, HEAD_SIZE), 1)
    trig[0] = jnp.cos(angle)
    sine = jnp.sin(angle)
    trig[1] = jnp.where(lane_of < HEAD_SIZE // 2, -sine, sine)

    for s in range(1, min(2, nd - 1)):
        relay(near_copy, s)

    @pl.when(owner & (k == 0))
    def _():
        h_x.start()

    for e in range(2):
        far_copy(d, UP, e).wait_recv()
        spread(far_copy, d, (UP, DOWN, SIB), e)

    for s in range(2, nd - 1):
        relay(near_copy, s)

    @pl.when(k == 1)
    def _():
        h_x.start()

    def h_wait(slot):
        remote(mine, xs.at[slot], h_send.at[0], h_recv.at[slot], {"tp": across}).wait_recv()

    far = (1 - y) * 2
    h_relay_x = remote(
        xs.at[far + 1], xs.at[far + 1], h_send.at[3], h_recv.at[far + 1], {"ctx": 1 - c}
    )
    h_relay_y = remote(
        xs.at[y * 2], xs.at[y * 2], h_send.at[3], h_recv.at[y * 2], {"tp": across}
    )

    @pl.when(owner)
    def _():
        h_wait(far + 1)
        h_relay_x.start()

    @pl.when(jnp.logical_not(owner))
    def _():
        h_wait(y * 2)
        h_relay_y.start()

    for s in range(1, min(2, nd - 1)):
        relay(far_copy, s)

    for s in range(2, nd - 1):
        relay(far_copy, s)

    for e in range(2):
        keep_loads[e].wait()
        remote(
            ostage.at[e], go.at[d * 2 + k, e, 1 - y], oy_send.at[0], oy_recv.at[e], {"tp": across}
        ).wait_recv()
        spread(o_copy, d, (UP, DOWN, SIB), e)

    @pl.when(owner)
    def _():
        local_load.wait()
        h_wait(sibling)
        h_wait(far)

    @pl.when(jnp.logical_not(owner))
    def _():
        h_wait(y * 2 + 1)
        h_wait(far)
        h_wait(far + 1)

    js = nd // 2
    keeps = (k == c) & (y == c)

    def slot_columns(slot):
        return pl.ds(pl.multiple_of(slot * hc, hc), hc)

    def nearest(i):
        return jnp.where(d < nd // 2, i, nd - 1 - i)

    last = nearest(nd - 1)
    last_j, last_core = last % js, last // js
    ships = k == last_core

    def want_copy(side):
        return remote(
            goal.at[:, slot_columns(last_j * 2 + side)],
            want,
            w_send.at[0],
            w_recv.at[0],
            {"ctx": y, "tp": side * 2 + c},
        )

    keep_want = pltpu.make_async_copy(
        target.at[:, slot_columns(last_j * 2 + y)], want, w_recv.at[0]
    )

    gain_load.wait()
    chunk = min(64, rows)
    per = wide // deep

    def norm_rows(i, carry):
        r = pl.multiple_of(i * chunk, chunk)
        total = jnp.zeros((chunk, 1), F32)
        for j in range(tp):
            v = xs[j, pl.ds(r, chunk), :].astype(F32)
            total = total + jnp.sum(v * v, axis=1, keepdims=True)
        scale = lax.rsqrt(total * (1.0 / (tp * wide)) + 1e-05)
        for j in range(tp):
            for m in range(per):
                v = xs[j, pl.ds(r, chunk), m * deep : (m + 1) * deep].astype(F32)
                g = gains[:, j * wide + m * deep : j * wide + (m + 1) * deep]
                normed[j * per + m, pl.ds(r, chunk), :] = (v * scale * g).astype(BF16)
        return carry

    lax.fori_loop(0, rows // chunk, norm_rows, 0)
    goal_load.wait()

    @pl.when(keeps & ships)
    def _():
        keep_want.start()

    for side in range(2):

        @pl.when(ships & jnp.logical_not(keeps & (side == y)))
        def _():
            want_copy(side).start()

    acc[...] = jnp.zeros_like(acc)

    def project(i, line):
        b = line * nd + i

        @pl.when(jnp.logical_not(owner & (b == b_own)))
        def _():
            ref = ga.at[b, pl.ds(0, deep // 2)]
            remote(ref, ref, a_send.at[1], sib_recv.at[b], {"tp": sibling}).wait_recv()

        acc[...] += jnp.dot(normed[b], ga[b], preferred_element_type=F32)

    def project_step(i, carry):
        @pl.when(i == nd - 1)
        def _():
            relay(near_copy, nd - 1)

        project(nearest(i), c)

        @pl.when(i == nd - 1)
        def _():
            relay(far_copy, nd - 1)

        project(nearest(i), 1 - c)
        return carry

    lax.fori_loop(0, nd, project_step, 0)

    def rotated(v):
        return (v * trig[0] + pltpu.roll(v, HEAD_SIZE // 2, 1) * trig[1]).astype(BF16)

    kv[k, :, 0:HEAD_SIZE] = rotated(acc[:, qcols : qcols + HEAD_SIZE])
    kv[k, :, HEAD_SIZE:] = acc[:, qcols + HEAD_SIZE :].astype(BF16)
    kv_copy = remote(kv.at[k], kv.at[k], kv_send.at[0], kv_recv.at[0], {"tp": sibling})
    kv_copy.start()
    for h in range(n_heads):
        part = slice(h * HEAD_SIZE, (h + 1) * HEAD_SIZE)
        query[h] = rotated(acc[:, part])
    remote(kv.at[1 - k], kv.at[1 - k], kv_send.at[0], kv_recv.at[0], {"tp": sibling}).wait_recv()
    qrows = min(256, rows)
    dims = (((1,), (1,)), ((), ()))
    group = y * 2 + c
    spots = ({"ctx": 1 - c}, {"tp": across})
    x_group, y_group = y * 2 + 1 - c, (1 - y) * 2 + c

    early = n_heads // 2

    def at_copy(h, way, source=group):
        ref = attn.at[source * n_heads + h]
        first = h < early if way == 0 else h >= early
        there = jnp.where(first & (source == group), h, n_heads)
        return remote(ref, ref, at_send.at[0], at_recv.at[there], spots[way])

    def at_arrival(h, source):
        ref = attn.at[source * n_heads + h]
        return remote(ref, ref, at_send.at[0], at_recv.at[h], spots[0])

    def attend_head(h, carry):
        def attend_block(i, inner):
            r = pl.multiple_of(i * qrows, qrows)
            q = query[h, pl.ds(r, qrows), :]
            qpos = positions_of(k, r + lax.broadcasted_iota(jnp.int32, (qrows, rows), 0))
            scores = []
            for n in range(2):
                kpos = positions_of(n, lax.broadcasted_iota(jnp.int32, (qrows, rows), 1))
                sc = lax.dot_general(
                    q, kv[n, :, 0:HEAD_SIZE], dims, preferred_element_type=F32
                ) * (1.0 / HEAD_SIZE**0.5)
                scores.append(jnp.where(qpos >= kpos, sc, -1e30))
            peak = jnp.maximum(
                jnp.max(scores[0], axis=1, keepdims=True),
                jnp.max(scores[1], axis=1, keepdims=True),
            )
            total = jnp.zeros((qrows, 1), F32)
            value = jnp.zeros((qrows, HEAD_SIZE), F32)
            for n in range(2):
                p = jnp.exp(scores[n] - peak)
                total = total + jnp.sum(p, axis=1, keepdims=True)
                value = value + jnp.dot(
                    p.astype(BF16), kv[n, :, HEAD_SIZE:], preferred_element_type=F32
                )
            attn[group * n_heads + h, pl.ds(r, qrows), :] = (value / total).astype(BF16)
            return inner

        lax.fori_loop(0, rows // qrows, attend_block, 0)
        for way in range(2):
            at_copy(h, way).start()
        return carry

    lax.fori_loop(0, n_heads, attend_head, 0)

    for s in range(1, min(2, nd - 1)):
        relay(o_copy, s)

    def at_relay(h, carry):
        at_arrival(h, x_group).wait_recv()
        at_copy(h, 1, x_group).start()
        at_arrival(early + h, y_group).wait_recv()
        at_copy(early + h, 0, y_group).start()
        return carry

    lax.fori_loop(0, early, at_relay, 0)

    for s in range(2, nd - 1):
        relay(o_copy, s)

    rest = attn.at[pl.ds(0, 2 * n_heads)]
    remote(rest, rest, at_send.at[0], at_recv.at[n_heads], spots[0]).wait_recv()

    orow = min(256, rows)

    def made_copy(i, e, rr):
        slot = (i % js) * 2 + y
        where = {"ctx": k, "tp": c * 2 + i // js}
        return remote(
            made.at[i, e, rr], arrived.at[slot, e, rr], r_send.at[0], r_recv.at[slot, e], where
        )

    def stays(i):
        return keeps & (i // js == k)

    def gathered(g, rr):
        return jnp.concatenate([attn[g * n_heads + h, rr, :] for h in range(n_heads)], axis=1)

    tile[...] = jnp.zeros_like(tile)

    def keep_or_send(i, e, rr, value, final):
        @pl.when(jnp.logical_not(stays(i)))
        def _():
            made[i, e, rr, :] = value
            made_copy(i, e, rr).start()

        @pl.when(stays(i))
        def _():
            arrived[(i % js) * 2 + y, e, rr, :] = value

        if not final:
            return
        spot = pl.ds(pl.multiple_of(((i % js) * 2 + y) * hc + e * hq, hq), hq)
        part = pl.ds(pl.multiple_of(e * hq, hq), hq)
        resid = xs[c * 2 + i // js, rr, spot].astype(F32) + value.astype(F32)
        resid = resid - want[rr, part].astype(F32)
        tile[...] += jnp.sum((resid * resid).reshape(orow // 8, 8, hq), axis=0)

    def rows_at(m):
        return pl.ds(pl.multiple_of(m * orow, orow), orow)

    def whole_block(n, carry):
        i = nearest(n)
        for e in range(2):
            o_copy(i, SIB, e, 1 - k).wait_recv()

        def all_rows(m, inner):
            rr = rows_at(m)
            total = jnp.zeros((orow, hc), F32)
            for g in range(tp):
                b = i * 2 + g % 2
                weights = jnp.concatenate([go[b, e, g // 2] for e in range(2)], axis=1)
                term = jnp.dot(gathered(g, rr), weights, preferred_element_type=F32)
                total = total + term.astype(BF16).astype(F32)
            for e in range(2):
                keep_or_send(i, e, rr, total[:, e * hq : (e + 1) * hq].astype(BF16), False)
            return inner

        lax.fori_loop(0, rows // orow, all_rows, 0)
        return carry

    lax.fori_loop(0, nd - 1, whole_block, 0)

    def finish_block(squares, n, carry):
        j = jnp.where(d < nd // 2, n // 4, js - 1 - n // 4)
        e, side = n // 2 % 2, n % 2
        slot = j * 2 + side

        @pl.when(jnp.logical_not(keeps & (side == y)))
        def _():
            remote(
                made.at[0, 0], arrived.at[slot, e], r_send.at[0], r_recv.at[slot, e],
                {"tp": sibling},
            ).wait_recv()

        place = pl.ds(pl.multiple_of(slot * hc + e * hq, hq), hq)
        if not squares:
            out[:, place] = arrived[slot, e]
            return carry

        def finish(m, inner):
            rr = rows_at(m)
            result = arrived[slot, e, rr, :]
            out[rr, place] = result
            resid = mine[rr, place].astype(F32) + result.astype(F32)
            resid = resid - goal[rr, place].astype(F32)
            tile[...] += jnp.sum((resid * resid).reshape(orow // 8, 8, hq), axis=0)
            return inner

        lax.fori_loop(0, rows // orow, finish, 0)
        return carry

    def half_block(e, carry):
        i = nearest(nd - 1)
        relay(o_copy, nd - 1, (e,))

        def terms(core, rr):
            total = jnp.zeros((orow, hq), F32)
            for side in range(2):
                weights = go[i * 2 + core, e, side]
                term = jnp.dot(
                    gathered(2 * side + core, rr), weights, preferred_element_type=F32
                )
                total = total + term.astype(BF16).astype(F32)
            return total

        def own_rows(m, inner):
            acc[rows_at(m), 0:hq] = terms(k, rows_at(m))
            return inner

        lax.fori_loop(0, rows // orow, own_rows, 0)
        o_copy(i, SIB, e, 1 - k).wait_recv()

        def all_rows(m, inner):
            rr = rows_at(m)
            value = (acc[rr, 0:hq] + terms(1 - k, rr)).astype(BF16)
            keep_or_send(i, e, rr, value, True)
            return inner

        lax.fori_loop(0, rows // orow, all_rows, 0)
        return carry

    early_end = jnp.where(ships, 0, 4 * js)
    others_end = 4 * js - 4 * ships.astype(jnp.int32)


    @pl.when(keeps & ships)
    def _():
        keep_want.wait()

    @pl.when(jnp.logical_not(keeps & ships))
    def _():
        remote(want, want, w_send.at[0], w_recv.at[0], {"tp": sibling}).wait_recv()

    def last_step(e, carry):
        half_block(e, carry)

        @pl.when(e == 0)
        def _():
            lax.fori_loop(0, early_end, functools.partial(finish_block, True), 0)

        return carry

    lax.fori_loop(0, 2, last_step, 0)
    lax.fori_loop(early_end, others_end, functools.partial(finish_block, True), 0)

    everyone = plane * nd
    number = d * plane + seat

    def l_copy(n):
        r = everyone - 1 - n
        p = (seat + r) % plane
        z = jnp.where(d < nd // 2, (d + r // plane) % nd, (d + nd - r // plane) % nd)
        return remote(
            sums.at[number], sums.at[number], l_send.at[0], l_recv.at[0],
            {"ctx": p // tp, "tp": p % tp, "dp": z},
        )

    others = sums.at[pl.ds(0, everyone - 1)]
    l_all = remote(others, others, l_send.at[0], l_recv.at[0], {"tp": sibling})
    sums[number] = tile[...]

    def share(n, carry):
        l_copy(n).start()
        return carry

    lax.fori_loop(0, everyone - 1, share, 0)
    lax.fori_loop(others_end, 4 * js, functools.partial(finish_block, False), 0)

    l_all.wait_recv()
    whole = sums[0]
    for b in range(1, everyone):
        whole = whole + sums[b]
    count = plane * nd * rows * wide
    loss[...] = jnp.full(loss.shape, jnp.sum(whole) / count, F32)

    def sent(ref, sem):
        remote(ref, ref, sem, kv_recv.at[0], {"tp": sibling}).wait_send()

    for line_at in range(nd):
        blocks = (line_at + 1) * (line_at < nd - 1) + (nd - line_at) * (line_at > 0)

        @pl.when(d == line_at)
        def _():
            sent(ga.at[pl.ds(0, blocks)], a_send.at[0])
            sent(go.at[pl.ds(0, blocks)], o_send.at[0])

    sent(go.at[pl.ds(0, nd)], o_send.at[1])

    @pl.when(owner)
    def _():
        sent(ga.at[0, pl.ds(0, deep // 2)], x_send.at[0])
        sent(ga.at[pl.ds(0, nd)], a_send.at[1])

    @pl.when(jnp.logical_not(owner))
    def _():
        sent(ga.at[0], x_send.at[0])
        sent(ga.at[pl.ds(0, 2 * nd - 1), pl.ds(0, deep // 2)], a_send.at[1])
        h_sib.wait_send()

    h_y.wait_send()
    h_x.wait_send()
    h_relay_x.wait_send()
    sent(ostage, oy_send.at[0])
    kv_copy.wait_send()
    sent(attn.at[pl.ds(0, 3 * n_heads)], at_send.at[0])

    @pl.when(keeps)
    def _():
        sent(made.at[pl.ds(0, nd - js)], r_send.at[0])

    @pl.when(jnp.logical_not(keeps))
    def _():
        sent(made, r_send.at[0])

    @pl.when(ships & keeps)
    def _():
        sent(want, w_send.at[0])

    @pl.when(ships & jnp.logical_not(keeps))
    def _():
        sent(arrived.at[pl.ds(0, 2)], w_send.at[0])

    l_all.wait_send()


def fused(nd, hidden, target, gain, w_query, w_key, value_matrix, w_out, block_order):
    rows, wide = hidden.shape[1:]
    nb = 2 * nd
    tp = 4
    plane = 2 * tp
    deep, qcols = w_query.shape
    all_cols = qcols + w_key.shape[1] + value_matrix.shape[1]
    orows, ocols = w_out.shape
    hc = ocols // 2
    order_shape = block_order.shape
    half = HEAD_SIZE // 2
    freqs = np.float64(rope_base) ** (-np.arange(half) * 2.0 / HEAD_SIZE)
    freqs = jnp.asarray(np.concatenate([freqs, freqs])[None, :].astype(np.float32))
    heads = qcols // HEAD_SIZE
    js = nd // 2
    anyspace = pl.BlockSpec(memory_space=pltpu.HBM)
    vmem = pl.BlockSpec(memory_space=pltpu.VMEM)
    dma = pltpu.SemaphoreType.DMA
    branch, loss = pl.pallas_call(
        functools.partial(layer, nd),
        out_shape=(
            jax.ShapeDtypeStruct((rows, wide), BF16),
            jax.ShapeDtypeStruct((1, 128), F32),
        ),
        in_specs=[
            anyspace,
            anyspace,
            anyspace,
            anyspace,
            anyspace,
            anyspace,
            anyspace,
            anyspace,
            anyspace,
        ],
        out_specs=(vmem, vmem),
        scratch_shapes=[
            pltpu.VMEM((nb, deep, all_cols), BF16),
            pltpu.VMEM((deep, all_cols), BF16),
            pltpu.VMEM((2 * nd, 2, 2, orows, hc // 2), BF16),
            pltpu.VMEM((2, orows, hc // 2), BF16),
            pltpu.VMEM((rows, wide), BF16),
            pltpu.VMEM((tp, rows, wide), BF16),
            pltpu.VMEM((rows, wide), BF16),
            pltpu.VMEM((nb, rows, deep), BF16),
            pltpu.VMEM((rows, all_cols), F32),
            pltpu.VMEM((2, rows, HEAD_SIZE), F32),
            pltpu.VMEM((heads, rows, HEAD_SIZE), BF16),
            pltpu.VMEM((2, rows, 2 * HEAD_SIZE), BF16),
            pltpu.VMEM((tp * heads, rows, HEAD_SIZE), BF16),
            pltpu.VMEM((nd, 2, rows, hc // 2), BF16),
            pltpu.VMEM((2 * js, 2, rows, hc // 2), BF16),
            pltpu.VMEM((rows, hc), BF16),
            pltpu.VMEM((8, hc // 2), F32),
            pltpu.VMEM((plane * nd, 8, hc // 2), F32),
            pltpu.VMEM((1, tp * wide), F32),
            pltpu.VMEM((1, HEAD_SIZE), F32),
            pltpu.SMEM(order_shape, jnp.int32),
            dma((13,)),
            dma((1,)),
            dma((2,)),
            dma((nb, 2)),
            dma((nb,)),
            dma((1,)),
            dma((2,)),
            dma((2,)),
            dma((nb, 2)),
            dma((4,)),
            dma((tp,)),
            dma((1,)),
            dma((1,)),
            dma((1,)),
            dma((heads + 1,)),
            dma((1,)),
            dma((2 * js, 2)),
            dma((1,)),
            dma((1,)),
            dma((1,)),
            dma((1,)),
        ],
        compiler_params=pltpu.CompilerParams(
            collective_id=1, has_side_effects=True, vmem_limit_bytes=36 * 1024 * 1024
        ),
    )(
        *(
            pltpu.with_memory_space_constraint(v, pltpu.HBM)
            for v in (
                block_order,
                hidden[0],
                target[0],
                gain[None, :],
                freqs,
                w_query,
                w_key,
                value_matrix,
                w_out,
            )
        )
    )
    return (branch[None], loss[0, 0])


def solution(mesh):
    in_specs = (
        P("dp", "ctx", "tp"),
        P("dp", "ctx", "tp"),
        P(),
        P(("ctx", "dp"), "tp"),
        P(("ctx", "dp"), "tp"),
        P(("ctx", "dp"), "tp"),
        P("tp", ("ctx", "dp")),
        P(),
    )
    out_specs = (P("dp", "ctx", "tp"), P())
    sizes = mesh.shape
    fits = sizes["ctx"] == 2 and sizes["tp"] == 4 and sizes["dp"] % 2 == 0
    body = functools.partial(fused, sizes["dp"]) if fits else on_device
    return jax.shard_map(
        body, mesh=mesh, in_specs=in_specs, out_specs=out_specs, check_vma=False
    )
```

```python
import functools

import jax
import numpy as np
import jax.numpy as jnp
from jax import lax
from jax.experimental import pallas as pl
from jax.experimental.pallas import tpu as pltpu
from jax.sharding import PartitionSpec as P

MODEL_WIDTH = 4096
QUERY_HEADS = 16
KEY_VALUE_HEADS = 4
HEAD_SIZE = 128


rope_base = 500000.0


def shifted(value, axis, by):
    peers = lax.axis_size(axis)
    return lax.ppermute(value, axis, [(i, (i + by) % peers) for i in range(peers)])


def positions(order, start, rows, half):
    index = start + lax.iota(jnp.int32, rows)
    block = index // half
    slots = lax.iota(jnp.int32, order.shape[0])
    chosen = jnp.sum(jnp.where(block[:, None] == slots[None, :], order[None, :], 0), axis=1)
    return chosen * half + index % half


def apply_rotary(values, token_places):
    half = values.shape[-1] // 2
    freqs = rope_base ** (-(jnp.arange(half, dtype=jnp.float32) * 2.0) / values.shape[-1])
    angles = token_places.astype(jnp.float32)[:, None] * freqs[None, :]
    cosine = jnp.cos(angles)[:, None, :]
    sine = jnp.sin(angles)[:, None, :]
    first = values[..., :half]
    second = values[..., half:]
    return jnp.concatenate(
        [first * cosine - second * sine, second * cosine + first * sine], axis=-1
    )


def attend(state, query_rows, qpos, piece, kpos):
    peak, total, accum = state
    rows = piece.shape[1]
    local_heads = query_rows.shape[1]
    pair = piece.reshape(2, rows, local_heads, HEAD_SIZE)
    scores = jnp.einsum(
        "qcgd,kcd->cgqk", query_rows, pair[0], preferred_element_type=jnp.float32
    ) * (1.0 / HEAD_SIZE**0.5)
    allowed = (qpos[:, None] >= kpos[None, :])[None, None]
    scores = jnp.where(allowed, scores, -1e30)
    new_peak = jnp.maximum(peak, jnp.max(scores, axis=-1))
    weights = jnp.where(allowed, jnp.exp(scores - new_peak[..., None]), 0.0)
    factor = jnp.exp(peak - new_peak)
    total = total * factor + jnp.sum(weights, axis=-1)
    update = jnp.einsum(
        "cgqk,kcd->qcgd", weights.astype(jnp.bfloat16), pair[1], preferred_element_type=jnp.float32
    )
    accum = accum * jnp.transpose(factor, (2, 0, 1))[..., None] + update
    return (new_peak, total, accum)


def on_device(hidden, target, gain, w_query, w_key, value_matrix, w_out, block_order):
    rows = hidden.shape[1]
    half = rows // 2
    local = hidden[0]
    whole = lax.all_gather(local, "tp", axis=1, tiled=True)
    wide = whole.astype(jnp.float32)
    normed = (
        wide * lax.rsqrt(jnp.mean(wide * wide, axis=1, keepdims=True) + 1e-05) * gain[None, :]
    ).astype(jnp.bfloat16)
    pieces = (
        lax.all_gather(w_query, ("ctx", "dp"), axis=0, tiled=True),
        lax.all_gather(w_key, ("ctx", "dp"), axis=0, tiled=True),
        lax.all_gather(value_matrix, ("ctx", "dp"), axis=0, tiled=True),
    )
    query_rows, key, value_rows = tuple(
        (jnp.dot(normed, piece, preferred_element_type=jnp.float32) for piece in pieces)
    )
    shard = lax.axis_index("ctx")
    qpos = positions(block_order, shard * rows, rows, half)
    local_heads = w_key.shape[1] // HEAD_SIZE
    query_group = QUERY_HEADS // KEY_VALUE_HEADS
    query_rows = (
        apply_rotary(query_rows.reshape(rows, local_heads * query_group, HEAD_SIZE), qpos)
        .astype(jnp.bfloat16)
        .reshape(rows, local_heads, query_group, HEAD_SIZE)
    )
    key = (
        apply_rotary(key.reshape(rows, local_heads, HEAD_SIZE), qpos)
        .astype(jnp.bfloat16)
        .reshape(rows, local_heads * HEAD_SIZE)
    )
    pair = jnp.stack([key, value_rows.astype(jnp.bfloat16)])
    state = (
        jnp.full((local_heads, query_group, rows), -1e30, jnp.float32),
        jnp.zeros((local_heads, query_group, rows), jnp.float32),
        jnp.zeros((rows, local_heads, query_group, HEAD_SIZE), jnp.float32),
    )
    count = lax.axis_size("ctx")
    state = attend(state, query_rows, qpos, pair, qpos)

    def turn(step, carry):
        moved, inner = carry
        moved = shifted(moved, "ctx", 1)
        source = (shard - step) % count
        return (
            moved,
            attend(
                inner, query_rows, qpos, moved, positions(block_order, source * rows, rows, half)
            ),
        )

    moved_end, state = lax.fori_loop(1, count, turn, (pair, state))
    peak, total, accum = state
    attn = (
        (accum / jnp.transpose(total, (2, 0, 1))[..., None])
        .astype(jnp.bfloat16)
        .reshape(rows, local_heads * query_group * HEAD_SIZE)
    )
    terms = jnp.dot(
        attn,
        lax.all_gather(w_out, ("ctx", "dp"), axis=1, tiled=True),
        preferred_element_type=jnp.float32,
    )
    summed = lax.psum_scatter(terms.astype(jnp.bfloat16), "tp", scatter_dimension=1, tiled=True)
    resid = local.astype(jnp.float32) + summed.astype(jnp.float32) - target[0].astype(jnp.float32)
    squares = lax.psum(jnp.sum(resid * resid), ("ctx", "tp", "dp"))
    loss = squares / (lax.axis_size("dp") * lax.axis_size("ctx") * rows * MODEL_WIDTH)
    return (summed[None], loss)


MESH = pl.DeviceIdType.MESH
F32 = jnp.float32
BF16 = jnp.bfloat16


def layer(
    nd,
    order_in,
    hidden,
    target,
    gain,
    freqs,
    w_query,
    w_key,
    value_matrix,
    w_out,
    out,
    loss,
    ga,
    stage,
    go,
    ostage,
    mine,
    xs,
    goal,
    normed,
    acc,
    trig,
    query,
    kv,
    attn,
    made,
    arrived,
    want,
    tile,
    sums,
    gains,
    turns,
    order,
    load_sem,
    x_send,
    a_send,
    a_recv,
    sib_recv,
    oy_send,
    oy_recv,
    o_send,
    o_recv,
    h_send,
    h_recv,
    kv_send,
    kv_recv,
    at_send,
    at_recv,
    r_send,
    r_recv,
    w_send,
    w_recv,
    l_send,
    l_recv,
):
    c, t, d = lax.axis_index("ctx"), lax.axis_index("tp"), lax.axis_index("dp")
    y, k = t // 2, t % 2
    sibling = y * 2 + (1 - k)
    across = (1 - y) * 2 + k
    rows, wide = hidden.shape
    deep, qcols = w_query.shape
    half = rows // 2
    n_heads = qcols // HEAD_SIZE
    tp = 4
    plane = 2 * tp
    owner = c == k
    up, down = d < nd - 1, d > 0

    def load(i, src, dst):
        return pltpu.make_async_copy(src, dst, load_sem.at[i])

    quarter = deep // 4

    def rows_of(piece):
        return pl.ds(pl.multiple_of(piece * quarter, quarter), quarter)

    def weight_loads(dst):
        return (
            load(0, w_query, dst.at[:, pl.ds(0, qcols)]),
            load(1, w_key, dst.at[:, pl.ds(qcols, HEAD_SIZE)]),
            load(2, value_matrix, dst.at[:, pl.ds(qcols + HEAD_SIZE, HEAD_SIZE)]),
        )

    hc = w_out.shape[1] // 2
    hq = hc // 2
    own_loads = weight_loads(ga.at[c * nd + d])
    stage_loads = weight_loads(stage)
    mine_load = load(3, hidden, mine)

    def columns_of(half_of, part):
        return pl.ds(pl.multiple_of(half_of * hc + part * hq, hq), hq)

    keep_loads = [
        load(4 + e, w_out.at[:, columns_of(y, e)], go.at[d * 2 + k, e, y]) for e in range(2)
    ]
    give_loads = [
        load(6 + e, w_out.at[:, columns_of(1 - y, e)], ostage.at[e]) for e in range(2)
    ]
    local_load = load(8, hidden, xs.at[t])
    goal_load = load(9, target, goal)
    gain_load = load(10, gain, gains)
    turn_load = load(11, freqs, turns)
    order_load = load(12, order_in, order)

    @pl.when(owner)
    def _():
        for copy in own_loads:
            copy.start()

    @pl.when(jnp.logical_not(owner))
    def _():
        for copy in stage_loads:
            copy.start()

    mine_load.start()
    order_load.start()
    turn_load.start()
    for copy in give_loads + keep_loads:
        copy.start()

    @pl.when(owner)
    def _():
        local_load.start()

    goal_load.start()
    gain_load.start()

    barrier = pltpu.get_barrier_semaphore()
    seat = c * tp + t
    beside = [{"tp": sibling}]
    for other in range(2):
        beside += [{"ctx": 1 - c, "tp": y * 2 + other}, {"tp": (1 - y) * 2 + other}]
    for where in beside:
        pl.semaphore_signal(barrier, inc=1, device_id=where, device_id_type=MESH)
    for there, step in ((up, 1), (down, -1)):

        @pl.when(there)
        def _():
            pl.semaphore_signal(barrier, inc=1, device_id={"dp": d + step}, device_id_type=MESH)

    near_count = len(beside) + up.astype(jnp.int32) + down.astype(jnp.int32)
    pl.semaphore_wait(barrier, near_count)

    def remote(src, dst, ssem, rsem, where):
        return pltpu.make_async_remote_copy(
            src_ref=src, dst_ref=dst, send_sem=ssem, recv_sem=rsem,
            device_id=where, device_id_type=MESH,
        )

    UP, DOWN, SIB = 0, 1, 2

    def target_of(way):
        return {
            UP: {"dp": jnp.minimum(d + 1, nd - 1)},
            DOWN: {"dp": jnp.maximum(d - 1, 0)},
            SIB: {"tp": sibling},
        }[way]

    def a_copy(line, i, way, e, core=k):
        b = line * nd + i
        ref = ga.at[b, rows_of(2 * core + e)]
        there = sib_recv.at[b] if way == SIB else a_recv.at[b, e]
        return remote(ref, ref, a_send.at[int(way == SIB)], there, target_of(way))

    def o_copy(i, way, e, core=k):
        ref = go.at[i * 2 + core, e]
        there = o_recv.at[core * nd + i, e]
        return remote(ref, ref, o_send.at[int(way == SIB)], there, target_of(way))

    def spread(copy, i, ways, e):
        copy_up = lambda: copy(i, UP, e).start()
        copy_down = lambda: copy(i, DOWN, e).start()
        if UP in ways:
            pl.when(up)(copy_up)
        if DOWN in ways:
            pl.when(down)(copy_down)
        if SIB in ways:
            copy(i, SIB, e).start()

    def relay(copy, s, parts=(0, 1)):
        for e in parts:

            @pl.when(d >= s)
            def _():
                copy(d - s, UP, e).wait_recv()
                spread(copy, d - s, (UP, SIB), e)

            @pl.when(d + s < nd)
            def _():
                copy(d + s, DOWN, e).wait_recv()
                spread(copy, d + s, (DOWN, SIB), e)

    near_copy = functools.partial(a_copy, c)
    far_copy = functools.partial(a_copy, 1 - c)
    b_own = c * nd + d
    half_copies = []
    x_copies = []
    for e in range(2):
        ref = ga.at[b_own, rows_of(2 * (1 - k) + e)]
        half_copies.append(
            remote(
                ref, ref, x_send.at[0], a_recv.at[b_own, e], {"tp": sibling}
            )
        )
        for h in range(2):
            piece = 2 * h + e
            x_copies.append(
                remote(
                    stage.at[rows_of(piece)],
                    ga.at[b_own, rows_of(piece)],
                    x_send.at[0],
                    a_recv.at[b_own, e],
                    {"ctx": 1 - c, "tp": y * 2 + h},
                )
            )

    @pl.when(owner)
    def _():
        for copy in own_loads:
            copy.wait()
        for e in range(2):
            half_copies[e].start()
            spread(near_copy, d, (UP, DOWN), e)
        for e in range(2):
            spread(near_copy, d, (SIB,), e)

    @pl.when(jnp.logical_not(owner))
    def _():
        for copy in stage_loads:
            copy.wait()
        for copy in x_copies:
            copy.start()

    mine_load.wait()
    h_y = remote(mine, xs.at[t], h_send.at[0], h_recv.at[t], {"tp": (1 - y) * 2 + c})
    h_x = remote(mine, xs.at[t], h_send.at[1], h_recv.at[t], {"ctx": 1 - c, "tp": y * 2 + c})
    h_sib = remote(mine, xs.at[t], h_send.at[2], h_recv.at[t], {"tp": sibling})
    h_y.start()

    @pl.when(jnp.logical_not(owner) & (k == 0))
    def _():
        h_x.start()

    @pl.when(jnp.logical_not(owner))
    def _():
        h_sib.start()
        for e in range(2):
            near_copy(d, UP, e).wait_recv()
            spread(near_copy, d, (UP, DOWN), e)

    oy_copies = []
    for e in range(2):
        give_loads[e].wait()
        oy_copies.append(
            remote(
                ostage.at[e], go.at[d * 2 + k, e, y], oy_send.at[0], oy_recv.at[e], {"tp": across}
            )
        )
        oy_copies[e].start()

    def positions_of(shard, index):
        low = order[2 * shard] * half
        high = order[2 * shard + 1] * half
        return jnp.where(index < half, low + index, high + index - half)

    order_load.wait()
    turn_load.wait()
    place = positions_of(k, lax.broadcasted_iota(jnp.int32, (rows, HEAD_SIZE), 0)).astype(F32)
    angle = place * turns[...]
    lane_of = lax.broadcasted_iota(jnp.int32, (rows, HEAD_SIZE), 1)
    trig[0] = jnp.cos(angle)
    sine = jnp.sin(angle)
    trig[1] = jnp.where(lane_of < HEAD_SIZE // 2, -sine, sine)

    for s in range(1, min(2, nd - 1)):
        relay(near_copy, s)

    @pl.when(owner & (k == 0))
    def _():
        h_x.start()

    for e in range(2):
        far_copy(d, UP, e).wait_recv()
        spread(far_copy, d, (UP, DOWN, SIB), e)

    for s in range(2, nd - 1):
        relay(near_copy, s)

    @pl.when(k == 1)
    def _():
        h_x.start()

    def h_wait(slot):
        remote(mine, xs.at[slot], h_send.at[0], h_recv.at[slot], {"tp": across}).wait_recv()

    far = (1 - y) * 2
    h_relay_x = remote(
        xs.at[far + 1], xs.at[far + 1], h_send.at[3], h_recv.at[far + 1], {"ctx": 1 - c}
    )
    h_relay_y = remote(
        xs.at[y * 2], xs.at[y * 2], h_send.at[3], h_recv.at[y * 2], {"tp": across}
    )

    @pl.when(owner)
    def _():
        h_wait(far + 1)
        h_relay_x.start()

    @pl.when(jnp.logical_not(owner))
    def _():
        h_wait(y * 2)
        h_relay_y.start()

    for s in range(1, min(2, nd - 1)):
        relay(far_copy, s)

    for s in range(2, nd - 1):
        relay(far_copy, s)

    for e in range(2):
        keep_loads[e].wait()
        remote(
            ostage.at[e], go.at[d * 2 + k, e, 1 - y], oy_send.at[0], oy_recv.at[e], {"tp": across}
        ).wait_recv()
        spread(o_copy, d, (UP, DOWN, SIB), e)

    @pl.when(owner)
    def _():
        local_load.wait()
        h_wait(sibling)
        h_wait(far)

    @pl.when(jnp.logical_not(owner))
    def _():
        h_wait(y * 2 + 1)
        h_wait(far)
        h_wait(far + 1)

    js = nd // 2
    keeps = (k == c) & (y == c)

    def slot_columns(slot):
        return pl.ds(pl.multiple_of(slot * hc, hc), hc)

    def nearest(i):
        return jnp.where(d < nd // 2, i, nd - 1 - i)

    last = nearest(nd - 1)
    last_j, last_core = last % js, last // js
    ships = k == last_core

    def want_copy(side):
        return remote(
            goal.at[:, slot_columns(last_j * 2 + side)],
            want,
            w_send.at[0],
            w_recv.at[0],
            {"ctx": y, "tp": side * 2 + c},
        )

    keep_want = pltpu.make_async_copy(
        target.at[:, slot_columns(last_j * 2 + y)], want, w_recv.at[0]
    )

    gain_load.wait()
    chunk = min(64, rows)
    per = wide // deep

    def norm_rows(i, carry):
        r = pl.multiple_of(i * chunk, chunk)
        total = jnp.zeros((chunk, 1), F32)
        for j in range(tp):
            v = xs[j, pl.ds(r, chunk), :].astype(F32)
            total = total + jnp.sum(v * v, axis=1, keepdims=True)
        scale = lax.rsqrt(total * (1.0 / (tp * wide)) + 1e-05)
        for j in range(tp):
            for m in range(per):
                v = xs[j, pl.ds(r, chunk), m * deep : (m + 1) * deep].astype(F32)
                g = gains[:, j * wide + m * deep : j * wide + (m + 1) * deep]
                normed[j * per + m, pl.ds(r, chunk), :] = (v * scale * g).astype(BF16)
        return carry

    lax.fori_loop(0, rows // chunk, norm_rows, 0)
    goal_load.wait()

    @pl.when(keeps & ships)
    def _():
        keep_want.start()

    for side in range(2):

        @pl.when(ships & jnp.logical_not(keeps & (side == y)))
        def _():
            want_copy(side).start()

    acc[...] = jnp.zeros_like(acc)

    def project(i, line):
        b = line * nd + i

        @pl.when(jnp.logical_not(owner & (b == b_own)))
        def _():
            ref = ga.at[b, pl.ds(0, deep // 2)]
            remote(ref, ref, a_send.at[1], sib_recv.at[b], {"tp": sibling}).wait_recv()

        acc[...] += jnp.dot(normed[b], ga[b], preferred_element_type=F32)

    def project_step(i, carry):
        @pl.when(i == nd - 1)
        def _():
            relay(near_copy, nd - 1)

        project(nearest(i), c)

        @pl.when(i == nd - 1)
        def _():
            relay(far_copy, nd - 1)

        project(nearest(i), 1 - c)
        return carry

    lax.fori_loop(0, nd, project_step, 0)

    def rotated(v):
        return (v * trig[0] + pltpu.roll(v, HEAD_SIZE // 2, 1) * trig[1]).astype(BF16)

    kv[k, :, 0:HEAD_SIZE] = rotated(acc[:, qcols : qcols + HEAD_SIZE])
    kv[k, :, HEAD_SIZE:] = acc[:, qcols + HEAD_SIZE :].astype(BF16)
    kv_copy = remote(kv.at[k], kv.at[k], kv_send.at[0], kv_recv.at[0], {"tp": sibling})
    kv_copy.start()
    for h in range(n_heads):
        part = slice(h * HEAD_SIZE, (h + 1) * HEAD_SIZE)
        query[h] = rotated(acc[:, part])
    remote(kv.at[1 - k], kv.at[1 - k], kv_send.at[0], kv_recv.at[0], {"tp": sibling}).wait_recv()
    qrows = min(256, rows)
    dims = (((1,), (1,)), ((), ()))
    group = y * 2 + c
    spots = ({"ctx": 1 - c}, {"tp": across})
    x_group, y_group = y * 2 + 1 - c, (1 - y) * 2 + c

    early = n_heads // 2

    def at_copy(h, way, source=group):
        ref = attn.at[source * n_heads + h]
        first = h < early if way == 0 else h >= early
        there = jnp.where(first & (source == group), h, n_heads)
        return remote(ref, ref, at_send.at[0], at_recv.at[there], spots[way])

    def at_arrival(h, source):
        ref = attn.at[source * n_heads + h]
        return remote(ref, ref, at_send.at[0], at_recv.at[h], spots[0])

    def attend_head(h, carry):
        def attend_block(i, inner):
            r = pl.multiple_of(i * qrows, qrows)
            q = query[h, pl.ds(r, qrows), :]
            qpos = positions_of(k, r + lax.broadcasted_iota(jnp.int32, (qrows, rows), 0))
            scores = []
            for n in range(2):
                kpos = positions_of(n, lax.broadcasted_iota(jnp.int32, (qrows, rows), 1))
                sc = lax.dot_general(
                    q, kv[n, :, 0:HEAD_SIZE], dims, preferred_element_type=F32
                ) * (1.0 / HEAD_SIZE**0.5)
                scores.append(jnp.where(qpos >= kpos, sc, -1e30))
            peak = jnp.maximum(
                jnp.max(scores[0], axis=1, keepdims=True),
                jnp.max(scores[1], axis=1, keepdims=True),
            )
            total = jnp.zeros((qrows, 1), F32)
            value = jnp.zeros((qrows, HEAD_SIZE), F32)
            for n in range(2):
                p = jnp.exp(scores[n] - peak)
                total = total + jnp.sum(p, axis=1, keepdims=True)
                value = value + jnp.dot(
                    p.astype(BF16), kv[n, :, HEAD_SIZE:], preferred_element_type=F32
                )
            attn[group * n_heads + h, pl.ds(r, qrows), :] = (value / total).astype(BF16)
            return inner

        lax.fori_loop(0, rows // qrows, attend_block, 0)
        for way in range(2):
            at_copy(h, way).start()
        return carry

    lax.fori_loop(0, n_heads, attend_head, 0)

    for s in range(1, min(2, nd - 1)):
        relay(o_copy, s)

    def at_relay(h, carry):
        at_arrival(h, x_group).wait_recv()
        at_copy(h, 1, x_group).start()
        at_arrival(early + h, y_group).wait_recv()
        at_copy(early + h, 0, y_group).start()
        return carry

    lax.fori_loop(0, early, at_relay, 0)

    for s in range(2, nd - 1):
        relay(o_copy, s)

    rest = attn.at[pl.ds(0, 2 * n_heads)]
    remote(rest, rest, at_send.at[0], at_recv.at[n_heads], spots[0]).wait_recv()

    orow = min(256, rows)

    def made_copy(i, e, rr):
        slot = (i % js) * 2 + y
        where = {"ctx": k, "tp": c * 2 + i // js}
        return remote(
            made.at[i, e, rr], arrived.at[slot, e, rr], r_send.at[0], r_recv.at[slot, e], where
        )

    def stays(i):
        return keeps & (i // js == k)

    def gathered(g, rr):
        return jnp.concatenate([attn[g * n_heads + h, rr, :] for h in range(n_heads)], axis=1)

    tile[...] = jnp.zeros_like(tile)

    def keep_or_send(i, e, rr, value, final):
        @pl.when(jnp.logical_not(stays(i)))
        def _():
            made[i, e, rr, :] = value
            made_copy(i, e, rr).start()

        @pl.when(stays(i))
        def _():
            arrived[(i % js) * 2 + y, e, rr, :] = value

        if not final:
            return
        spot = pl.ds(pl.multiple_of(((i % js) * 2 + y) * hc + e * hq, hq), hq)
        part = pl.ds(pl.multiple_of(e * hq, hq), hq)
        resid = xs[c * 2 + i // js, rr, spot].astype(F32) + value.astype(F32)
        resid = resid - want[rr, part].astype(F32)
        tile[...] += jnp.sum((resid * resid).reshape(orow // 8, 8, hq), axis=0)

    def rows_at(m):
        return pl.ds(pl.multiple_of(m * orow, orow), orow)

    def whole_block(n, carry):
        i = nearest(n)
        for e in range(2):
            o_copy(i, SIB, e, 1 - k).wait_recv()

        def all_rows(m, inner):
            rr = rows_at(m)
            total = jnp.zeros((orow, hc), F32)
            for g in range(tp):
                b = i * 2 + g % 2
                weights = jnp.concatenate([go[b, e, g // 2] for e in range(2)], axis=1)
                term = jnp.dot(gathered(g, rr), weights, preferred_element_type=F32)
                total = total + term.astype(BF16).astype(F32)
            for e in range(2):
                keep_or_send(i, e, rr, total[:, e * hq : (e + 1) * hq].astype(BF16), False)
            return inner

        lax.fori_loop(0, rows // orow, all_rows, 0)
        return carry

    lax.fori_loop(0, nd - 1, whole_block, 0)

    def finish_block(squares, n, carry):
        j = jnp.where(d < nd // 2, n // 4, js - 1 - n // 4)
        e, side = n // 2 % 2, n % 2
        slot = j * 2 + side

        @pl.when(jnp.logical_not(keeps & (side == y)))
        def _():
            remote(
                made.at[0, 0], arrived.at[slot, e], r_send.at[0], r_recv.at[slot, e],
                {"tp": sibling},
            ).wait_recv()

        place = pl.ds(pl.multiple_of(slot * hc + e * hq, hq), hq)
        if not squares:
            out[:, place] = arrived[slot, e]
            return carry

        def finish(m, inner):
            rr = rows_at(m)
            result = arrived[slot, e, rr, :]
            out[rr, place] = result
            resid = mine[rr, place].astype(F32) + result.astype(F32)
            resid = resid - goal[rr, place].astype(F32)
            tile[...] += jnp.sum((resid * resid).reshape(orow // 8, 8, hq), axis=0)
            return inner

        lax.fori_loop(0, rows // orow, finish, 0)
        return carry

    def half_block(e, carry):
        i = nearest(nd - 1)
        relay(o_copy, nd - 1, (e,))

        def terms(core, rr):
            total = jnp.zeros((orow, hq), F32)
            for side in range(2):
                weights = go[i * 2 + core, e, side]
                term = jnp.dot(
                    gathered(2 * side + core, rr), weights, preferred_element_type=F32
                )
                total = total + term.astype(BF16).astype(F32)
            return total

        def own_rows(m, inner):
            acc[rows_at(m), 0:hq] = terms(k, rows_at(m))
            return inner

        lax.fori_loop(0, rows // orow, own_rows, 0)
        o_copy(i, SIB, e, 1 - k).wait_recv()

        def all_rows(m, inner):
            rr = rows_at(m)
            value = (acc[rr, 0:hq] + terms(1 - k, rr)).astype(BF16)
            keep_or_send(i, e, rr, value, True)
            return inner

        lax.fori_loop(0, rows // orow, all_rows, 0)
        return carry

    early_end = jnp.where(ships, 0, 4 * js)
    others_end = 4 * js - 4 * ships.astype(jnp.int32)


    @pl.when(keeps & ships)
    def _():
        keep_want.wait()

    @pl.when(jnp.logical_not(keeps & ships))
    def _():
        remote(want, want, w_send.at[0], w_recv.at[0], {"tp": sibling}).wait_recv()

    def last_step(e, carry):
        half_block(e, carry)

        @pl.when(e == 0)
        def _():
            lax.fori_loop(0, early_end, functools.partial(finish_block, True), 0)

        return carry

    lax.fori_loop(0, 2, last_step, 0)
    lax.fori_loop(early_end, others_end, functools.partial(finish_block, True), 0)

    everyone = plane * nd
    number = d * plane + seat

    def l_copy(n):
        r = everyone - 1 - n
        p = (seat + r) % plane
        z = jnp.where(d < nd // 2, (d + r // plane) % nd, (d + nd - r // plane) % nd)
        return remote(
            sums.at[number], sums.at[number], l_send.at[0], l_recv.at[0],
            {"ctx": p // tp, "tp": p % tp, "dp": z},
        )

    others = sums.at[pl.ds(0, everyone - 1)]
    l_all = remote(others, others, l_send.at[0], l_recv.at[0], {"tp": sibling})
    sums[number] = tile[...]

    def share(n, carry):
        l_copy(n).start()
        return carry

    lax.fori_loop(0, everyone - 1, share, 0)
    lax.fori_loop(others_end, 4 * js, functools.partial(finish_block, False), 0)

    l_all.wait_recv()
    whole = sums[0]
    for b in range(1, everyone):
        whole = whole + sums[b]
    count = plane * nd * rows * wide
    loss[...] = jnp.full(loss.shape, jnp.sum(whole) / count, F32)

    def sent(ref, sem):
        remote(ref, ref, sem, kv_recv.at[0], {"tp": sibling}).wait_send()

    for line_at in range(nd):
        blocks = (line_at + 1) * (line_at < nd - 1) + (nd - line_at) * (line_at > 0)

        @pl.when(d == line_at)
        def _():
            sent(ga.at[pl.ds(0, blocks)], a_send.at[0])
            sent(go.at[pl.ds(0, blocks)], o_send.at[0])

    sent(go.at[pl.ds(0, nd)], o_send.at[1])

    @pl.when(owner)
    def _():
        sent(ga.at[0, pl.ds(0, deep // 2)], x_send.at[0])
        sent(ga.at[pl.ds(0, nd)], a_send.at[1])

    @pl.when(jnp.logical_not(owner))
    def _():
        sent(ga.at[0], x_send.at[0])
        sent(ga.at[pl.ds(0, 2 * nd - 1), pl.ds(0, deep // 2)], a_send.at[1])
        h_sib.wait_send()

    h_y.wait_send()
    h_x.wait_send()
    h_relay_x.wait_send()
    sent(ostage, oy_send.at[0])
    kv_copy.wait_send()
    sent(attn.at[pl.ds(0, 3 * n_heads)], at_send.at[0])

    @pl.when(keeps)
    def _():
        sent(made.at[pl.ds(0, nd - js)], r_send.at[0])

    @pl.when(jnp.logical_not(keeps))
    def _():
        sent(made, r_send.at[0])

    @pl.when(ships & keeps)
    def _():
        sent(want, w_send.at[0])

    @pl.when(ships & jnp.logical_not(keeps))
    def _():
        sent(arrived.at[pl.ds(0, 2)], w_send.at[0])

    l_all.wait_send()


def fused(nd, hidden, target, gain, w_query, w_key, value_matrix, w_out, block_order):
    rows, wide = hidden.shape[1:]
    nb = 2 * nd
    tp = 4
    plane = 2 * tp
    deep, qcols = w_query.shape
    all_cols = qcols + w_key.shape[1] + value_matrix.shape[1]
    orows, ocols = w_out.shape
    hc = ocols // 2
    order_shape = block_order.shape
    half = HEAD_SIZE // 2
    freqs = np.float64(rope_base) ** (-np.arange(half) * 2.0 / HEAD_SIZE)
    freqs = jnp.asarray(np.concatenate([freqs, freqs])[None, :].astype(np.float32))
    heads = qcols // HEAD_SIZE
    js = nd // 2
    anyspace = pl.BlockSpec(memory_space=pltpu.HBM)
    vmem = pl.BlockSpec(memory_space=pltpu.VMEM)
    dma = pltpu.SemaphoreType.DMA
    branch, loss = pl.pallas_call(
        functools.partial(layer, nd),
        out_shape=(
            jax.ShapeDtypeStruct((rows, wide), BF16),
            jax.ShapeDtypeStruct((1, 128), F32),
        ),
        in_specs=[
            anyspace,
            anyspace,
            anyspace,
            anyspace,
            anyspace,
            anyspace,
            anyspace,
            anyspace,
            anyspace,
        ],
        out_specs=(vmem, vmem),
        scratch_shapes=[
            pltpu.VMEM((nb, deep, all_cols), BF16),
            pltpu.VMEM((deep, all_cols), BF16),
            pltpu.VMEM((2 * nd, 2, 2, orows, hc // 2), BF16),
            pltpu.VMEM((2, orows, hc // 2), BF16),
            pltpu.VMEM((rows, wide), BF16),
            pltpu.VMEM((tp, rows, wide), BF16),
            pltpu.VMEM((rows, wide), BF16),
            pltpu.VMEM((nb, rows, deep), BF16),
            pltpu.VMEM((rows, all_cols), F32),
            pltpu.VMEM((2, rows, HEAD_SIZE), F32),
            pltpu.VMEM((heads, rows, HEAD_SIZE), BF16),
            pltpu.VMEM((2, rows, 2 * HEAD_SIZE), BF16),
            pltpu.VMEM((tp * heads, rows, HEAD_SIZE), BF16),
            pltpu.VMEM((nd, 2, rows, hc // 2), BF16),
            pltpu.VMEM((2 * js, 2, rows, hc // 2), BF16),
            pltpu.VMEM((rows, hc), BF16),
            pltpu.VMEM((8, hc // 2), F32),
            pltpu.VMEM((plane * nd, 8, hc // 2), F32),
            pltpu.VMEM((1, tp * wide), F32),
            pltpu.VMEM((1, HEAD_SIZE), F32),
            pltpu.SMEM(order_shape, jnp.int32),
            dma((13,)),
            dma((1,)),
            dma((2,)),
            dma((nb, 2)),
            dma((nb,)),
            dma((1,)),
            dma((2,)),
            dma((2,)),
            dma((nb, 2)),
            dma((4,)),
            dma((tp,)),
            dma((1,)),
            dma((1,)),
            dma((1,)),
            dma((heads + 1,)),
            dma((1,)),
            dma((2 * js, 2)),
            dma((1,)),
            dma((1,)),
            dma((1,)),
            dma((1,)),
        ],
        compiler_params=pltpu.CompilerParams(
            collective_id=1, has_side_effects=True, vmem_limit_bytes=36 * 1024 * 1024
        ),
    )(
        *(
            pltpu.with_memory_space_constraint(v, pltpu.HBM)
            for v in (
                block_order,
                hidden[0],
                target[0],
                gain[None, :],
                freqs,
                w_query,
                w_key,
                value_matrix,
                w_out,
            )
        )
    )
    return (branch[None], loss[0, 0])


def solution(mesh):
    in_specs = (
        P("dp", "ctx", "tp"),
        P("dp", "ctx", "tp"),
        P(),
        P(("ctx", "dp"), "tp"),
        P(("ctx", "dp"), "tp"),
        P(("ctx", "dp"), "tp"),
        P("tp", ("ctx", "dp")),
        P(),
    )
    out_specs = (P("dp", "ctx", "tp"), P())
    sizes = mesh.shape
    fits = sizes["ctx"] == 2 and sizes["tp"] == 4 and sizes["dp"] % 2 == 0
    body = functools.partial(fused, sizes["dp"]) if fits else on_device
    return jax.shard_map(
        body, mesh=mesh, in_specs=in_specs, out_specs=out_specs, check_vma=False
    )
```

```python
import functools

import jax
import numpy as np
import jax.numpy as jnp
from jax import lax
from jax.experimental import pallas as pl
from jax.experimental.pallas import tpu as pltpu
from jax.sharding import PartitionSpec as P

MODEL_WIDTH = 4096
QUERY_HEADS = 16
KEY_VALUE_HEADS = 4
HEAD_SIZE = 128


rope_base = 500000.0


def shifted(value, axis, by):
    peers = lax.axis_size(axis)
    return lax.ppermute(value, axis, [(i, (i + by) % peers) for i in range(peers)])


def positions(order, start, rows, half):
    index = start + lax.iota(jnp.int32, rows)
    block = index // half
    slots = lax.iota(jnp.int32, order.shape[0])
    chosen = jnp.sum(jnp.where(block[:, None] == slots[None, :], order[None, :], 0), axis=1)
    return chosen * half + index % half


def apply_rotary(values, token_places):
    half = values.shape[-1] // 2
    freqs = rope_base ** (-(jnp.arange(half, dtype=jnp.float32) * 2.0) / values.shape[-1])
    angles = token_places.astype(jnp.float32)[:, None] * freqs[None, :]
    cosine = jnp.cos(angles)[:, None, :]
    sine = jnp.sin(angles)[:, None, :]
    first = values[..., :half]
    second = values[..., half:]
    return jnp.concatenate(
        [first * cosine - second * sine, second * cosine + first * sine], axis=-1
    )


def attend(state, query_rows, qpos, piece, kpos):
    peak, total, accum = state
    rows = piece.shape[1]
    local_heads = query_rows.shape[1]
    pair = piece.reshape(2, rows, local_heads, HEAD_SIZE)
    scores = jnp.einsum(
        "qcgd,kcd->cgqk", query_rows, pair[0], preferred_element_type=jnp.float32
    ) * (1.0 / HEAD_SIZE**0.5)
    allowed = (qpos[:, None] >= kpos[None, :])[None, None]
    scores = jnp.where(allowed, scores, -1e30)
    new_peak = jnp.maximum(peak, jnp.max(scores, axis=-1))
    weights = jnp.where(allowed, jnp.exp(scores - new_peak[..., None]), 0.0)
    factor = jnp.exp(peak - new_peak)
    total = total * factor + jnp.sum(weights, axis=-1)
    update = jnp.einsum(
        "cgqk,kcd->qcgd", weights.astype(jnp.bfloat16), pair[1], preferred_element_type=jnp.float32
    )
    accum = accum * jnp.transpose(factor, (2, 0, 1))[..., None] + update
    return (new_peak, total, accum)


def on_device(hidden, target, gain, w_query, w_key, value_matrix, w_out, block_order):
    rows = hidden.shape[1]
    half = rows // 2
    local = hidden[0]
    whole = lax.all_gather(local, "tp", axis=1, tiled=True)
    wide = whole.astype(jnp.float32)
    normed = (
        wide * lax.rsqrt(jnp.mean(wide * wide, axis=1, keepdims=True) + 1e-05) * gain[None, :]
    ).astype(jnp.bfloat16)
    pieces = (
        lax.all_gather(w_query, ("ctx", "dp"), axis=0, tiled=True),
        lax.all_gather(w_key, ("ctx", "dp"), axis=0, tiled=True),
        lax.all_gather(value_matrix, ("ctx", "dp"), axis=0, tiled=True),
    )
    query_rows, key, value_rows = tuple(
        (jnp.dot(normed, piece, preferred_element_type=jnp.float32) for piece in pieces)
    )
    shard = lax.axis_index("ctx")
    qpos = positions(block_order, shard * rows, rows, half)
    local_heads = w_key.shape[1] // HEAD_SIZE
    query_group = QUERY_HEADS // KEY_VALUE_HEADS
    query_rows = (
        apply_rotary(query_rows.reshape(rows, local_heads * query_group, HEAD_SIZE), qpos)
        .astype(jnp.bfloat16)
        .reshape(rows, local_heads, query_group, HEAD_SIZE)
    )
    key = (
        apply_rotary(key.reshape(rows, local_heads, HEAD_SIZE), qpos)
        .astype(jnp.bfloat16)
        .reshape(rows, local_heads * HEAD_SIZE)
    )
    pair = jnp.stack([key, value_rows.astype(jnp.bfloat16)])
    state = (
        jnp.full((local_heads, query_group, rows), -1e30, jnp.float32),
        jnp.zeros((local_heads, query_group, rows), jnp.float32),
        jnp.zeros((rows, local_heads, query_group, HEAD_SIZE), jnp.float32),
    )
    count = lax.axis_size("ctx")
    state = attend(state, query_rows, qpos, pair, qpos)

    def turn(step, carry):
        moved, inner = carry
        moved = shifted(moved, "ctx", 1)
        source = (shard - step) % count
        return (
            moved,
            attend(
                inner, query_rows, qpos, moved, positions(block_order, source * rows, rows, half)
            ),
        )

    moved_end, state = lax.fori_loop(1, count, turn, (pair, state))
    peak, total, accum = state
    attn = (
        (accum / jnp.transpose(total, (2, 0, 1))[..., None])
        .astype(jnp.bfloat16)
        .reshape(rows, local_heads * query_group * HEAD_SIZE)
    )
    terms = jnp.dot(
        attn,
        lax.all_gather(w_out, ("ctx", "dp"), axis=1, tiled=True),
        preferred_element_type=jnp.float32,
    )
    summed = lax.psum_scatter(terms.astype(jnp.bfloat16), "tp", scatter_dimension=1, tiled=True)
    resid = local.astype(jnp.float32) + summed.astype(jnp.float32) - target[0].astype(jnp.float32)
    squares = lax.psum(jnp.sum(resid * resid), ("ctx", "tp", "dp"))
    loss = squares / (lax.axis_size("dp") * lax.axis_size("ctx") * rows * MODEL_WIDTH)
    return (summed[None], loss)


MESH = pl.DeviceIdType.MESH
F32 = jnp.float32
BF16 = jnp.bfloat16


def layer(
    nd,
    order_in,
    hidden,
    target,
    gain,
    freqs,
    w_query,
    w_key,
    value_matrix,
    w_out,
    out,
    loss,
    ga,
    stage,
    go,
    ostage,
    mine,
    xs,
    goal,
    normed,
    acc,
    trig,
    query,
    kv,
    attn,
    made,
    arrived,
    want,
    tile,
    sums,
    gains,
    turns,
    order,
    load_sem,
    x_send,
    a_send,
    a_recv,
    sib_recv,
    oy_send,
    oy_recv,
    o_send,
    o_recv,
    h_send,
    h_recv,
    kv_send,
    kv_recv,
    at_send,
    at_recv,
    r_send,
    r_recv,
    w_send,
    w_recv,
    l_send,
    l_recv,
):
    c, t, d = lax.axis_index("ctx"), lax.axis_index("tp"), lax.axis_index("dp")
    y, k = t // 2, t % 2
    sibling = y * 2 + (1 - k)
    across = (1 - y) * 2 + k
    rows, wide = hidden.shape
    deep, qcols = w_query.shape
    half = rows // 2
    n_heads = qcols // HEAD_SIZE
    tp = 4
    plane = 2 * tp
    owner = c == k
    up, down = d < nd - 1, d > 0

    def load(i, src, dst):
        return pltpu.make_async_copy(src, dst, load_sem.at[i])

    quarter = deep // 4

    def rows_of(piece):
        return pl.ds(pl.multiple_of(piece * quarter, quarter), quarter)

    def weight_loads(dst):
        return (
            load(0, w_query, dst.at[:, pl.ds(0, qcols)]),
            load(1, w_key, dst.at[:, pl.ds(qcols, HEAD_SIZE)]),
            load(2, value_matrix, dst.at[:, pl.ds(qcols + HEAD_SIZE, HEAD_SIZE)]),
        )

    hc = w_out.shape[1] // 2
    hq = hc // 2
    own_loads = weight_loads(ga.at[c * nd + d])
    stage_loads = weight_loads(stage)
    mine_load = load(3, hidden, mine)

    def columns_of(half_of, part):
        return pl.ds(pl.multiple_of(half_of * hc + part * hq, hq), hq)

    keep_loads = [
        load(4 + e, w_out.at[:, columns_of(y, e)], go.at[d * 2 + k, e, y]) for e in range(2)
    ]
    give_loads = [
        load(6 + e, w_out.at[:, columns_of(1 - y, e)], ostage.at[e]) for e in range(2)
    ]
    local_load = load(8, hidden, xs.at[t])
    goal_load = load(9, target, goal)
    gain_load = load(10, gain, gains)
    turn_load = load(11, freqs, turns)
    order_load = load(12, order_in, order)

    @pl.when(owner)
    def _():
        for copy in own_loads:
            copy.start()

    @pl.when(jnp.logical_not(owner))
    def _():
        for copy in stage_loads:
            copy.start()

    mine_load.start()
    order_load.start()
    turn_load.start()
    for copy in give_loads + keep_loads:
        copy.start()

    @pl.when(owner)
    def _():
        local_load.start()

    goal_load.start()
    gain_load.start()

    barrier = pltpu.get_barrier_semaphore()
    seat = c * tp + t
    beside = [{"tp": sibling}]
    for other in range(2):
        beside += [{"ctx": 1 - c, "tp": y * 2 + other}, {"tp": (1 - y) * 2 + other}]
    for where in beside:
        pl.semaphore_signal(barrier, inc=1, device_id=where, device_id_type=MESH)
    for there, step in ((up, 1), (down, -1)):

        @pl.when(there)
        def _():
            pl.semaphore_signal(barrier, inc=1, device_id={"dp": d + step}, device_id_type=MESH)

    near_count = len(beside) + up.astype(jnp.int32) + down.astype(jnp.int32)
    pl.semaphore_wait(barrier, near_count)

    def remote(src, dst, ssem, rsem, where):
        return pltpu.make_async_remote_copy(
            src_ref=src, dst_ref=dst, send_sem=ssem, recv_sem=rsem,
            device_id=where, device_id_type=MESH,
        )

    UP, DOWN, SIB = 0, 1, 2

    def target_of(way):
        return {
            UP: {"dp": jnp.minimum(d + 1, nd - 1)},
            DOWN: {"dp": jnp.maximum(d - 1, 0)},
            SIB: {"tp": sibling},
        }[way]

    def a_copy(line, i, way, e, core=k):
        b = line * nd + i
        ref = ga.at[b, rows_of(2 * core + e)]
        there = sib_recv.at[b] if way == SIB else a_recv.at[b, e]
        return remote(ref, ref, a_send.at[int(way == SIB)], there, target_of(way))

    def o_copy(i, way, e, core=k):
        ref = go.at[i * 2 + core, e]
        there = o_recv.at[core * nd + i, e]
        return remote(ref, ref, o_send.at[int(way == SIB)], there, target_of(way))

    def spread(copy, i, ways, e):
        copy_up = lambda: copy(i, UP, e).start()
        copy_down = lambda: copy(i, DOWN, e).start()
        if UP in ways:
            pl.when(up)(copy_up)
        if DOWN in ways:
            pl.when(down)(copy_down)
        if SIB in ways:
            copy(i, SIB, e).start()

    def relay(copy, s, parts=(0, 1)):
        for e in parts:

            @pl.when(d >= s)
            def _():
                copy(d - s, UP, e).wait_recv()
                spread(copy, d - s, (UP, SIB), e)

            @pl.when(d + s < nd)
            def _():
                copy(d + s, DOWN, e).wait_recv()
                spread(copy, d + s, (DOWN, SIB), e)

    near_copy = functools.partial(a_copy, c)
    far_copy = functools.partial(a_copy, 1 - c)
    b_own = c * nd + d
    half_copies = []
    x_copies = []
    for e in range(2):
        ref = ga.at[b_own, rows_of(2 * (1 - k) + e)]
        half_copies.append(
            remote(
                ref, ref, x_send.at[0], a_recv.at[b_own, e], {"tp": sibling}
            )
        )
        for h in range(2):
            piece = 2 * h + e
            x_copies.append(
                remote(
                    stage.at[rows_of(piece)],
                    ga.at[b_own, rows_of(piece)],
                    x_send.at[0],
                    a_recv.at[b_own, e],
                    {"ctx": 1 - c, "tp": y * 2 + h},
                )
            )

    @pl.when(owner)
    def _():
        for copy in own_loads:
            copy.wait()
        for e in range(2):
            half_copies[e].start()
            spread(near_copy, d, (UP, DOWN), e)

    @pl.when(jnp.logical_not(owner))
    def _():
        for copy in stage_loads:
            copy.wait()
        for copy in x_copies:
            copy.start()

    mine_load.wait()
    h_y = remote(mine, xs.at[t], h_send.at[0], h_recv.at[t], {"tp": (1 - y) * 2 + c})
    h_x = remote(mine, xs.at[t], h_send.at[1], h_recv.at[t], {"ctx": 1 - c, "tp": y * 2 + c})
    h_sib = remote(mine, xs.at[t], h_send.at[2], h_recv.at[t], {"tp": sibling})
    h_y.start()

    @pl.when(jnp.logical_not(owner) & (k == 0))
    def _():
        h_x.start()

    @pl.when(jnp.logical_not(owner))
    def _():
        for e in range(2):
            near_copy(d, UP, e).wait_recv()
            spread(near_copy, d, (UP, DOWN), e)

    oy_copies = []
    for e in range(2):
        give_loads[e].wait()
        oy_copies.append(
            remote(
                ostage.at[e], go.at[d * 2 + k, e, y], oy_send.at[0], oy_recv.at[e], {"tp": across}
            )
        )
        oy_copies[e].start()

    def positions_of(shard, index):
        low = order[2 * shard] * half
        high = order[2 * shard + 1] * half
        return jnp.where(index < half, low + index, high + index - half)

    order_load.wait()
    turn_load.wait()
    place = positions_of(k, lax.broadcasted_iota(jnp.int32, (rows, HEAD_SIZE), 0)).astype(F32)
    angle = place * turns[...]
    lane_of = lax.broadcasted_iota(jnp.int32, (rows, HEAD_SIZE), 1)
    trig[0] = jnp.cos(angle)
    sine = jnp.sin(angle)
    trig[1] = jnp.where(lane_of < HEAD_SIZE // 2, -sine, sine)

    for s in range(1, min(2, nd - 1)):
        relay(near_copy, s)

    @pl.when(owner & (k == 0))
    def _():
        h_x.start()

    @pl.when(owner)
    def _():
        for e in range(2):
            spread(near_copy, d, (SIB,), e)

    @pl.when(jnp.logical_not(owner))
    def _():
        h_sib.start()

    for e in range(2):
        far_copy(d, UP, e).wait_recv()
        spread(far_copy, d, (UP, DOWN, SIB), e)

    for s in range(2, nd - 1):
        relay(near_copy, s)

    @pl.when(k == 1)
    def _():
        h_x.start()

    def h_wait(slot):
        remote(mine, xs.at[slot], h_send.at[0], h_recv.at[slot], {"tp": across}).wait_recv()

    far = (1 - y) * 2
    h_relay_x = remote(
        xs.at[far + 1], xs.at[far + 1], h_send.at[3], h_recv.at[far + 1], {"ctx": 1 - c}
    )
    h_relay_y = remote(
        xs.at[y * 2], xs.at[y * 2], h_send.at[3], h_recv.at[y * 2], {"tp": across}
    )

    @pl.when(owner)
    def _():
        h_wait(far + 1)
        h_relay_x.start()

    @pl.when(jnp.logical_not(owner))
    def _():
        h_wait(y * 2)
        h_relay_y.start()

    for s in range(1, min(2, nd - 1)):
        relay(far_copy, s)

    for s in range(2, nd - 1):
        relay(far_copy, s)

    for e in range(2):
        keep_loads[e].wait()
        remote(
            ostage.at[e], go.at[d * 2 + k, e, 1 - y], oy_send.at[0], oy_recv.at[e], {"tp": across}
        ).wait_recv()
        spread(o_copy, d, (UP, DOWN, SIB), e)

    @pl.when(owner)
    def _():
        local_load.wait()
        h_wait(sibling)
        h_wait(far)

    @pl.when(jnp.logical_not(owner))
    def _():
        h_wait(y * 2 + 1)
        h_wait(far)
        h_wait(far + 1)

    js = nd // 2
    keeps = (k == c) & (y == c)

    def slot_columns(slot):
        return pl.ds(pl.multiple_of(slot * hc, hc), hc)

    def nearest(i):
        return jnp.where(d < nd // 2, i, nd - 1 - i)

    last = nearest(nd - 1)
    ships = k == last // js

    def want_copy(j, side):
        return remote(
            goal.at[:, slot_columns(j * 2 + side)],
            want.at[j],
            w_send.at[0],
            w_recv.at[j],
            {"ctx": y, "tp": side * 2 + c},
        )

    def keep_want(j):
        return pltpu.make_async_copy(
            target.at[:, slot_columns(j * 2 + y)], want.at[j], w_recv.at[j]
        )

    gain_load.wait()
    chunk = min(64, rows)
    per = wide // deep

    def norm_rows(i, carry):
        r = pl.multiple_of(i * chunk, chunk)
        total = jnp.zeros((chunk, 1), F32)
        for j in range(tp):
            v = xs[j, pl.ds(r, chunk), :].astype(F32)
            total = total + jnp.sum(v * v, axis=1, keepdims=True)
        scale = lax.rsqrt(total * (1.0 / (tp * wide)) + 1e-05)
        for j in range(tp):
            for m in range(per):
                v = xs[j, pl.ds(r, chunk), m * deep : (m + 1) * deep].astype(F32)
                g = gains[:, j * wide + m * deep : j * wide + (m + 1) * deep]
                normed[j * per + m, pl.ds(r, chunk), :] = (v * scale * g).astype(BF16)
        return carry

    lax.fori_loop(0, rows // chunk, norm_rows, 0)
    goal_load.wait()

    @pl.when(keeps & ships)
    def _():
        for j in range(js):
            keep_want(j).start()

    for side in range(2):

        @pl.when(ships & jnp.logical_not(keeps & (side == y)))
        def _():
            for j in range(js):
                want_copy(j, side).start()

    acc[...] = jnp.zeros_like(acc)

    def project(i, line):
        b = line * nd + i

        @pl.when(jnp.logical_not(owner & (b == b_own)))
        def _():
            ref = ga.at[b, pl.ds(0, deep // 2)]
            remote(ref, ref, a_send.at[1], sib_recv.at[b], {"tp": sibling}).wait_recv()

        acc[...] += jnp.dot(normed[b], ga[b], preferred_element_type=F32)

    def project_step(i, carry):
        @pl.when(i == nd - 1)
        def _():
            relay(near_copy, nd - 1)

        project(nearest(i), c)

        @pl.when(i == nd - 1)
        def _():
            relay(far_copy, nd - 1)

        project(nearest(i), 1 - c)
        return carry

    lax.fori_loop(0, nd, project_step, 0)

    def rotated(v):
        return (v * trig[0] + pltpu.roll(v, HEAD_SIZE // 2, 1) * trig[1]).astype(BF16)

    kv[k, :, 0:HEAD_SIZE] = rotated(acc[:, qcols : qcols + HEAD_SIZE])
    kv[k, :, HEAD_SIZE:] = acc[:, qcols + HEAD_SIZE :].astype(BF16)
    kv_copy = remote(kv.at[k], kv.at[k], kv_send.at[0], kv_recv.at[0], {"tp": sibling})
    kv_copy.start()
    for h in range(n_heads):
        part = slice(h * HEAD_SIZE, (h + 1) * HEAD_SIZE)
        query[h] = rotated(acc[:, part])
    remote(kv.at[1 - k], kv.at[1 - k], kv_send.at[0], kv_recv.at[0], {"tp": sibling}).wait_recv()
    qrows = min(256, rows)
    dims = (((1,), (1,)), ((), ()))
    group = y * 2 + c
    spots = ({"ctx": 1 - c}, {"tp": across})
    x_group, y_group = y * 2 + 1 - c, (1 - y) * 2 + c

    early = n_heads // 2

    def at_copy(h, way, source=group):
        ref = attn.at[source * n_heads + h]
        first = h < early if way == 0 else h >= early
        there = jnp.where(first & (source == group), h, n_heads)
        return remote(ref, ref, at_send.at[0], at_recv.at[there], spots[way])

    def at_arrival(h, source):
        ref = attn.at[source * n_heads + h]
        return remote(ref, ref, at_send.at[0], at_recv.at[h], spots[0])

    def attend_head(h, carry):
        def attend_block(i, inner):
            r = pl.multiple_of(i * qrows, qrows)
            q = query[h, pl.ds(r, qrows), :]
            qpos = positions_of(k, r + lax.broadcasted_iota(jnp.int32, (qrows, rows), 0))
            scores = []
            for n in range(2):
                kpos = positions_of(n, lax.broadcasted_iota(jnp.int32, (qrows, rows), 1))
                sc = lax.dot_general(
                    q, kv[n, :, 0:HEAD_SIZE], dims, preferred_element_type=F32
                ) * (1.0 / HEAD_SIZE**0.5)
                scores.append(jnp.where(qpos >= kpos, sc, -1e30))
            peak = jnp.maximum(
                jnp.max(scores[0], axis=1, keepdims=True),
                jnp.max(scores[1], axis=1, keepdims=True),
            )
            total = jnp.zeros((qrows, 1), F32)
            value = jnp.zeros((qrows, HEAD_SIZE), F32)
            for n in range(2):
                p = jnp.exp(scores[n] - peak)
                total = total + jnp.sum(p, axis=1, keepdims=True)
                value = value + jnp.dot(
                    p.astype(BF16), kv[n, :, HEAD_SIZE:], preferred_element_type=F32
                )
            attn[group * n_heads + h, pl.ds(r, qrows), :] = (value / total).astype(BF16)
            return inner

        lax.fori_loop(0, rows // qrows, attend_block, 0)
        for way in range(2):
            at_copy(h, way).start()
        return carry

    lax.fori_loop(0, n_heads, attend_head, 0)

    for s in range(1, min(2, nd - 1)):
        relay(o_copy, s)

    def at_relay(h, carry):
        at_arrival(h, x_group).wait_recv()
        at_copy(h, 1, x_group).start()
        at_arrival(early + h, y_group).wait_recv()
        at_copy(early + h, 0, y_group).start()
        return carry

    lax.fori_loop(0, early, at_relay, 0)

    for s in range(2, nd - 1):
        relay(o_copy, s)

    rest = attn.at[pl.ds(0, 2 * n_heads)]
    remote(rest, rest, at_send.at[0], at_recv.at[n_heads], spots[0]).wait_recv()

    orow = min(256, rows)

    def made_copy(i, e, rr):
        slot = (i % js) * 2 + y
        where = {"ctx": k, "tp": c * 2 + i // js}
        return remote(
            made.at[i, e, rr], arrived.at[slot, e, rr], r_send.at[0], r_recv.at[slot, e], where
        )

    def stays(i):
        return keeps & (i // js == k)

    def gathered(g, rr):
        return jnp.concatenate([attn[g * n_heads + h, rr, :] for h in range(n_heads)], axis=1)

    tile[...] = jnp.zeros_like(tile)

    def keep_or_send(i, e, rr, value, final):
        @pl.when(jnp.logical_not(stays(i)))
        def _():
            made[i, e, rr, :] = value
            made_copy(i, e, rr).start()

        @pl.when(stays(i))
        def _():
            arrived[(i % js) * 2 + y, e, rr, :] = value

        if not final:
            return
        spot = pl.ds(pl.multiple_of(((i % js) * 2 + y) * hc + e * hq, hq), hq)
        part = pl.ds(pl.multiple_of(e * hq, hq), hq)
        resid = xs[c * 2 + i // js, rr, spot].astype(F32) + value.astype(F32)
        resid = resid - want[i % js, rr, part].astype(F32)
        tile[...] += jnp.sum((resid * resid).reshape(orow // 8, 8, hq), axis=0)

    def rows_at(m):
        return pl.ds(pl.multiple_of(m * orow, orow), orow)

    def want_wait(i):
        @pl.when(keeps & ships)
        def _():
            keep_want(i % js).wait()

        @pl.when(jnp.logical_not(keeps & ships))
        def _():
            ref = want.at[i % js]
            remote(ref, ref, w_send.at[0], w_recv.at[i % js], {"tp": sibling}).wait_recv()

    others_end = jnp.where(ships, 0, 4 * js)

    def whole_block(final, n, carry):
        i = nearest(n)
        if final:
            want_wait(i)
        for e in range(2):
            o_copy(i, SIB, e, 1 - k).wait_recv()

        def all_rows(m, inner):
            rr = rows_at(m)
            total = jnp.zeros((orow, hc), F32)
            for g in range(tp):
                b = i * 2 + g % 2
                weights = jnp.concatenate([go[b, e, g // 2] for e in range(2)], axis=1)
                term = jnp.dot(gathered(g, rr), weights, preferred_element_type=F32)
                total = total + term.astype(BF16).astype(F32)
            for e in range(2):
                keep_or_send(i, e, rr, total[:, e * hq : (e + 1) * hq].astype(BF16), final)
            return inner

        lax.fori_loop(0, rows // orow, all_rows, 0)
        return carry

    lax.fori_loop(0, js, functools.partial(whole_block, False), 0)
    lax.fori_loop(js, nd - 1, functools.partial(whole_block, True), 0)

    def finish_block(squares, n, carry):
        j = jnp.where(d < nd // 2, n // 4, js - 1 - n // 4)
        e, side = n // 2 % 2, n % 2
        slot = j * 2 + side

        @pl.when(jnp.logical_not(keeps & (side == y)))
        def _():
            remote(
                made.at[0, 0], arrived.at[slot, e], r_send.at[0], r_recv.at[slot, e],
                {"tp": sibling},
            ).wait_recv()

        place = pl.ds(pl.multiple_of(slot * hc + e * hq, hq), hq)
        if not squares:
            out[:, place] = arrived[slot, e]
            return carry

        def finish(m, inner):
            rr = rows_at(m)
            result = arrived[slot, e, rr, :]
            out[rr, place] = result
            resid = mine[rr, place].astype(F32) + result.astype(F32)
            resid = resid - goal[rr, place].astype(F32)
            tile[...] += jnp.sum((resid * resid).reshape(orow // 8, 8, hq), axis=0)
            return inner

        lax.fori_loop(0, rows // orow, finish, 0)
        return carry

    def half_block(e, carry):
        i = nearest(nd - 1)
        relay(o_copy, nd - 1, (e,))

        def terms(core, rr):
            total = jnp.zeros((orow, hq), F32)
            for side in range(2):
                weights = go[i * 2 + core, e, side]
                term = jnp.dot(
                    gathered(2 * side + core, rr), weights, preferred_element_type=F32
                )
                total = total + term.astype(BF16).astype(F32)
            return total

        def own_rows(m, inner):
            acc[rows_at(m), 0:hq] = terms(k, rows_at(m))
            return inner

        lax.fori_loop(0, rows // orow, own_rows, 0)
        o_copy(i, SIB, e, 1 - k).wait_recv()

        def all_rows(m, inner):
            rr = rows_at(m)
            value = (acc[rr, 0:hq] + terms(1 - k, rr)).astype(BF16)
            keep_or_send(i, e, rr, value, True)
            return inner

        lax.fori_loop(0, rows // orow, all_rows, 0)
        return carry


    want_wait(last)

    def last_step(e, carry):
        half_block(e, carry)

        @pl.when(e == 0)
        def _():
            lax.fori_loop(0, others_end, functools.partial(finish_block, True), 0)

        return carry

    lax.fori_loop(0, 2, last_step, 0)
    everyone = plane * nd
    number = d * plane + seat

    def l_copy(n):
        r = everyone - 1 - n
        p = (seat + r) % plane
        z = jnp.where(d < nd // 2, (d + r // plane) % nd, (d + nd - r // plane) % nd)
        return remote(
            sums.at[number], sums.at[number], l_send.at[0], l_recv.at[0],
            {"ctx": p // tp, "tp": p % tp, "dp": z},
        )

    others = sums.at[pl.ds(0, everyone - 1)]
    l_all = remote(others, others, l_send.at[0], l_recv.at[0], {"tp": sibling})
    sums[number] = jnp.sum(tile[...], axis=0, keepdims=True)

    for n in range(everyone - 1):
        l_copy(n).start()
    lax.fori_loop(others_end, 4 * js, functools.partial(finish_block, False), 0)

    l_all.wait_recv()
    whole = sums[0]
    for b in range(1, everyone):
        whole = whole + sums[b]
    count = plane * nd * rows * wide
    loss[...] = jnp.full(loss.shape, jnp.sum(whole) / count, F32)

    def sent(ref, sem):
        remote(ref, ref, sem, kv_recv.at[0], {"tp": sibling}).wait_send()

    for line_at in range(nd):
        blocks = (line_at + 1) * (line_at < nd - 1) + (nd - line_at) * (line_at > 0)

        @pl.when(d == line_at)
        def _():
            sent(ga.at[pl.ds(0, blocks)], a_send.at[0])
            sent(go.at[pl.ds(0, blocks)], o_send.at[0])

    sent(go.at[pl.ds(0, nd)], o_send.at[1])

    @pl.when(owner)
    def _():
        sent(ga.at[0, pl.ds(0, deep // 2)], x_send.at[0])
        sent(ga.at[pl.ds(0, nd)], a_send.at[1])

    @pl.when(jnp.logical_not(owner))
    def _():
        sent(ga.at[0], x_send.at[0])
        sent(ga.at[pl.ds(0, 2 * nd - 1), pl.ds(0, deep // 2)], a_send.at[1])
        h_sib.wait_send()

    h_y.wait_send()
    h_x.wait_send()
    h_relay_x.wait_send()
    sent(ostage, oy_send.at[0])
    kv_copy.wait_send()
    sent(attn.at[pl.ds(0, 3 * n_heads)], at_send.at[0])

    @pl.when(keeps)
    def _():
        sent(made.at[pl.ds(0, nd - js)], r_send.at[0])

    @pl.when(jnp.logical_not(keeps))
    def _():
        sent(made, r_send.at[0])

    @pl.when(ships & keeps)
    def _():
        sent(arrived.at[pl.ds(0, js)], w_send.at[0])

    @pl.when(ships & jnp.logical_not(keeps))
    def _():
        sent(arrived, w_send.at[0])

    l_all.wait_send()


def fused(nd, hidden, target, gain, w_query, w_key, value_matrix, w_out, block_order):
    rows, wide = hidden.shape[1:]
    nb = 2 * nd
    tp = 4
    plane = 2 * tp
    deep, qcols = w_query.shape
    all_cols = qcols + w_key.shape[1] + value_matrix.shape[1]
    orows, ocols = w_out.shape
    hc = ocols // 2
    order_shape = block_order.shape
    half = HEAD_SIZE // 2
    freqs = np.float64(rope_base) ** (-np.arange(half) * 2.0 / HEAD_SIZE)
    freqs = jnp.asarray(np.concatenate([freqs, freqs])[None, :].astype(np.float32))
    heads = qcols // HEAD_SIZE
    js = nd // 2
    anyspace = pl.BlockSpec(memory_space=pltpu.HBM)
    vmem = pl.BlockSpec(memory_space=pltpu.VMEM)
    dma = pltpu.SemaphoreType.DMA
    branch, loss = pl.pallas_call(
        functools.partial(layer, nd),
        out_shape=(
            jax.ShapeDtypeStruct((rows, wide), BF16),
            jax.ShapeDtypeStruct((1, 128), F32),
        ),
        in_specs=[
            anyspace,
            anyspace,
            anyspace,
            anyspace,
            anyspace,
            anyspace,
            anyspace,
            anyspace,
            anyspace,
        ],
        out_specs=(vmem, vmem),
        scratch_shapes=[
            pltpu.VMEM((nb, deep, all_cols), BF16),
            pltpu.VMEM((deep, all_cols), BF16),
            pltpu.VMEM((2 * nd, 2, 2, orows, hc // 2), BF16),
            pltpu.VMEM((2, orows, hc // 2), BF16),
            pltpu.VMEM((rows, wide), BF16),
            pltpu.VMEM((tp, rows, wide), BF16),
            pltpu.VMEM((rows, wide), BF16),
            pltpu.VMEM((nb, rows, deep), BF16),
            pltpu.VMEM((rows, all_cols), F32),
            pltpu.VMEM((2, rows, HEAD_SIZE), F32),
            pltpu.VMEM((heads, rows, HEAD_SIZE), BF16),
            pltpu.VMEM((2, rows, 2 * HEAD_SIZE), BF16),
            pltpu.VMEM((tp * heads, rows, HEAD_SIZE), BF16),
            pltpu.VMEM((nd, 2, rows, hc // 2), BF16),
            pltpu.VMEM((2 * js, 2, rows, hc // 2), BF16),
            pltpu.VMEM((js, rows, hc), BF16),
            pltpu.VMEM((8, hc // 2), F32),
            pltpu.VMEM((plane * nd, 1, hc // 2), F32),
            pltpu.VMEM((1, tp * wide), F32),
            pltpu.VMEM((1, HEAD_SIZE), F32),
            pltpu.SMEM(order_shape, jnp.int32),
            dma((13,)),
            dma((1,)),
            dma((2,)),
            dma((nb, 2)),
            dma((nb,)),
            dma((1,)),
            dma((2,)),
            dma((2,)),
            dma((nb, 2)),
            dma((4,)),
            dma((tp,)),
            dma((1,)),
            dma((1,)),
            dma((1,)),
            dma((heads + 1,)),
            dma((1,)),
            dma((2 * js, 2)),
            dma((1,)),
            dma((js,)),
            dma((1,)),
            dma((1,)),
        ],
        compiler_params=pltpu.CompilerParams(
            collective_id=1, has_side_effects=True, vmem_limit_bytes=36 * 1024 * 1024
        ),
    )(
        *(
            pltpu.with_memory_space_constraint(v, pltpu.HBM)
            for v in (
                block_order,
                hidden[0],
                target[0],
                gain[None, :],
                freqs,
                w_query,
                w_key,
                value_matrix,
                w_out,
            )
        )
    )
    return (branch[None], loss[0, 0])


def solution(mesh):
    in_specs = (
        P("dp", "ctx", "tp"),
        P("dp", "ctx", "tp"),
        P(),
        P(("ctx", "dp"), "tp"),
        P(("ctx", "dp"), "tp"),
        P(("ctx", "dp"), "tp"),
        P("tp", ("ctx", "dp")),
        P(),
    )
    out_specs = (P("dp", "ctx", "tp"), P())
    sizes = mesh.shape
    fits = sizes["ctx"] == 2 and sizes["tp"] == 4 and sizes["dp"] % 2 == 0
    body = functools.partial(fused, sizes["dp"]) if fits else on_device
    return jax.shard_map(
        body, mesh=mesh, in_specs=in_specs, out_specs=out_specs, check_vma=False
    )
```

```python
import functools

import jax
import numpy as np
import jax.numpy as jnp
from jax import lax
from jax.experimental import pallas as pl
from jax.experimental.pallas import tpu as pltpu
from jax.sharding import PartitionSpec as P

MODEL_WIDTH = 4096
QUERY_HEADS = 16
KEY_VALUE_HEADS = 4
HEAD_SIZE = 128


rope_base = 500000.0


def shifted(value, axis, by):
    peers = lax.axis_size(axis)
    return lax.ppermute(value, axis, [(i, (i + by) % peers) for i in range(peers)])


def positions(order, start, rows, half):
    index = start + lax.iota(jnp.int32, rows)
    block = index // half
    slots = lax.iota(jnp.int32, order.shape[0])
    chosen = jnp.sum(jnp.where(block[:, None] == slots[None, :], order[None, :], 0), axis=1)
    return chosen * half + index % half


def apply_rotary(values, token_places):
    half = values.shape[-1] // 2
    freqs = rope_base ** (-(jnp.arange(half, dtype=jnp.float32) * 2.0) / values.shape[-1])
    angles = token_places.astype(jnp.float32)[:, None] * freqs[None, :]
    cosine = jnp.cos(angles)[:, None, :]
    sine = jnp.sin(angles)[:, None, :]
    first = values[..., :half]
    second = values[..., half:]
    return jnp.concatenate(
        [first * cosine - second * sine, second * cosine + first * sine], axis=-1
    )


def attend(state, query_rows, qpos, piece, kpos):
    peak, total, accum = state
    rows = piece.shape[1]
    local_heads = query_rows.shape[1]
    pair = piece.reshape(2, rows, local_heads, HEAD_SIZE)
    scores = jnp.einsum(
        "qcgd,kcd->cgqk", query_rows, pair[0], preferred_element_type=jnp.float32
    ) * (1.0 / HEAD_SIZE**0.5)
    allowed = (qpos[:, None] >= kpos[None, :])[None, None]
    scores = jnp.where(allowed, scores, -1e30)
    new_peak = jnp.maximum(peak, jnp.max(scores, axis=-1))
    weights = jnp.where(allowed, jnp.exp(scores - new_peak[..., None]), 0.0)
    factor = jnp.exp(peak - new_peak)
    total = total * factor + jnp.sum(weights, axis=-1)
    update = jnp.einsum(
        "cgqk,kcd->qcgd", weights.astype(jnp.bfloat16), pair[1], preferred_element_type=jnp.float32
    )
    accum = accum * jnp.transpose(factor, (2, 0, 1))[..., None] + update
    return (new_peak, total, accum)


def on_device(hidden, target, gain, w_query, w_key, value_matrix, w_out, block_order):
    rows = hidden.shape[1]
    half = rows // 2
    local = hidden[0]
    whole = lax.all_gather(local, "tp", axis=1, tiled=True)
    wide = whole.astype(jnp.float32)
    normed = (
        wide * lax.rsqrt(jnp.mean(wide * wide, axis=1, keepdims=True) + 1e-05) * gain[None, :]
    ).astype(jnp.bfloat16)
    pieces = (
        lax.all_gather(w_query, ("ctx", "dp"), axis=0, tiled=True),
        lax.all_gather(w_key, ("ctx", "dp"), axis=0, tiled=True),
        lax.all_gather(value_matrix, ("ctx", "dp"), axis=0, tiled=True),
    )
    query_rows, key, value_rows = tuple(
        (jnp.dot(normed, piece, preferred_element_type=jnp.float32) for piece in pieces)
    )
    shard = lax.axis_index("ctx")
    qpos = positions(block_order, shard * rows, rows, half)
    local_heads = w_key.shape[1] // HEAD_SIZE
    query_group = QUERY_HEADS // KEY_VALUE_HEADS
    query_rows = (
        apply_rotary(query_rows.reshape(rows, local_heads * query_group, HEAD_SIZE), qpos)
        .astype(jnp.bfloat16)
        .reshape(rows, local_heads, query_group, HEAD_SIZE)
    )
    key = (
        apply_rotary(key.reshape(rows, local_heads, HEAD_SIZE), qpos)
        .astype(jnp.bfloat16)
        .reshape(rows, local_heads * HEAD_SIZE)
    )
    pair = jnp.stack([key, value_rows.astype(jnp.bfloat16)])
    state = (
        jnp.full((local_heads, query_group, rows), -1e30, jnp.float32),
        jnp.zeros((local_heads, query_group, rows), jnp.float32),
        jnp.zeros((rows, local_heads, query_group, HEAD_SIZE), jnp.float32),
    )
    count = lax.axis_size("ctx")
    state = attend(state, query_rows, qpos, pair, qpos)

    def turn(step, carry):
        moved, inner = carry
        moved = shifted(moved, "ctx", 1)
        source = (shard - step) % count
        return (
            moved,
            attend(
                inner, query_rows, qpos, moved, positions(block_order, source * rows, rows, half)
            ),
        )

    moved_end, state = lax.fori_loop(1, count, turn, (pair, state))
    peak, total, accum = state
    attn = (
        (accum / jnp.transpose(total, (2, 0, 1))[..., None])
        .astype(jnp.bfloat16)
        .reshape(rows, local_heads * query_group * HEAD_SIZE)
    )
    terms = jnp.dot(
        attn,
        lax.all_gather(w_out, ("ctx", "dp"), axis=1, tiled=True),
        preferred_element_type=jnp.float32,
    )
    summed = lax.psum_scatter(terms.astype(jnp.bfloat16), "tp", scatter_dimension=1, tiled=True)
    resid = local.astype(jnp.float32) + summed.astype(jnp.float32) - target[0].astype(jnp.float32)
    squares = lax.psum(jnp.sum(resid * resid), ("ctx", "tp", "dp"))
    loss = squares / (lax.axis_size("dp") * lax.axis_size("ctx") * rows * MODEL_WIDTH)
    return (summed[None], loss)


MESH = pl.DeviceIdType.MESH
F32 = jnp.float32
BF16 = jnp.bfloat16


def layer(
    nd,
    order_in,
    hidden,
    target,
    gain,
    freqs,
    w_query,
    w_key,
    value_matrix,
    w_out,
    out,
    loss,
    ga,
    stage,
    go,
    ostage,
    mine,
    xs,
    goal,
    normed,
    acc,
    trig,
    query,
    kv,
    attn,
    made,
    arrived,
    want,
    tile,
    sums,
    gains,
    turns,
    order,
    load_sem,
    x_send,
    a_send,
    a_recv,
    sib_recv,
    oy_send,
    oy_recv,
    o_send,
    o_recv,
    h_send,
    h_recv,
    kv_send,
    kv_recv,
    at_send,
    at_recv,
    r_send,
    r_recv,
    w_send,
    w_recv,
    l_send,
    l_recv,
):
    c, t, d = lax.axis_index("ctx"), lax.axis_index("tp"), lax.axis_index("dp")
    y, k = t // 2, t % 2
    sibling = y * 2 + (1 - k)
    across = (1 - y) * 2 + k
    rows, wide = hidden.shape
    deep, qcols = w_query.shape
    half = rows // 2
    n_heads = qcols // HEAD_SIZE
    tp = 4
    plane = 2 * tp
    owner = c == k
    up, down = d < nd - 1, d > 0

    def load(i, src, dst):
        return pltpu.make_async_copy(src, dst, load_sem.at[i])

    quarter = deep // 4

    def rows_of(piece):
        return pl.ds(pl.multiple_of(piece * quarter, quarter), quarter)

    def weight_loads(dst):
        return (
            load(0, w_query, dst.at[:, pl.ds(0, qcols)]),
            load(1, w_key, dst.at[:, pl.ds(qcols, HEAD_SIZE)]),
            load(2, value_matrix, dst.at[:, pl.ds(qcols + HEAD_SIZE, HEAD_SIZE)]),
        )

    hc = w_out.shape[1] // 2
    hq = hc // 2
    own_loads = weight_loads(ga.at[c * nd + d])
    stage_loads = weight_loads(stage)
    mine_load = load(3, hidden, mine)

    def columns_of(half_of, part):
        return pl.ds(pl.multiple_of(half_of * hc + part * hq, hq), hq)

    keep_loads = [
        load(4 + e, w_out.at[:, columns_of(y, e)], go.at[d * 2 + k, e, y]) for e in range(2)
    ]
    give_loads = [
        load(6 + e, w_out.at[:, columns_of(1 - y, e)], ostage.at[e]) for e in range(2)
    ]
    local_load = load(8, hidden, xs.at[t])
    goal_load = load(9, target, goal)
    gain_load = load(10, gain, gains)
    turn_load = load(11, freqs, turns)
    order_load = load(12, order_in, order)

    @pl.when(owner)
    def _():
        for copy in own_loads:
            copy.start()

    @pl.when(jnp.logical_not(owner))
    def _():
        for copy in stage_loads:
            copy.start()

    mine_load.start()
    order_load.start()
    turn_load.start()
    for copy in give_loads + keep_loads:
        copy.start()

    @pl.when(owner)
    def _():
        local_load.start()

    goal_load.start()
    gain_load.start()

    barrier = pltpu.get_barrier_semaphore()
    seat = c * tp + t
    beside = [{"tp": sibling}]
    for other in range(2):
        beside += [{"ctx": 1 - c, "tp": y * 2 + other}, {"tp": (1 - y) * 2 + other}]
    for where in beside:
        pl.semaphore_signal(barrier, inc=1, device_id=where, device_id_type=MESH)
    for there, step in ((up, 1), (down, -1)):

        @pl.when(there)
        def _():
            pl.semaphore_signal(barrier, inc=1, device_id={"dp": d + step}, device_id_type=MESH)

    near_count = len(beside) + up.astype(jnp.int32) + down.astype(jnp.int32)
    pl.semaphore_wait(barrier, near_count)

    def remote(src, dst, ssem, rsem, where):
        return pltpu.make_async_remote_copy(
            src_ref=src, dst_ref=dst, send_sem=ssem, recv_sem=rsem,
            device_id=where, device_id_type=MESH,
        )

    UP, DOWN, SIB = 0, 1, 2

    def target_of(way):
        return {
            UP: {"dp": jnp.minimum(d + 1, nd - 1)},
            DOWN: {"dp": jnp.maximum(d - 1, 0)},
            SIB: {"tp": sibling},
        }[way]

    def a_copy(line, i, way, e, core=k):
        b = line * nd + i
        ref = ga.at[b, rows_of(2 * core + e)]
        there = sib_recv.at[b] if way == SIB else a_recv.at[b, e]
        return remote(ref, ref, a_send.at[int(way == SIB)], there, target_of(way))

    def o_copy(i, way, e, core=k):
        ref = go.at[i * 2 + core, e]
        there = o_recv.at[core * nd + i, e]
        return remote(ref, ref, o_send.at[int(way == SIB)], there, target_of(way))

    def spread(copy, i, ways, e):
        copy_up = lambda: copy(i, UP, e).start()
        copy_down = lambda: copy(i, DOWN, e).start()
        if UP in ways:
            pl.when(up)(copy_up)
        if DOWN in ways:
            pl.when(down)(copy_down)
        if SIB in ways:
            copy(i, SIB, e).start()

    def relay(copy, s, parts=(0, 1)):
        for e in parts:

            @pl.when(d >= s)
            def _():
                copy(d - s, UP, e).wait_recv()
                spread(copy, d - s, (UP, SIB), e)

            @pl.when(d + s < nd)
            def _():
                copy(d + s, DOWN, e).wait_recv()
                spread(copy, d + s, (DOWN, SIB), e)

    near_copy = functools.partial(a_copy, c)
    far_copy = functools.partial(a_copy, 1 - c)
    b_own = c * nd + d
    half_copies = []
    x_copies = []
    for e in range(2):
        ref = ga.at[b_own, rows_of(2 * (1 - k) + e)]
        half_copies.append(
            remote(
                ref, ref, x_send.at[0], a_recv.at[b_own, e], {"tp": sibling}
            )
        )
        for h in range(2):
            piece = 2 * h + e
            x_copies.append(
                remote(
                    stage.at[rows_of(piece)],
                    ga.at[b_own, rows_of(piece)],
                    x_send.at[0],
                    a_recv.at[b_own, e],
                    {"ctx": 1 - c, "tp": y * 2 + h},
                )
            )

    @pl.when(owner)
    def _():
        for copy in own_loads:
            copy.wait()
        for e in range(2):
            half_copies[e].start()
            spread(near_copy, d, (UP, DOWN), e)

    @pl.when(jnp.logical_not(owner))
    def _():
        for copy in stage_loads:
            copy.wait()
        for copy in x_copies:
            copy.start()

    mine_load.wait()
    h_y = remote(mine, xs.at[t], h_send.at[0], h_recv.at[t], {"tp": (1 - y) * 2 + c})
    h_x = remote(mine, xs.at[t], h_send.at[1], h_recv.at[t], {"ctx": 1 - c, "tp": y * 2 + c})
    h_sib = remote(mine, xs.at[t], h_send.at[2], h_recv.at[t], {"tp": sibling})
    h_y.start()

    @pl.when(jnp.logical_not(owner) & (k == 0))
    def _():
        h_x.start()

    @pl.when(jnp.logical_not(owner))
    def _():
        for e in range(2):
            near_copy(d, UP, e).wait_recv()
            spread(near_copy, d, (UP, DOWN), e)

    oy_copies = []
    for e in range(2):
        give_loads[e].wait()
        oy_copies.append(
            remote(
                ostage.at[e], go.at[d * 2 + k, e, y], oy_send.at[0], oy_recv.at[e], {"tp": across}
            )
        )
        oy_copies[e].start()

    def positions_of(shard, index):
        low = order[2 * shard] * half
        high = order[2 * shard + 1] * half
        return jnp.where(index < half, low + index, high + index - half)

    order_load.wait()
    turn_load.wait()
    place = positions_of(k, lax.broadcasted_iota(jnp.int32, (rows, HEAD_SIZE), 0)).astype(F32)
    angle = place * turns[...]
    lane_of = lax.broadcasted_iota(jnp.int32, (rows, HEAD_SIZE), 1)
    trig[0] = jnp.cos(angle)
    sine = jnp.sin(angle)
    trig[1] = jnp.where(lane_of < HEAD_SIZE // 2, -sine, sine)

    for s in range(1, min(2, nd - 1)):
        relay(near_copy, s)

    @pl.when(owner & (k == 0))
    def _():
        h_x.start()

    @pl.when(owner)
    def _():
        for e in range(2):
            spread(near_copy, d, (SIB,), e)

    @pl.when(jnp.logical_not(owner))
    def _():
        h_sib.start()

    for e in range(2):
        far_copy(d, UP, e).wait_recv()
        spread(far_copy, d, (UP, DOWN, SIB), e)

    for s in range(2, nd - 1):
        relay(near_copy, s)

    @pl.when(k == 1)
    def _():
        h_x.start()

    def h_wait(slot):
        remote(mine, xs.at[slot], h_send.at[0], h_recv.at[slot], {"tp": across}).wait_recv()

    far = (1 - y) * 2
    h_relay_x = remote(
        xs.at[far + 1], xs.at[far + 1], h_send.at[3], h_recv.at[far + 1], {"ctx": 1 - c}
    )
    h_relay_y = remote(
        xs.at[y * 2], xs.at[y * 2], h_send.at[3], h_recv.at[y * 2], {"tp": across}
    )

    @pl.when(owner)
    def _():
        h_wait(far + 1)
        h_relay_x.start()

    @pl.when(jnp.logical_not(owner))
    def _():
        h_wait(y * 2)
        h_relay_y.start()

    for s in range(1, min(2, nd - 1)):
        relay(far_copy, s)

    for s in range(2, nd - 1):
        relay(far_copy, s)

    for e in range(2):
        keep_loads[e].wait()
        remote(
            ostage.at[e], go.at[d * 2 + k, e, 1 - y], oy_send.at[0], oy_recv.at[e], {"tp": across}
        ).wait_recv()
        spread(o_copy, d, (UP, DOWN, SIB), e)

    @pl.when(owner)
    def _():
        local_load.wait()
        h_wait(sibling)
        h_wait(far)

    @pl.when(jnp.logical_not(owner))
    def _():
        h_wait(y * 2 + 1)
        h_wait(far)
        h_wait(far + 1)

    js = nd // 2
    keeps = (k == c) & (y == c)

    def slot_columns(slot):
        return pl.ds(pl.multiple_of(slot * hc, hc), hc)

    def nearest(i):
        return jnp.where(d < nd // 2, i, nd - 1 - i)

    last = nearest(nd - 1)
    ships = k == last // js

    def want_copy(j, side):
        return remote(
            goal.at[:, slot_columns(j * 2 + side)],
            want.at[j],
            w_send.at[0],
            w_recv.at[j],
            {"ctx": y, "tp": side * 2 + c},
        )

    def keep_want(j):
        return pltpu.make_async_copy(
            target.at[:, slot_columns(j * 2 + y)], want.at[j], w_recv.at[j]
        )

    gain_load.wait()
    chunk = min(64, rows)
    per = wide // deep

    def norm_rows(i, carry):
        r = pl.multiple_of(i * chunk, chunk)
        total = jnp.zeros((chunk, 1), F32)
        for j in range(tp):
            v = xs[j, pl.ds(r, chunk), :].astype(F32)
            total = total + jnp.sum(v * v, axis=1, keepdims=True)
        scale = lax.rsqrt(total * (1.0 / (tp * wide)) + 1e-05)
        for j in range(tp):
            for m in range(per):
                v = xs[j, pl.ds(r, chunk), m * deep : (m + 1) * deep].astype(F32)
                g = gains[:, j * wide + m * deep : j * wide + (m + 1) * deep]
                normed[j * per + m, pl.ds(r, chunk), :] = (v * scale * g).astype(BF16)
        return carry

    lax.fori_loop(0, rows // chunk, norm_rows, 0)
    goal_load.wait()

    @pl.when(keeps & ships)
    def _():
        for j in range(js):
            keep_want(j).start()

    for side in range(2):

        @pl.when(ships & jnp.logical_not(keeps & (side == y)))
        def _():
            for j in range(js):
                want_copy(j, side).start()

    acc[...] = jnp.zeros_like(acc)

    def project(i, line):
        b = line * nd + i

        @pl.when(jnp.logical_not(owner & (b == b_own)))
        def _():
            ref = ga.at[b, pl.ds(0, deep // 2)]
            remote(ref, ref, a_send.at[1], sib_recv.at[b], {"tp": sibling}).wait_recv()

        acc[...] += jnp.dot(normed[b], ga[b], preferred_element_type=F32)

    def project_step(i, carry):
        @pl.when(i == nd - 1)
        def _():
            relay(near_copy, nd - 1)

        project(nearest(i), c)

        @pl.when(i == nd - 1)
        def _():
            relay(far_copy, nd - 1)

        project(nearest(i), 1 - c)
        return carry

    lax.fori_loop(0, nd, project_step, 0)

    def rotated(v):
        return (v * trig[0] + pltpu.roll(v, HEAD_SIZE // 2, 1) * trig[1]).astype(BF16)

    kv[k, :, 0:HEAD_SIZE] = rotated(acc[:, qcols : qcols + HEAD_SIZE])
    kv[k, :, HEAD_SIZE:] = acc[:, qcols + HEAD_SIZE :].astype(BF16)
    kv_copy = remote(kv.at[k], kv.at[k], kv_send.at[0], kv_recv.at[0], {"tp": sibling})
    kv_copy.start()
    for h in range(n_heads):
        part = slice(h * HEAD_SIZE, (h + 1) * HEAD_SIZE)
        query[h] = rotated(acc[:, part])
    remote(kv.at[1 - k], kv.at[1 - k], kv_send.at[0], kv_recv.at[0], {"tp": sibling}).wait_recv()
    qrows = min(256, rows)
    dims = (((1,), (1,)), ((), ()))
    group = y * 2 + c
    spots = ({"ctx": 1 - c}, {"tp": across})
    x_group, y_group = y * 2 + 1 - c, (1 - y) * 2 + c

    early = n_heads // 2

    def at_copy(h, way, source=group):
        ref = attn.at[source * n_heads + h]
        first = h < early if way == 0 else h >= early
        there = jnp.where(first & (source == group), h, n_heads)
        return remote(ref, ref, at_send.at[0], at_recv.at[there], spots[way])

    def at_arrival(h, source):
        ref = attn.at[source * n_heads + h]
        return remote(ref, ref, at_send.at[0], at_recv.at[h], spots[0])

    def attend_head(h, carry):
        def attend_block(i, inner):
            r = pl.multiple_of(i * qrows, qrows)
            q = query[h, pl.ds(r, qrows), :]
            qpos = positions_of(k, r + lax.broadcasted_iota(jnp.int32, (qrows, rows), 0))
            scores = []
            for n in range(2):
                kpos = positions_of(n, lax.broadcasted_iota(jnp.int32, (qrows, rows), 1))
                sc = lax.dot_general(
                    q, kv[n, :, 0:HEAD_SIZE], dims, preferred_element_type=F32
                ) * (1.0 / HEAD_SIZE**0.5)
                scores.append(jnp.where(qpos >= kpos, sc, -1e30))
            peak = jnp.maximum(
                jnp.max(scores[0], axis=1, keepdims=True),
                jnp.max(scores[1], axis=1, keepdims=True),
            )
            total = jnp.zeros((qrows, 1), F32)
            value = jnp.zeros((qrows, HEAD_SIZE), F32)
            for n in range(2):
                p = jnp.exp(scores[n] - peak)
                total = total + jnp.sum(p, axis=1, keepdims=True)
                value = value + jnp.dot(
                    p.astype(BF16), kv[n, :, HEAD_SIZE:], preferred_element_type=F32
                )
            attn[group * n_heads + h, pl.ds(r, qrows), :] = (value / total).astype(BF16)
            return inner

        lax.fori_loop(0, rows // qrows, attend_block, 0)
        for way in range(2):
            at_copy(h, way).start()
        return carry

    lax.fori_loop(0, n_heads, attend_head, 0)

    for s in range(1, min(2, nd - 1)):
        relay(o_copy, s)

    def at_relay(h, carry):
        at_arrival(h, x_group).wait_recv()
        at_copy(h, 1, x_group).start()
        at_arrival(early + h, y_group).wait_recv()
        at_copy(early + h, 0, y_group).start()
        return carry

    lax.fori_loop(0, early, at_relay, 0)

    for s in range(2, nd - 1):
        relay(o_copy, s)

    rest = attn.at[pl.ds(0, 2 * n_heads)]
    remote(rest, rest, at_send.at[0], at_recv.at[n_heads], spots[0]).wait_recv()

    orow = min(256, rows)

    def made_copy(i, e, rr):
        slot = (i % js) * 2 + y
        where = {"ctx": k, "tp": c * 2 + i // js}
        return remote(
            made.at[i, e, rr], arrived.at[slot, e, rr], r_send.at[0], r_recv.at[slot, e], where
        )

    def stays(i):
        return keeps & (i // js == k)

    def gathered(g, rr):
        return jnp.concatenate([attn[g * n_heads + h, rr, :] for h in range(n_heads)], axis=1)

    tile[...] = jnp.zeros_like(tile)

    def keep_or_send(i, e, rr, value, final):
        @pl.when(jnp.logical_not(stays(i)))
        def _():
            made[i, e, rr, :] = value
            made_copy(i, e, rr).start()

        @pl.when(stays(i))
        def _():
            arrived[(i % js) * 2 + y, e, rr, :] = value

        if not final:
            return
        spot = pl.ds(pl.multiple_of(((i % js) * 2 + y) * hc + e * hq, hq), hq)
        part = pl.ds(pl.multiple_of(e * hq, hq), hq)
        resid = xs[c * 2 + i // js, rr, spot].astype(F32) + value.astype(F32)
        resid = resid - want[i % js, rr, part].astype(F32)
        tile[...] += jnp.sum((resid * resid).reshape(orow // 8, 8, hq), axis=0)

    def rows_at(m):
        return pl.ds(pl.multiple_of(m * orow, orow), orow)

    def want_wait(i):
        @pl.when(keeps & ships)
        def _():
            keep_want(i % js).wait()

        @pl.when(jnp.logical_not(keeps & ships))
        def _():
            ref = want.at[i % js]
            remote(ref, ref, w_send.at[0], w_recv.at[i % js], {"tp": sibling}).wait_recv()

    others_end = jnp.where(ships, 0, 4 * js)

    def whole_block(final, n, carry):
        i = nearest(n)
        if final:
            want_wait(i)
        for e in range(2):
            o_copy(i, SIB, e, 1 - k).wait_recv()

        def all_rows(m, inner):
            rr = rows_at(m)
            total = jnp.zeros((orow, hc), F32)
            for g in range(tp):
                b = i * 2 + g % 2
                weights = jnp.concatenate([go[b, e, g // 2] for e in range(2)], axis=1)
                term = jnp.dot(gathered(g, rr), weights, preferred_element_type=F32)
                total = total + term.astype(BF16).astype(F32)
            for e in range(2):
                keep_or_send(i, e, rr, total[:, e * hq : (e + 1) * hq].astype(BF16), final)
            return inner

        lax.fori_loop(0, rows // orow, all_rows, 0)
        return carry

    lax.fori_loop(0, js, functools.partial(whole_block, False), 0)
    lax.fori_loop(js, nd - 1, functools.partial(whole_block, True), 0)

    def finish_block(squares, n, carry):
        j = jnp.where(d < nd // 2, n // 4, js - 1 - n // 4)
        e, side = n // 2 % 2, n % 2
        slot = j * 2 + side

        @pl.when(jnp.logical_not(keeps & (side == y)))
        def _():
            remote(
                made.at[0, 0], arrived.at[slot, e], r_send.at[0], r_recv.at[slot, e],
                {"tp": sibling},
            ).wait_recv()

        place = pl.ds(pl.multiple_of(slot * hc + e * hq, hq), hq)
        if not squares:
            out[:, place] = arrived[slot, e]
            return carry

        def finish(m, inner):
            rr = rows_at(m)
            result = arrived[slot, e, rr, :]
            out[rr, place] = result
            resid = mine[rr, place].astype(F32) + result.astype(F32)
            resid = resid - goal[rr, place].astype(F32)
            tile[...] += jnp.sum((resid * resid).reshape(orow // 8, 8, hq), axis=0)
            return inner

        lax.fori_loop(0, rows // orow, finish, 0)
        return carry

    def half_block(e, carry):
        i = nearest(nd - 1)
        relay(o_copy, nd - 1, (e,))

        def terms(core, rr):
            total = jnp.zeros((orow, hq), F32)
            for side in range(2):
                weights = go[i * 2 + core, e, side]
                term = jnp.dot(
                    gathered(2 * side + core, rr), weights, preferred_element_type=F32
                )
                total = total + term.astype(BF16).astype(F32)
            return total

        def own_rows(m, inner):
            acc[rows_at(m), 0:hq] = terms(k, rows_at(m))
            return inner

        lax.fori_loop(0, rows // orow, own_rows, 0)
        o_copy(i, SIB, e, 1 - k).wait_recv()

        def all_rows(m, inner):
            rr = rows_at(m)
            value = (acc[rr, 0:hq] + terms(1 - k, rr)).astype(BF16)
            keep_or_send(i, e, rr, value, True)
            return inner

        lax.fori_loop(0, rows // orow, all_rows, 0)
        return carry


    want_wait(last)

    def last_step(e, carry):
        half_block(e, carry)

        @pl.when(e == 0)
        def _():
            lax.fori_loop(0, others_end, functools.partial(finish_block, True), 0)

        return carry

    lax.fori_loop(0, 2, last_step, 0)
    everyone = plane * nd
    number = d * plane + seat

    def l_copy(n):
        r = everyone - 1 - n
        p = (seat + r) % plane
        z = jnp.where(d < nd // 2, (d + r // plane) % nd, (d + nd - r // plane) % nd)
        return remote(
            sums.at[number], sums.at[number], l_send.at[0], l_recv.at[0],
            {"ctx": p // tp, "tp": p % tp, "dp": z},
        )

    others = sums.at[pl.ds(0, everyone - 1)]
    l_all = remote(others, others, l_send.at[0], l_recv.at[0], {"tp": sibling})
    sums[number] = jnp.sum(tile[...], axis=0, keepdims=True)

    for n in range(everyone - 1):
        l_copy(n).start()
    lax.fori_loop(others_end, 4 * js, functools.partial(finish_block, False), 0)

    l_all.wait_recv()
    whole = sums[0]
    for b in range(1, everyone):
        whole = whole + sums[b]
    count = plane * nd * rows * wide
    loss[...] = whole / count

    def sent(ref, sem):
        remote(ref, ref, sem, kv_recv.at[0], {"tp": sibling}).wait_send()

    for line_at in range(nd):
        blocks = (line_at + 1) * (line_at < nd - 1) + (nd - line_at) * (line_at > 0)

        @pl.when(d == line_at)
        def _():
            sent(ga.at[pl.ds(0, blocks)], a_send.at[0])
            sent(go.at[pl.ds(0, blocks)], o_send.at[0])

    sent(go.at[pl.ds(0, nd)], o_send.at[1])

    @pl.when(owner)
    def _():
        sent(ga.at[0, pl.ds(0, deep // 2)], x_send.at[0])
        sent(ga.at[pl.ds(0, nd)], a_send.at[1])

    @pl.when(jnp.logical_not(owner))
    def _():
        sent(ga.at[0], x_send.at[0])
        sent(ga.at[pl.ds(0, 2 * nd - 1), pl.ds(0, deep // 2)], a_send.at[1])
        h_sib.wait_send()

    h_y.wait_send()
    h_x.wait_send()
    h_relay_x.wait_send()
    sent(ostage, oy_send.at[0])
    kv_copy.wait_send()
    sent(attn.at[pl.ds(0, 3 * n_heads)], at_send.at[0])

    @pl.when(keeps)
    def _():
        sent(made.at[pl.ds(0, nd - js)], r_send.at[0])

    @pl.when(jnp.logical_not(keeps))
    def _():
        sent(made, r_send.at[0])

    @pl.when(ships & keeps)
    def _():
        sent(arrived.at[pl.ds(0, js)], w_send.at[0])

    @pl.when(ships & jnp.logical_not(keeps))
    def _():
        sent(arrived, w_send.at[0])

    l_all.wait_send()


def fused(nd, hidden, target, gain, w_query, w_key, value_matrix, w_out, block_order):
    rows, wide = hidden.shape[1:]
    nb = 2 * nd
    tp = 4
    plane = 2 * tp
    deep, qcols = w_query.shape
    all_cols = qcols + w_key.shape[1] + value_matrix.shape[1]
    orows, ocols = w_out.shape
    hc = ocols // 2
    order_shape = block_order.shape
    half = HEAD_SIZE // 2
    freqs = np.float64(rope_base) ** (-np.arange(half) * 2.0 / HEAD_SIZE)
    freqs = jnp.asarray(np.concatenate([freqs, freqs])[None, :].astype(np.float32))
    heads = qcols // HEAD_SIZE
    js = nd // 2
    anyspace = pl.BlockSpec(memory_space=pltpu.HBM)
    vmem = pl.BlockSpec(memory_space=pltpu.VMEM)
    dma = pltpu.SemaphoreType.DMA
    branch, loss = pl.pallas_call(
        functools.partial(layer, nd),
        out_shape=(
            jax.ShapeDtypeStruct((rows, wide), BF16),
            jax.ShapeDtypeStruct((1, hc // 2), F32),
        ),
        in_specs=[
            anyspace,
            anyspace,
            anyspace,
            anyspace,
            anyspace,
            anyspace,
            anyspace,
            anyspace,
            anyspace,
        ],
        out_specs=(vmem, vmem),
        scratch_shapes=[
            pltpu.VMEM((nb, deep, all_cols), BF16),
            pltpu.VMEM((deep, all_cols), BF16),
            pltpu.VMEM((2 * nd, 2, 2, orows, hc // 2), BF16),
            pltpu.VMEM((2, orows, hc // 2), BF16),
            pltpu.VMEM((rows, wide), BF16),
            pltpu.VMEM((tp, rows, wide), BF16),
            pltpu.VMEM((rows, wide), BF16),
            pltpu.VMEM((nb, rows, deep), BF16),
            pltpu.VMEM((rows, all_cols), F32),
            pltpu.VMEM((2, rows, HEAD_SIZE), F32),
            pltpu.VMEM((heads, rows, HEAD_SIZE), BF16),
            pltpu.VMEM((2, rows, 2 * HEAD_SIZE), BF16),
            pltpu.VMEM((tp * heads, rows, HEAD_SIZE), BF16),
            pltpu.VMEM((nd, 2, rows, hc // 2), BF16),
            pltpu.VMEM((2 * js, 2, rows, hc // 2), BF16),
            pltpu.VMEM((js, rows, hc), BF16),
            pltpu.VMEM((8, hc // 2), F32),
            pltpu.VMEM((plane * nd, 1, hc // 2), F32),
            pltpu.VMEM((1, tp * wide), F32),
            pltpu.VMEM((1, HEAD_SIZE), F32),
            pltpu.SMEM(order_shape, jnp.int32),
            dma((13,)),
            dma((1,)),
            dma((2,)),
            dma((nb, 2)),
            dma((nb,)),
            dma((1,)),
            dma((2,)),
            dma((2,)),
            dma((nb, 2)),
            dma((4,)),
            dma((tp,)),
            dma((1,)),
            dma((1,)),
            dma((1,)),
            dma((heads + 1,)),
            dma((1,)),
            dma((2 * js, 2)),
            dma((1,)),
            dma((js,)),
            dma((1,)),
            dma((1,)),
        ],
        compiler_params=pltpu.CompilerParams(
            collective_id=1, has_side_effects=True, vmem_limit_bytes=36 * 1024 * 1024
        ),
    )(
        *(
            pltpu.with_memory_space_constraint(v, pltpu.HBM)
            for v in (
                block_order,
                hidden[0],
                target[0],
                gain[None, :],
                freqs,
                w_query,
                w_key,
                value_matrix,
                w_out,
            )
        )
    )
    return (branch[None], jnp.sum(loss))


def solution(mesh):
    in_specs = (
        P("dp", "ctx", "tp"),
        P("dp", "ctx", "tp"),
        P(),
        P(("ctx", "dp"), "tp"),
        P(("ctx", "dp"), "tp"),
        P(("ctx", "dp"), "tp"),
        P("tp", ("ctx", "dp")),
        P(),
    )
    out_specs = (P("dp", "ctx", "tp"), P())
    sizes = mesh.shape
    fits = sizes["ctx"] == 2 and sizes["tp"] == 4 and sizes["dp"] % 2 == 0
    body = functools.partial(fused, sizes["dp"]) if fits else on_device
    return jax.shard_map(
        body, mesh=mesh, in_specs=in_specs, out_specs=out_specs, check_vma=False
    )
```

```python
import functools

import jax
import numpy as np
import jax.numpy as jnp
from jax import lax
from jax.experimental import pallas as pl
from jax.experimental.pallas import tpu as pltpu
from jax.sharding import PartitionSpec as P

MODEL_WIDTH = 4096
QUERY_HEADS = 16
KEY_VALUE_HEADS = 4
HEAD_SIZE = 128


rope_base = 500000.0


def shifted(value, axis, by):
    peers = lax.axis_size(axis)
    return lax.ppermute(value, axis, [(i, (i + by) % peers) for i in range(peers)])


def positions(order, start, rows, half):
    index = start + lax.iota(jnp.int32, rows)
    block = index // half
    slots = lax.iota(jnp.int32, order.shape[0])
    chosen = jnp.sum(jnp.where(block[:, None] == slots[None, :], order[None, :], 0), axis=1)
    return chosen * half + index % half


def apply_rotary(values, token_places):
    half = values.shape[-1] // 2
    freqs = rope_base ** (-(jnp.arange(half, dtype=jnp.float32) * 2.0) / values.shape[-1])
    angles = token_places.astype(jnp.float32)[:, None] * freqs[None, :]
    cosine = jnp.cos(angles)[:, None, :]
    sine = jnp.sin(angles)[:, None, :]
    first = values[..., :half]
    second = values[..., half:]
    return jnp.concatenate(
        [first * cosine - second * sine, second * cosine + first * sine], axis=-1
    )


def attend(state, query_rows, qpos, piece, kpos):
    peak, total, accum = state
    rows = piece.shape[1]
    local_heads = query_rows.shape[1]
    pair = piece.reshape(2, rows, local_heads, HEAD_SIZE)
    scores = jnp.einsum(
        "qcgd,kcd->cgqk", query_rows, pair[0], preferred_element_type=jnp.float32
    ) * (1.0 / HEAD_SIZE**0.5)
    allowed = (qpos[:, None] >= kpos[None, :])[None, None]
    scores = jnp.where(allowed, scores, -1e30)
    new_peak = jnp.maximum(peak, jnp.max(scores, axis=-1))
    weights = jnp.where(allowed, jnp.exp(scores - new_peak[..., None]), 0.0)
    factor = jnp.exp(peak - new_peak)
    total = total * factor + jnp.sum(weights, axis=-1)
    update = jnp.einsum(
        "cgqk,kcd->qcgd", weights.astype(jnp.bfloat16), pair[1], preferred_element_type=jnp.float32
    )
    accum = accum * jnp.transpose(factor, (2, 0, 1))[..., None] + update
    return (new_peak, total, accum)


def on_device(hidden, target, gain, w_query, w_key, value_matrix, w_out, block_order):
    rows = hidden.shape[1]
    half = rows // 2
    local = hidden[0]
    whole = lax.all_gather(local, "tp", axis=1, tiled=True)
    wide = whole.astype(jnp.float32)
    normed = (
        wide * lax.rsqrt(jnp.mean(wide * wide, axis=1, keepdims=True) + 1e-05) * gain[None, :]
    ).astype(jnp.bfloat16)
    pieces = (
        lax.all_gather(w_query, ("ctx", "dp"), axis=0, tiled=True),
        lax.all_gather(w_key, ("ctx", "dp"), axis=0, tiled=True),
        lax.all_gather(value_matrix, ("ctx", "dp"), axis=0, tiled=True),
    )
    query_rows, key, value_rows = tuple(
        (jnp.dot(normed, piece, preferred_element_type=jnp.float32) for piece in pieces)
    )
    shard = lax.axis_index("ctx")
    qpos = positions(block_order, shard * rows, rows, half)
    local_heads = w_key.shape[1] // HEAD_SIZE
    query_group = QUERY_HEADS // KEY_VALUE_HEADS
    query_rows = (
        apply_rotary(query_rows.reshape(rows, local_heads * query_group, HEAD_SIZE), qpos)
        .astype(jnp.bfloat16)
        .reshape(rows, local_heads, query_group, HEAD_SIZE)
    )
    key = (
        apply_rotary(key.reshape(rows, local_heads, HEAD_SIZE), qpos)
        .astype(jnp.bfloat16)
        .reshape(rows, local_heads * HEAD_SIZE)
    )
    pair = jnp.stack([key, value_rows.astype(jnp.bfloat16)])
    state = (
        jnp.full((local_heads, query_group, rows), -1e30, jnp.float32),
        jnp.zeros((local_heads, query_group, rows), jnp.float32),
        jnp.zeros((rows, local_heads, query_group, HEAD_SIZE), jnp.float32),
    )
    count = lax.axis_size("ctx")
    state = attend(state, query_rows, qpos, pair, qpos)

    def turn(step, carry):
        moved, inner = carry
        moved = shifted(moved, "ctx", 1)
        source = (shard - step) % count
        return (
            moved,
            attend(
                inner, query_rows, qpos, moved, positions(block_order, source * rows, rows, half)
            ),
        )

    moved_end, state = lax.fori_loop(1, count, turn, (pair, state))
    peak, total, accum = state
    attn = (
        (accum / jnp.transpose(total, (2, 0, 1))[..., None])
        .astype(jnp.bfloat16)
        .reshape(rows, local_heads * query_group * HEAD_SIZE)
    )
    terms = jnp.dot(
        attn,
        lax.all_gather(w_out, ("ctx", "dp"), axis=1, tiled=True),
        preferred_element_type=jnp.float32,
    )
    summed = lax.psum_scatter(terms.astype(jnp.bfloat16), "tp", scatter_dimension=1, tiled=True)
    resid = local.astype(jnp.float32) + summed.astype(jnp.float32) - target[0].astype(jnp.float32)
    squares = lax.psum(jnp.sum(resid * resid), ("ctx", "tp", "dp"))
    loss = squares / (lax.axis_size("dp") * lax.axis_size("ctx") * rows * MODEL_WIDTH)
    return (summed[None], loss)


MESH = pl.DeviceIdType.MESH
F32 = jnp.float32
BF16 = jnp.bfloat16


def layer(
    nd,
    order_in,
    hidden,
    target,
    gain,
    freqs,
    w_query,
    w_key,
    value_matrix,
    w_out,
    out,
    loss,
    ga,
    stage,
    go,
    ostage,
    mine,
    xs,
    goal,
    normed,
    acc,
    trig,
    query,
    kv,
    attn,
    made,
    arrived,
    want,
    tile,
    sums,
    gains,
    turns,
    order,
    load_sem,
    x_send,
    a_send,
    a_recv,
    sib_recv,
    oy_send,
    oy_recv,
    o_send,
    o_recv,
    h_send,
    h_recv,
    kv_send,
    kv_recv,
    at_send,
    at_recv,
    r_send,
    r_recv,
    w_send,
    w_recv,
    l_send,
    l_recv,
):
    c, t, d = lax.axis_index("ctx"), lax.axis_index("tp"), lax.axis_index("dp")
    y, k = t // 2, t % 2
    sibling = y * 2 + (1 - k)
    across = (1 - y) * 2 + k
    rows, wide = hidden.shape
    deep, qcols = w_query.shape
    half = rows // 2
    n_heads = qcols // HEAD_SIZE
    tp = 4
    plane = 2 * tp
    owner = c == k
    up, down = d < nd - 1, d > 0

    def load(i, src, dst):
        return pltpu.make_async_copy(src, dst, load_sem.at[i])

    quarter = deep // 4

    def rows_of(piece):
        return pl.ds(pl.multiple_of(piece * quarter, quarter), quarter)

    def weight_loads(dst):
        return (
            load(0, w_query, dst.at[:, pl.ds(0, qcols)]),
            load(1, w_key, dst.at[:, pl.ds(qcols, HEAD_SIZE)]),
            load(2, value_matrix, dst.at[:, pl.ds(qcols + HEAD_SIZE, HEAD_SIZE)]),
        )

    hc = w_out.shape[1] // 2
    hq = hc // 2
    own_loads = weight_loads(ga.at[c * nd + d])
    stage_loads = weight_loads(stage)
    mine_load = load(3, hidden, mine)

    def columns_of(half_of, part):
        return pl.ds(pl.multiple_of(half_of * hc + part * hq, hq), hq)

    keep_loads = [
        load(4 + e, w_out.at[:, columns_of(y, e)], go.at[d * 2 + k, e, y]) for e in range(2)
    ]
    give_loads = [
        load(6 + e, w_out.at[:, columns_of(1 - y, e)], ostage.at[e]) for e in range(2)
    ]
    local_load = load(8, hidden, xs.at[t])
    goal_load = load(9, target, goal)
    gain_load = load(10, gain, gains)
    turn_load = load(11, freqs, turns)
    order_load = load(12, order_in, order)

    @pl.when(owner)
    def _():
        for copy in own_loads:
            copy.start()

    @pl.when(jnp.logical_not(owner))
    def _():
        for copy in stage_loads:
            copy.start()

    mine_load.start()
    order_load.start()
    turn_load.start()
    for copy in give_loads + keep_loads:
        copy.start()

    @pl.when(owner)
    def _():
        local_load.start()

    goal_load.start()
    gain_load.start()

    barrier = pltpu.get_barrier_semaphore()
    seat = c * tp + t
    beside = [{"tp": sibling}]
    for other in range(2):
        beside += [{"ctx": 1 - c, "tp": y * 2 + other}, {"tp": (1 - y) * 2 + other}]
    for where in beside:
        pl.semaphore_signal(barrier, inc=1, device_id=where, device_id_type=MESH)
    for there, step in ((up, 1), (down, -1)):

        @pl.when(there)
        def _():
            pl.semaphore_signal(barrier, inc=1, device_id={"dp": d + step}, device_id_type=MESH)

    near_count = len(beside) + up.astype(jnp.int32) + down.astype(jnp.int32)
    pl.semaphore_wait(barrier, near_count)

    def remote(src, dst, ssem, rsem, where):
        return pltpu.make_async_remote_copy(
            src_ref=src, dst_ref=dst, send_sem=ssem, recv_sem=rsem,
            device_id=where, device_id_type=MESH,
        )

    UP, DOWN, SIB = 0, 1, 2

    def target_of(way):
        return {
            UP: {"dp": jnp.minimum(d + 1, nd - 1)},
            DOWN: {"dp": jnp.maximum(d - 1, 0)},
            SIB: {"tp": sibling},
        }[way]

    def a_copy(line, i, way, e, core=k):
        b = line * nd + i
        ref = ga.at[b, rows_of(2 * core + e)]
        there = sib_recv.at[b] if way == SIB else a_recv.at[b, e]
        return remote(ref, ref, a_send.at[int(way == SIB)], there, target_of(way))

    def o_copy(i, way, e, core=k):
        ref = go.at[i * 2 + core, e]
        there = o_recv.at[core * nd + i, e]
        return remote(ref, ref, o_send.at[int(way == SIB)], there, target_of(way))

    def spread(copy, i, ways, e):
        copy_up = lambda: copy(i, UP, e).start()
        copy_down = lambda: copy(i, DOWN, e).start()
        if UP in ways:
            pl.when(up)(copy_up)
        if DOWN in ways:
            pl.when(down)(copy_down)
        if SIB in ways:
            copy(i, SIB, e).start()

    def relay(copy, s, parts=(0, 1)):
        for e in parts:

            @pl.when(d >= s)
            def _():
                copy(d - s, UP, e).wait_recv()
                spread(copy, d - s, (UP, SIB), e)

            @pl.when(d + s < nd)
            def _():
                copy(d + s, DOWN, e).wait_recv()
                spread(copy, d + s, (DOWN, SIB), e)

    near_copy = functools.partial(a_copy, c)
    far_copy = functools.partial(a_copy, 1 - c)
    b_own = c * nd + d
    half_copies = []
    x_copies = []
    for e in range(2):
        ref = ga.at[b_own, rows_of(2 * (1 - k) + e)]
        half_copies.append(
            remote(
                ref, ref, x_send.at[0], a_recv.at[b_own, e], {"tp": sibling}
            )
        )
        for h in range(2):
            piece = 2 * h + e
            x_copies.append(
                remote(
                    stage.at[rows_of(piece)],
                    ga.at[b_own, rows_of(piece)],
                    x_send.at[0],
                    a_recv.at[b_own, e],
                    {"ctx": 1 - c, "tp": y * 2 + h},
                )
            )

    @pl.when(owner)
    def _():
        for copy in own_loads:
            copy.wait()
        for e in range(2):
            half_copies[e].start()
            spread(near_copy, d, (UP, DOWN), e)

    @pl.when(jnp.logical_not(owner))
    def _():
        for copy in stage_loads:
            copy.wait()
        for copy in x_copies:
            copy.start()

    mine_load.wait()
    h_y = remote(mine, xs.at[t], h_send.at[0], h_recv.at[t], {"tp": (1 - y) * 2 + c})
    h_x = remote(mine, xs.at[t], h_send.at[0], h_recv.at[t], {"ctx": 1 - c, "tp": y * 2 + c})
    h_sib = remote(mine, xs.at[t], h_send.at[0], h_recv.at[t], {"tp": sibling})
    h_y.start()

    @pl.when(jnp.logical_not(owner) & (k == 0))
    def _():
        h_x.start()

    @pl.when(jnp.logical_not(owner))
    def _():
        for e in range(2):
            near_copy(d, UP, e).wait_recv()
            spread(near_copy, d, (UP, DOWN), e)

    oy_copies = []
    for e in range(2):
        give_loads[e].wait()
        oy_copies.append(
            remote(
                ostage.at[e], go.at[d * 2 + k, e, y], oy_send.at[0], oy_recv.at[e], {"tp": across}
            )
        )
        oy_copies[e].start()

    def positions_of(shard, index):
        low = order[2 * shard] * half
        high = order[2 * shard + 1] * half
        return jnp.where(index < half, low + index, high + index - half)

    order_load.wait()
    turn_load.wait()
    place = positions_of(k, lax.broadcasted_iota(jnp.int32, (rows, HEAD_SIZE), 0)).astype(F32)
    angle = place * turns[...]
    lane_of = lax.broadcasted_iota(jnp.int32, (rows, HEAD_SIZE), 1)
    trig[0] = jnp.cos(angle)
    sine = jnp.sin(angle)
    trig[1] = jnp.where(lane_of < HEAD_SIZE // 2, -sine, sine)

    for s in range(1, min(2, nd - 1)):
        relay(near_copy, s)

    @pl.when(owner & (k == 0))
    def _():
        h_x.start()

    @pl.when(owner)
    def _():
        for e in range(2):
            spread(near_copy, d, (SIB,), e)

    @pl.when(jnp.logical_not(owner))
    def _():
        h_sib.start()

    for e in range(2):
        far_copy(d, UP, e).wait_recv()
        spread(far_copy, d, (UP, DOWN, SIB), e)

    for s in range(2, nd - 1):
        relay(near_copy, s)

    @pl.when(k == 1)
    def _():
        h_x.start()

    def h_wait(slot):
        remote(mine, xs.at[slot], h_send.at[0], h_recv.at[slot], {"tp": across}).wait_recv()

    far = (1 - y) * 2
    h_relay_x = remote(
        xs.at[far + 1], xs.at[far + 1], h_send.at[0], h_recv.at[far + 1], {"ctx": 1 - c}
    )
    h_relay_y = remote(
        xs.at[y * 2], xs.at[y * 2], h_send.at[0], h_recv.at[y * 2], {"tp": across}
    )

    @pl.when(owner)
    def _():
        h_wait(far + 1)
        h_relay_x.start()

    @pl.when(jnp.logical_not(owner))
    def _():
        h_wait(y * 2)
        h_relay_y.start()

    for s in range(1, min(2, nd - 1)):
        relay(far_copy, s)

    for s in range(2, nd - 1):
        relay(far_copy, s)

    for e in range(2):
        keep_loads[e].wait()
        remote(
            ostage.at[e], go.at[d * 2 + k, e, 1 - y], oy_send.at[0], oy_recv.at[e], {"tp": across}
        ).wait_recv()
        spread(o_copy, d, (UP, DOWN, SIB), e)

    @pl.when(owner)
    def _():
        local_load.wait()
        h_wait(sibling)
        h_wait(far)

    @pl.when(jnp.logical_not(owner))
    def _():
        h_wait(y * 2 + 1)
        h_wait(far)
        h_wait(far + 1)

    js = nd // 2
    keeps = (k == c) & (y == c)

    def slot_columns(slot):
        return pl.ds(pl.multiple_of(slot * hc, hc), hc)

    def nearest(i):
        return jnp.where(d < nd // 2, i, nd - 1 - i)

    last = nearest(nd - 1)
    ships = k == last // js

    def want_copy(j, side):
        return remote(
            goal.at[:, slot_columns(j * 2 + side)],
            want.at[j],
            w_send.at[0],
            w_recv.at[j],
            {"ctx": y, "tp": side * 2 + c},
        )

    def keep_want(j):
        return pltpu.make_async_copy(
            target.at[:, slot_columns(j * 2 + y)], want.at[j], w_recv.at[j]
        )

    gain_load.wait()
    chunk = min(64, rows)
    per = wide // deep

    def norm_rows(i, carry):
        r = pl.multiple_of(i * chunk, chunk)
        total = jnp.zeros((chunk, 1), F32)
        for j in range(tp):
            v = xs[j, pl.ds(r, chunk), :].astype(F32)
            total = total + jnp.sum(v * v, axis=1, keepdims=True)
        scale = lax.rsqrt(total * (1.0 / (tp * wide)) + 1e-05)
        for j in range(tp):
            for m in range(per):
                v = xs[j, pl.ds(r, chunk), m * deep : (m + 1) * deep].astype(F32)
                g = gains[:, j * wide + m * deep : j * wide + (m + 1) * deep]
                normed[j * per + m, pl.ds(r, chunk), :] = (v * scale * g).astype(BF16)
        return carry

    lax.fori_loop(0, rows // chunk, norm_rows, 0)
    goal_load.wait()

    @pl.when(keeps & ships)
    def _():
        for j in range(js):
            keep_want(j).start()

    for side in range(2):

        @pl.when(ships & jnp.logical_not(keeps & (side == y)))
        def _():
            for j in range(js):
                want_copy(j, side).start()

    acc[...] = jnp.zeros_like(acc)

    def project(i, line):
        b = line * nd + i

        @pl.when(jnp.logical_not(owner & (b == b_own)))
        def _():
            ref = ga.at[b, pl.ds(0, deep // 2)]
            remote(ref, ref, a_send.at[1], sib_recv.at[b], {"tp": sibling}).wait_recv()

        acc[...] += jnp.dot(normed[b], ga[b], preferred_element_type=F32)

    def project_step(i, carry):
        @pl.when(i == nd - 1)
        def _():
            relay(near_copy, nd - 1)

        project(nearest(i), c)

        @pl.when(i == nd - 1)
        def _():
            relay(far_copy, nd - 1)

        project(nearest(i), 1 - c)
        return carry

    lax.fori_loop(0, nd, project_step, 0)

    def rotated(v):
        return (v * trig[0] + pltpu.roll(v, HEAD_SIZE // 2, 1) * trig[1]).astype(BF16)

    kv[k, :, 0:HEAD_SIZE] = rotated(acc[:, qcols : qcols + HEAD_SIZE])
    kv[k, :, HEAD_SIZE:] = acc[:, qcols + HEAD_SIZE :].astype(BF16)
    kv_copy = remote(kv.at[k], kv.at[k], kv_send.at[0], kv_recv.at[0], {"tp": sibling})
    kv_copy.start()
    for h in range(n_heads):
        part = slice(h * HEAD_SIZE, (h + 1) * HEAD_SIZE)
        query[h] = rotated(acc[:, part])
    remote(kv.at[1 - k], kv.at[1 - k], kv_send.at[0], kv_recv.at[0], {"tp": sibling}).wait_recv()
    qrows = min(256, rows)
    dims = (((1,), (1,)), ((), ()))
    group = y * 2 + c
    spots = ({"ctx": 1 - c}, {"tp": across})
    x_group, y_group = y * 2 + 1 - c, (1 - y) * 2 + c

    early = n_heads // 2

    def at_copy(h, way, source=group):
        ref = attn.at[source * n_heads + h]
        first = h < early if way == 0 else h >= early
        there = jnp.where(first & (source == group), h, n_heads)
        return remote(ref, ref, at_send.at[0], at_recv.at[there], spots[way])

    def at_arrival(h, source):
        ref = attn.at[source * n_heads + h]
        return remote(ref, ref, at_send.at[0], at_recv.at[h], spots[0])

    def attend_head(h, carry):
        def attend_block(i, inner):
            r = pl.multiple_of(i * qrows, qrows)
            q = query[h, pl.ds(r, qrows), :]
            qpos = positions_of(k, r + lax.broadcasted_iota(jnp.int32, (qrows, rows), 0))
            scores = []
            for n in range(2):
                kpos = positions_of(n, lax.broadcasted_iota(jnp.int32, (qrows, rows), 1))
                sc = lax.dot_general(
                    q, kv[n, :, 0:HEAD_SIZE], dims, preferred_element_type=F32
                ) * (1.0 / HEAD_SIZE**0.5)
                scores.append(jnp.where(qpos >= kpos, sc, -1e30))
            peak = jnp.maximum(
                jnp.max(scores[0], axis=1, keepdims=True),
                jnp.max(scores[1], axis=1, keepdims=True),
            )
            total = jnp.zeros((qrows, 1), F32)
            value = jnp.zeros((qrows, HEAD_SIZE), F32)
            for n in range(2):
                p = jnp.exp(scores[n] - peak)
                total = total + jnp.sum(p, axis=1, keepdims=True)
                value = value + jnp.dot(
                    p.astype(BF16), kv[n, :, HEAD_SIZE:], preferred_element_type=F32
                )
            attn[group * n_heads + h, pl.ds(r, qrows), :] = (value / total).astype(BF16)
            return inner

        lax.fori_loop(0, rows // qrows, attend_block, 0)
        for way in range(2):
            at_copy(h, way).start()
        return carry

    lax.fori_loop(0, n_heads, attend_head, 0)

    for s in range(1, min(2, nd - 1)):
        relay(o_copy, s)

    def at_relay(h, carry):
        at_arrival(h, x_group).wait_recv()
        at_copy(h, 1, x_group).start()
        at_arrival(early + h, y_group).wait_recv()
        at_copy(early + h, 0, y_group).start()
        return carry

    lax.fori_loop(0, early, at_relay, 0)

    for s in range(2, nd - 1):
        relay(o_copy, s)

    rest = attn.at[pl.ds(0, 2 * n_heads)]
    remote(rest, rest, at_send.at[0], at_recv.at[n_heads], spots[0]).wait_recv()

    orow = min(256, rows)

    def made_copy(i, e, rr):
        slot = (i % js) * 2 + y
        where = {"ctx": k, "tp": c * 2 + i // js}
        return remote(
            made.at[i, e, rr], arrived.at[slot, e, rr], r_send.at[0], r_recv.at[slot, e], where
        )

    def stays(i):
        return keeps & (i // js == k)

    def gathered(g, rr):
        return jnp.concatenate([attn[g * n_heads + h, rr, :] for h in range(n_heads)], axis=1)

    tile[...] = jnp.zeros_like(tile)

    def keep_or_send(i, e, rr, value, final):
        @pl.when(jnp.logical_not(stays(i)))
        def _():
            made[i, e, rr, :] = value
            made_copy(i, e, rr).start()

        @pl.when(stays(i))
        def _():
            arrived[(i % js) * 2 + y, e, rr, :] = value

        if not final:
            return
        spot = pl.ds(pl.multiple_of(((i % js) * 2 + y) * hc + e * hq, hq), hq)
        part = pl.ds(pl.multiple_of(e * hq, hq), hq)
        resid = xs[c * 2 + i // js, rr, spot].astype(F32) + value.astype(F32)
        resid = resid - want[i % js, rr, part].astype(F32)
        tile[...] += jnp.sum((resid * resid).reshape(orow // 8, 8, hq), axis=0)

    def rows_at(m):
        return pl.ds(pl.multiple_of(m * orow, orow), orow)

    def want_wait(i):
        @pl.when(keeps & ships)
        def _():
            keep_want(i % js).wait()

        @pl.when(jnp.logical_not(keeps & ships))
        def _():
            ref = want.at[i % js]
            remote(ref, ref, w_send.at[0], w_recv.at[i % js], {"tp": sibling}).wait_recv()

    others_end = jnp.where(ships, 0, 4 * js)

    def whole_block(final, n, carry):
        i = nearest(n)
        if final:
            want_wait(i)
        for e in range(2):
            o_copy(i, SIB, e, 1 - k).wait_recv()

        def all_rows(m, inner):
            rr = rows_at(m)
            total = jnp.zeros((orow, hc), F32)
            for g in range(tp):
                b = i * 2 + g % 2
                weights = jnp.concatenate([go[b, e, g // 2] for e in range(2)], axis=1)
                term = jnp.dot(gathered(g, rr), weights, preferred_element_type=F32)
                total = total + term.astype(BF16).astype(F32)
            for e in range(2):
                keep_or_send(i, e, rr, total[:, e * hq : (e + 1) * hq].astype(BF16), final)
            return inner

        lax.fori_loop(0, rows // orow, all_rows, 0)
        return carry

    lax.fori_loop(0, js, functools.partial(whole_block, False), 0)
    lax.fori_loop(js, nd - 1, functools.partial(whole_block, True), 0)

    def finish_block(squares, n, carry):
        j = jnp.where(d < nd // 2, n // 4, js - 1 - n // 4)
        e, side = n // 2 % 2, n % 2
        slot = j * 2 + side

        @pl.when(jnp.logical_not(keeps & (side == y)))
        def _():
            remote(
                made.at[0, 0], arrived.at[slot, e], r_send.at[0], r_recv.at[slot, e],
                {"tp": sibling},
            ).wait_recv()

        place = pl.ds(pl.multiple_of(slot * hc + e * hq, hq), hq)
        if not squares:
            out[:, place] = arrived[slot, e]
            return carry

        def finish(m, inner):
            rr = rows_at(m)
            result = arrived[slot, e, rr, :]
            out[rr, place] = result
            resid = mine[rr, place].astype(F32) + result.astype(F32)
            resid = resid - goal[rr, place].astype(F32)
            tile[...] += jnp.sum((resid * resid).reshape(orow // 8, 8, hq), axis=0)
            return inner

        lax.fori_loop(0, rows // orow, finish, 0)
        return carry

    def half_block(e, carry):
        i = nearest(nd - 1)
        relay(o_copy, nd - 1, (e,))

        def terms(core, rr):
            total = jnp.zeros((orow, hq), F32)
            for side in range(2):
                weights = go[i * 2 + core, e, side]
                term = jnp.dot(
                    gathered(2 * side + core, rr), weights, preferred_element_type=F32
                )
                total = total + term.astype(BF16).astype(F32)
            return total

        def own_rows(m, inner):
            acc[rows_at(m), 0:hq] = terms(k, rows_at(m))
            return inner

        lax.fori_loop(0, rows // orow, own_rows, 0)
        o_copy(i, SIB, e, 1 - k).wait_recv()

        def all_rows(m, inner):
            rr = rows_at(m)
            value = (acc[rr, 0:hq] + terms(1 - k, rr)).astype(BF16)
            keep_or_send(i, e, rr, value, True)
            return inner

        lax.fori_loop(0, rows // orow, all_rows, 0)
        return carry


    want_wait(last)

    def last_step(e, carry):
        half_block(e, carry)

        @pl.when(e == 0)
        def _():
            lax.fori_loop(0, others_end, functools.partial(finish_block, True), 0)

        return carry

    lax.fori_loop(0, 2, last_step, 0)
    everyone = plane * nd
    number = d * plane + seat

    def l_copy(n):
        r = everyone - 1 - n
        p = (seat + r) % plane
        z = jnp.where(d < nd // 2, (d + r // plane) % nd, (d + nd - r // plane) % nd)
        return remote(
            sums.at[number], sums.at[number], l_send.at[0], l_recv.at[0],
            {"ctx": p // tp, "tp": p % tp, "dp": z},
        )

    others = sums.at[pl.ds(0, everyone - 1)]
    l_all = remote(others, others, l_send.at[0], l_recv.at[0], {"tp": sibling})
    sums[number] = jnp.sum(tile[...], axis=0, keepdims=True)

    for n in range(everyone - 1):
        l_copy(n).start()
    lax.fori_loop(others_end, 4 * js, functools.partial(finish_block, False), 0)

    def sent(ref, sem):
        remote(ref, ref, sem, kv_recv.at[0], {"tp": sibling}).wait_send()

    for line_at in range(nd):
        blocks = (line_at + 1) * (line_at < nd - 1) + (nd - line_at) * (line_at > 0)

        @pl.when(d == line_at)
        def _():
            sent(ga.at[pl.ds(0, blocks)], a_send.at[0])
            sent(go.at[pl.ds(0, blocks)], o_send.at[0])

    sent(go.at[pl.ds(0, nd)], o_send.at[1])

    @pl.when(owner)
    def _():
        sent(ga.at[0, pl.ds(0, deep // 2)], x_send.at[0])
        sent(ga.at[pl.ds(0, nd)], a_send.at[1])
        sent(xs.at[pl.ds(0, 3)], h_send.at[0])

    @pl.when(jnp.logical_not(owner))
    def _():
        sent(ga.at[0], x_send.at[0])
        sent(ga.at[pl.ds(0, 2 * nd - 1), pl.ds(0, deep // 2)], a_send.at[1])
        sent(xs, h_send.at[0])

    sent(ostage, oy_send.at[0])
    kv_copy.wait_send()
    sent(attn.at[pl.ds(0, 3 * n_heads)], at_send.at[0])

    @pl.when(keeps)
    def _():
        sent(made.at[pl.ds(0, nd - js)], r_send.at[0])

    @pl.when(jnp.logical_not(keeps))
    def _():
        sent(made, r_send.at[0])

    @pl.when(ships & keeps)
    def _():
        sent(arrived.at[pl.ds(0, js)], w_send.at[0])

    @pl.when(ships & jnp.logical_not(keeps))
    def _():
        sent(arrived, w_send.at[0])

    l_all.wait_send()

    l_all.wait_recv()
    whole = sums[0]
    for b in range(1, everyone):
        whole = whole + sums[b]
    count = plane * nd * rows * wide
    loss[...] = whole / count


def fused(nd, hidden, target, gain, w_query, w_key, value_matrix, w_out, block_order):
    rows, wide = hidden.shape[1:]
    nb = 2 * nd
    tp = 4
    plane = 2 * tp
    deep, qcols = w_query.shape
    all_cols = qcols + w_key.shape[1] + value_matrix.shape[1]
    orows, ocols = w_out.shape
    hc = ocols // 2
    order_shape = block_order.shape
    half = HEAD_SIZE // 2
    freqs = np.float64(rope_base) ** (-np.arange(half) * 2.0 / HEAD_SIZE)
    freqs = jnp.asarray(np.concatenate([freqs, freqs])[None, :].astype(np.float32))
    heads = qcols // HEAD_SIZE
    js = nd // 2
    anyspace = pl.BlockSpec(memory_space=pltpu.HBM)
    vmem = pl.BlockSpec(memory_space=pltpu.VMEM)
    dma = pltpu.SemaphoreType.DMA
    branch, loss = pl.pallas_call(
        functools.partial(layer, nd),
        out_shape=(
            jax.ShapeDtypeStruct((rows, wide), BF16),
            jax.ShapeDtypeStruct((1, hc // 2), F32),
        ),
        in_specs=[
            anyspace,
            anyspace,
            anyspace,
            anyspace,
            anyspace,
            anyspace,
            anyspace,
            anyspace,
            anyspace,
        ],
        out_specs=(vmem, vmem),
        scratch_shapes=[
            pltpu.VMEM((nb, deep, all_cols), BF16),
            pltpu.VMEM((deep, all_cols), BF16),
            pltpu.VMEM((2 * nd, 2, 2, orows, hc // 2), BF16),
            pltpu.VMEM((2, orows, hc // 2), BF16),
            pltpu.VMEM((rows, wide), BF16),
            pltpu.VMEM((tp, rows, wide), BF16),
            pltpu.VMEM((rows, wide), BF16),
            pltpu.VMEM((nb, rows, deep), BF16),
            pltpu.VMEM((rows, all_cols), F32),
            pltpu.VMEM((2, rows, HEAD_SIZE), F32),
            pltpu.VMEM((heads, rows, HEAD_SIZE), BF16),
            pltpu.VMEM((2, rows, 2 * HEAD_SIZE), BF16),
            pltpu.VMEM((tp * heads, rows, HEAD_SIZE), BF16),
            pltpu.VMEM((nd, 2, rows, hc // 2), BF16),
            pltpu.VMEM((2 * js, 2, rows, hc // 2), BF16),
            pltpu.VMEM((js, rows, hc), BF16),
            pltpu.VMEM((8, hc // 2), F32),
            pltpu.VMEM((plane * nd, 1, hc // 2), F32),
            pltpu.VMEM((1, tp * wide), F32),
            pltpu.VMEM((1, HEAD_SIZE), F32),
            pltpu.SMEM(order_shape, jnp.int32),
            dma((13,)),
            dma((1,)),
            dma((2,)),
            dma((nb, 2)),
            dma((nb,)),
            dma((1,)),
            dma((2,)),
            dma((2,)),
            dma((nb, 2)),
            dma((1,)),
            dma((tp,)),
            dma((1,)),
            dma((1,)),
            dma((1,)),
            dma((heads + 1,)),
            dma((1,)),
            dma((2 * js, 2)),
            dma((1,)),
            dma((js,)),
            dma((1,)),
            dma((1,)),
        ],
        compiler_params=pltpu.CompilerParams(
            collective_id=1, has_side_effects=True, vmem_limit_bytes=36 * 1024 * 1024
        ),
    )(
        *(
            pltpu.with_memory_space_constraint(v, pltpu.HBM)
            for v in (
                block_order,
                hidden[0],
                target[0],
                gain[None, :],
                freqs,
                w_query,
                w_key,
                value_matrix,
                w_out,
            )
        )
    )
    return (branch[None], jnp.sum(loss))


def solution(mesh):
    in_specs = (
        P("dp", "ctx", "tp"),
        P("dp", "ctx", "tp"),
        P(),
        P(("ctx", "dp"), "tp"),
        P(("ctx", "dp"), "tp"),
        P(("ctx", "dp"), "tp"),
        P("tp", ("ctx", "dp")),
        P(),
    )
    out_specs = (P("dp", "ctx", "tp"), P())
    sizes = mesh.shape
    fits = sizes["ctx"] == 2 and sizes["tp"] == 4 and sizes["dp"] % 2 == 0
    body = functools.partial(fused, sizes["dp"]) if fits else on_device
    return jax.shard_map(
        body, mesh=mesh, in_specs=in_specs, out_specs=out_specs, check_vma=False
    )
```

```python
import functools

import jax
import numpy as np
import jax.numpy as jnp
from jax import lax
from jax.experimental import pallas as pl
from jax.experimental.pallas import tpu as pltpu
from jax.sharding import PartitionSpec as P

MODEL_WIDTH = 4096
QUERY_HEADS = 16
KEY_VALUE_HEADS = 4
HEAD_SIZE = 128


rope_base = 500000.0


def shifted(value, axis, by):
    peers = lax.axis_size(axis)
    return lax.ppermute(value, axis, [(i, (i + by) % peers) for i in range(peers)])


def positions(order, start, rows, half):
    index = start + lax.iota(jnp.int32, rows)
    block = index // half
    slots = lax.iota(jnp.int32, order.shape[0])
    chosen = jnp.sum(jnp.where(block[:, None] == slots[None, :], order[None, :], 0), axis=1)
    return chosen * half + index % half


def apply_rotary(values, token_places):
    half = values.shape[-1] // 2
    freqs = rope_base ** (-(jnp.arange(half, dtype=jnp.float32) * 2.0) / values.shape[-1])
    angles = token_places.astype(jnp.float32)[:, None] * freqs[None, :]
    cosine = jnp.cos(angles)[:, None, :]
    sine = jnp.sin(angles)[:, None, :]
    first = values[..., :half]
    second = values[..., half:]
    return jnp.concatenate(
        [first * cosine - second * sine, second * cosine + first * sine], axis=-1
    )


def attend(state, query_rows, qpos, piece, kpos):
    peak, total, accum = state
    rows = piece.shape[1]
    local_heads = query_rows.shape[1]
    pair = piece.reshape(2, rows, local_heads, HEAD_SIZE)
    scores = jnp.einsum(
        "qcgd,kcd->cgqk", query_rows, pair[0], preferred_element_type=jnp.float32
    ) * (1.0 / HEAD_SIZE**0.5)
    allowed = (qpos[:, None] >= kpos[None, :])[None, None]
    scores = jnp.where(allowed, scores, -1e30)
    new_peak = jnp.maximum(peak, jnp.max(scores, axis=-1))
    weights = jnp.where(allowed, jnp.exp(scores - new_peak[..., None]), 0.0)
    factor = jnp.exp(peak - new_peak)
    total = total * factor + jnp.sum(weights, axis=-1)
    update = jnp.einsum(
        "cgqk,kcd->qcgd", weights.astype(jnp.bfloat16), pair[1], preferred_element_type=jnp.float32
    )
    accum = accum * jnp.transpose(factor, (2, 0, 1))[..., None] + update
    return (new_peak, total, accum)


def on_device(hidden, target, gain, w_query, w_key, value_matrix, w_out, block_order):
    rows = hidden.shape[1]
    half = rows // 2
    local = hidden[0]
    whole = lax.all_gather(local, "tp", axis=1, tiled=True)
    wide = whole.astype(jnp.float32)
    normed = (
        wide * lax.rsqrt(jnp.mean(wide * wide, axis=1, keepdims=True) + 1e-05) * gain[None, :]
    ).astype(jnp.bfloat16)
    pieces = (
        lax.all_gather(w_query, ("ctx", "dp"), axis=0, tiled=True),
        lax.all_gather(w_key, ("ctx", "dp"), axis=0, tiled=True),
        lax.all_gather(value_matrix, ("ctx", "dp"), axis=0, tiled=True),
    )
    query_rows, key, value_rows = tuple(
        (jnp.dot(normed, piece, preferred_element_type=jnp.float32) for piece in pieces)
    )
    shard = lax.axis_index("ctx")
    qpos = positions(block_order, shard * rows, rows, half)
    local_heads = w_key.shape[1] // HEAD_SIZE
    query_group = QUERY_HEADS // KEY_VALUE_HEADS
    query_rows = (
        apply_rotary(query_rows.reshape(rows, local_heads * query_group, HEAD_SIZE), qpos)
        .astype(jnp.bfloat16)
        .reshape(rows, local_heads, query_group, HEAD_SIZE)
    )
    key = (
        apply_rotary(key.reshape(rows, local_heads, HEAD_SIZE), qpos)
        .astype(jnp.bfloat16)
        .reshape(rows, local_heads * HEAD_SIZE)
    )
    pair = jnp.stack([key, value_rows.astype(jnp.bfloat16)])
    state = (
        jnp.full((local_heads, query_group, rows), -1e30, jnp.float32),
        jnp.zeros((local_heads, query_group, rows), jnp.float32),
        jnp.zeros((rows, local_heads, query_group, HEAD_SIZE), jnp.float32),
    )
    count = lax.axis_size("ctx")
    state = attend(state, query_rows, qpos, pair, qpos)

    def turn(step, carry):
        moved, inner = carry
        moved = shifted(moved, "ctx", 1)
        source = (shard - step) % count
        return (
            moved,
            attend(
                inner, query_rows, qpos, moved, positions(block_order, source * rows, rows, half)
            ),
        )

    moved_end, state = lax.fori_loop(1, count, turn, (pair, state))
    peak, total, accum = state
    attn = (
        (accum / jnp.transpose(total, (2, 0, 1))[..., None])
        .astype(jnp.bfloat16)
        .reshape(rows, local_heads * query_group * HEAD_SIZE)
    )
    terms = jnp.dot(
        attn,
        lax.all_gather(w_out, ("ctx", "dp"), axis=1, tiled=True),
        preferred_element_type=jnp.float32,
    )
    summed = lax.psum_scatter(terms.astype(jnp.bfloat16), "tp", scatter_dimension=1, tiled=True)
    resid = local.astype(jnp.float32) + summed.astype(jnp.float32) - target[0].astype(jnp.float32)
    squares = lax.psum(jnp.sum(resid * resid), ("ctx", "tp", "dp"))
    loss = squares / (lax.axis_size("dp") * lax.axis_size("ctx") * rows * MODEL_WIDTH)
    return (summed[None], loss)


MESH = pl.DeviceIdType.MESH
F32 = jnp.float32
BF16 = jnp.bfloat16


def layer(
    nd,
    order_in,
    hidden,
    target,
    gain,
    freqs,
    w_query,
    w_key,
    value_matrix,
    w_out,
    out,
    loss,
    ga,
    stage,
    go,
    ostage,
    mine,
    xs,
    goal,
    normed,
    acc,
    trig,
    query,
    kv,
    attn,
    made,
    arrived,
    want,
    tile,
    sums,
    gains,
    turns,
    order,
    load_sem,
    x_send,
    a_send,
    a_recv,
    sib_recv,
    oy_send,
    oy_recv,
    o_send,
    o_recv,
    h_send,
    h_recv,
    kv_send,
    kv_recv,
    at_send,
    at_recv,
    r_send,
    r_recv,
    w_send,
    w_recv,
    l_send,
    l_recv,
):
    c, t, d = lax.axis_index("ctx"), lax.axis_index("tp"), lax.axis_index("dp")
    y, k = t // 2, t % 2
    sibling = y * 2 + (1 - k)
    across = (1 - y) * 2 + k
    rows, wide = hidden.shape
    deep, qcols = w_query.shape
    half = rows // 2
    n_heads = qcols // HEAD_SIZE
    tp = 4
    plane = 2 * tp
    owner = c == k
    up, down = d < nd - 1, d > 0

    def load(i, src, dst):
        return pltpu.make_async_copy(src, dst, load_sem.at[i])

    quarter = deep // 4

    def rows_of(piece):
        return pl.ds(pl.multiple_of(piece * quarter, quarter), quarter)

    def weight_loads(dst):
        return (
            load(0, w_query, dst.at[:, pl.ds(0, qcols)]),
            load(1, w_key, dst.at[:, pl.ds(qcols, HEAD_SIZE)]),
            load(2, value_matrix, dst.at[:, pl.ds(qcols + HEAD_SIZE, HEAD_SIZE)]),
        )

    hc = w_out.shape[1] // 2
    hq = hc // 2
    own_loads = weight_loads(ga.at[c * nd + d])
    stage_loads = weight_loads(stage)
    mine_load = load(3, hidden, mine)

    def columns_of(half_of, part):
        return pl.ds(pl.multiple_of(half_of * hc + part * hq, hq), hq)

    keep_loads = [
        load(4 + e, w_out.at[:, columns_of(y, e)], go.at[d * 2 + k, e, y]) for e in range(2)
    ]
    give_loads = [
        load(6 + e, w_out.at[:, columns_of(1 - y, e)], ostage.at[e]) for e in range(2)
    ]
    local_load = load(8, hidden, xs.at[t])
    goal_load = load(9, target, goal)
    gain_load = load(10, gain, gains)
    turn_load = load(11, freqs, turns)
    order_load = load(12, order_in, order)

    @pl.when(owner)
    def _():
        for copy in own_loads:
            copy.start()

    @pl.when(jnp.logical_not(owner))
    def _():
        for copy in stage_loads:
            copy.start()

    mine_load.start()
    order_load.start()
    turn_load.start()
    for copy in give_loads + keep_loads:
        copy.start()

    @pl.when(owner)
    def _():
        local_load.start()

    goal_load.start()
    gain_load.start()

    barrier = pltpu.get_barrier_semaphore()
    seat = c * tp + t
    beside = [{"tp": sibling}]
    for other in range(2):
        beside += [{"ctx": 1 - c, "tp": y * 2 + other}, {"tp": (1 - y) * 2 + other}]
    for where in beside:
        pl.semaphore_signal(barrier, inc=1, device_id=where, device_id_type=MESH)
    for there, step in ((up, 1), (down, -1)):

        @pl.when(there)
        def _():
            pl.semaphore_signal(barrier, inc=1, device_id={"dp": d + step}, device_id_type=MESH)

    near_count = len(beside) + up.astype(jnp.int32) + down.astype(jnp.int32)
    pl.semaphore_wait(barrier, near_count)

    def remote(src, dst, ssem, rsem, where):
        return pltpu.make_async_remote_copy(
            src_ref=src, dst_ref=dst, send_sem=ssem, recv_sem=rsem,
            device_id=where, device_id_type=MESH,
        )

    UP, DOWN, SIB = 0, 1, 2

    def target_of(way):
        return {
            UP: {"dp": jnp.minimum(d + 1, nd - 1)},
            DOWN: {"dp": jnp.maximum(d - 1, 0)},
            SIB: {"tp": sibling},
        }[way]

    def a_copy(line, i, way, e, core=k):
        b = line * nd + i
        ref = ga.at[b, rows_of(2 * core + e)]
        there = sib_recv.at[b] if way == SIB else a_recv.at[b, e]
        return remote(ref, ref, a_send.at[int(way == SIB)], there, target_of(way))

    def o_copy(i, way, e, core=k):
        ref = go.at[i * 2 + core, e]
        there = o_recv.at[core * nd + i, e]
        return remote(ref, ref, o_send.at[int(way == SIB)], there, target_of(way))

    def spread(copy, i, ways, e):
        copy_up = lambda: copy(i, UP, e).start()
        copy_down = lambda: copy(i, DOWN, e).start()
        if UP in ways:
            pl.when(up)(copy_up)
        if DOWN in ways:
            pl.when(down)(copy_down)
        if SIB in ways:
            copy(i, SIB, e).start()

    def relay(copy, s, parts=(0, 1)):
        for e in parts:

            @pl.when(d >= s)
            def _():
                copy(d - s, UP, e).wait_recv()
                spread(copy, d - s, (UP, SIB), e)

            @pl.when(d + s < nd)
            def _():
                copy(d + s, DOWN, e).wait_recv()
                spread(copy, d + s, (DOWN, SIB), e)

    near_copy = functools.partial(a_copy, c)
    far_copy = functools.partial(a_copy, 1 - c)
    b_own = c * nd + d
    half_copies = []
    x_copies = []
    for e in range(2):
        ref = ga.at[b_own, rows_of(2 * (1 - k) + e)]
        half_copies.append(
            remote(
                ref, ref, x_send.at[0], a_recv.at[b_own, e], {"tp": sibling}
            )
        )
        for h in range(2):
            piece = 2 * h + e
            x_copies.append(
                remote(
                    stage.at[rows_of(piece)],
                    ga.at[b_own, rows_of(piece)],
                    x_send.at[0],
                    a_recv.at[b_own, e],
                    {"ctx": 1 - c, "tp": y * 2 + h},
                )
            )

    @pl.when(owner)
    def _():
        for copy in own_loads:
            copy.wait()
        for e in range(2):
            half_copies[e].start()
            spread(near_copy, d, (UP, DOWN), e)

    @pl.when(jnp.logical_not(owner))
    def _():
        for copy in stage_loads:
            copy.wait()
        for copy in x_copies:
            copy.start()

    mine_load.wait()
    h_y = remote(mine, xs.at[t], h_send.at[0], h_recv.at[t], {"tp": (1 - y) * 2 + c})
    h_x = remote(mine, xs.at[t], h_send.at[0], h_recv.at[t], {"ctx": 1 - c, "tp": y * 2 + c})
    h_sib = remote(mine, xs.at[t], h_send.at[0], h_recv.at[t], {"tp": sibling})
    h_y.start()

    @pl.when(jnp.logical_not(owner) & (k == 0))
    def _():
        h_x.start()

    @pl.when(jnp.logical_not(owner))
    def _():
        for e in range(2):
            near_copy(d, UP, e).wait_recv()
            spread(near_copy, d, (UP, DOWN), e)

    oy_copies = []
    for e in range(2):
        give_loads[e].wait()
        oy_copies.append(
            remote(
                ostage.at[e], go.at[d * 2 + k, e, y], oy_send.at[0], oy_recv.at[e], {"tp": across}
            )
        )
        oy_copies[e].start()

    def positions_of(shard, index):
        low = order[2 * shard] * half
        high = order[2 * shard + 1] * half
        return jnp.where(index < half, low + index, high + index - half)

    order_load.wait()
    turn_load.wait()
    place = positions_of(k, lax.broadcasted_iota(jnp.int32, (rows, HEAD_SIZE), 0)).astype(F32)
    angle = place * turns[...]
    lane_of = lax.broadcasted_iota(jnp.int32, (rows, HEAD_SIZE), 1)
    trig[0] = jnp.cos(angle)
    sine = jnp.sin(angle)
    trig[1] = jnp.where(lane_of < HEAD_SIZE // 2, -sine, sine)

    for s in range(1, min(2, nd - 1)):
        relay(near_copy, s)

    @pl.when(owner & (k == 0))
    def _():
        h_x.start()

    @pl.when(owner)
    def _():
        for e in range(2):
            spread(near_copy, d, (SIB,), e)

    @pl.when(jnp.logical_not(owner))
    def _():
        h_sib.start()

    for e in range(2):
        far_copy(d, UP, e).wait_recv()
        spread(far_copy, d, (UP, DOWN, SIB), e)

    for s in range(2, nd - 1):
        relay(near_copy, s)

    @pl.when(k == 1)
    def _():
        h_x.start()

    def h_wait(slot):
        remote(mine, xs.at[slot], h_send.at[0], h_recv.at[slot], {"tp": across}).wait_recv()

    far = (1 - y) * 2
    h_relay_x = remote(
        xs.at[far + 1], xs.at[far + 1], h_send.at[0], h_recv.at[far + 1], {"ctx": 1 - c}
    )
    h_relay_y = remote(
        xs.at[y * 2], xs.at[y * 2], h_send.at[0], h_recv.at[y * 2], {"tp": across}
    )

    @pl.when(owner)
    def _():
        h_wait(far + 1)
        h_relay_x.start()

    @pl.when(jnp.logical_not(owner))
    def _():
        h_wait(y * 2)
        h_relay_y.start()

    for s in range(1, min(2, nd - 1)):
        relay(far_copy, s)

    for s in range(2, nd - 1):
        relay(far_copy, s)

    for e in range(2):
        keep_loads[e].wait()
        remote(
            ostage.at[e], go.at[d * 2 + k, e, 1 - y], oy_send.at[0], oy_recv.at[e], {"tp": across}
        ).wait_recv()
        spread(o_copy, d, (UP, DOWN, SIB), e)

    @pl.when(owner)
    def _():
        local_load.wait()
        h_wait(sibling)
        h_wait(far)

    @pl.when(jnp.logical_not(owner))
    def _():
        h_wait(y * 2 + 1)
        h_wait(far)
        h_wait(far + 1)

    js = nd // 2
    keeps = (k == c) & (y == c)

    def slot_columns(slot):
        return pl.ds(pl.multiple_of(slot * hc, hc), hc)

    def nearest(i):
        return jnp.where(d < nd // 2, i, nd - 1 - i)

    last = nearest(nd - 1)
    ships = k == last // js

    def want_copy(j, side):
        return remote(
            goal.at[:, slot_columns(j * 2 + side)],
            want.at[j],
            w_send.at[0],
            w_recv.at[j],
            {"ctx": y, "tp": side * 2 + c},
        )

    def keep_want(j):
        return pltpu.make_async_copy(
            target.at[:, slot_columns(j * 2 + y)], want.at[j], w_recv.at[j]
        )

    gain_load.wait()
    chunk = min(64, rows)
    per = wide // deep

    def norm_rows(i, carry):
        r = pl.multiple_of(i * chunk, chunk)
        total = jnp.zeros((chunk, 1), F32)
        for j in range(tp):
            v = xs[j, pl.ds(r, chunk), :].astype(F32)
            total = total + jnp.sum(v * v, axis=1, keepdims=True)
        scale = lax.rsqrt(total * (1.0 / (tp * wide)) + 1e-05)
        for j in range(tp):
            for m in range(per):
                v = xs[j, pl.ds(r, chunk), m * deep : (m + 1) * deep].astype(F32)
                g = gains[:, j * wide + m * deep : j * wide + (m + 1) * deep]
                normed[j * per + m, pl.ds(r, chunk), :] = (v * scale * g).astype(BF16)
        return carry

    lax.fori_loop(0, rows // chunk, norm_rows, 0)
    goal_load.wait()

    @pl.when(keeps & ships)
    def _():
        for j in range(js):
            keep_want(j).start()

    for side in range(2):

        @pl.when(ships & jnp.logical_not(keeps & (side == y)))
        def _():
            for j in range(js):
                want_copy(j, side).start()

    acc[...] = jnp.zeros_like(acc)

    def project(i, line):
        b = line * nd + i

        @pl.when(jnp.logical_not(owner & (b == b_own)))
        def _():
            ref = ga.at[b, pl.ds(0, deep // 2)]
            remote(ref, ref, a_send.at[1], sib_recv.at[b], {"tp": sibling}).wait_recv()

        acc[...] += jnp.dot(normed[b], ga[b], preferred_element_type=F32)

    def project_step(i, carry):
        @pl.when(i == nd - 1)
        def _():
            relay(near_copy, nd - 1)

        project(nearest(i), c)

        @pl.when(i == nd - 1)
        def _():
            relay(far_copy, nd - 1)

        project(nearest(i), 1 - c)
        return carry

    lax.fori_loop(0, nd, project_step, 0)

    def rotated(v):
        return (v * trig[0] + pltpu.roll(v, HEAD_SIZE // 2, 1) * trig[1]).astype(BF16)

    kv[k, :, 0:HEAD_SIZE] = rotated(acc[:, qcols : qcols + HEAD_SIZE])
    kv[k, :, HEAD_SIZE:] = acc[:, qcols + HEAD_SIZE :].astype(BF16)
    kv_copy = remote(kv.at[k], kv.at[k], kv_send.at[0], kv_recv.at[0], {"tp": sibling})
    kv_copy.start()
    for h in range(n_heads):
        part = slice(h * HEAD_SIZE, (h + 1) * HEAD_SIZE)
        query[h] = rotated(acc[:, part])
    remote(kv.at[1 - k], kv.at[1 - k], kv_send.at[0], kv_recv.at[0], {"tp": sibling}).wait_recv()
    qrows = min(256, rows)
    dims = (((1,), (1,)), ((), ()))
    group = y * 2 + c
    spots = ({"ctx": 1 - c}, {"tp": across})
    x_group, y_group = y * 2 + 1 - c, (1 - y) * 2 + c

    early = n_heads // 2

    def at_copy(h, way, source=group):
        ref = attn.at[source * n_heads + h]
        first = h < early if way == 0 else h >= early
        there = jnp.where(first & (source == group), h, n_heads)
        return remote(ref, ref, at_send.at[0], at_recv.at[there], spots[way])

    def at_arrival(h, source):
        ref = attn.at[source * n_heads + h]
        return remote(ref, ref, at_send.at[0], at_recv.at[h], spots[0])

    def attend_head(h, carry):
        def attend_block(i, inner):
            r = pl.multiple_of(i * qrows, qrows)
            q = query[h, pl.ds(r, qrows), :]
            qpos = positions_of(k, r + lax.broadcasted_iota(jnp.int32, (qrows, rows), 0))
            scores = []
            for n in range(2):
                kpos = positions_of(n, lax.broadcasted_iota(jnp.int32, (qrows, rows), 1))
                sc = lax.dot_general(
                    q, kv[n, :, 0:HEAD_SIZE], dims, preferred_element_type=F32
                ) * (1.0 / HEAD_SIZE**0.5)
                scores.append(jnp.where(qpos >= kpos, sc, -1e30))
            peak = jnp.maximum(
                jnp.max(scores[0], axis=1, keepdims=True),
                jnp.max(scores[1], axis=1, keepdims=True),
            )
            total = jnp.zeros((qrows, 1), F32)
            value = jnp.zeros((qrows, HEAD_SIZE), F32)
            for n in range(2):
                p = jnp.exp(scores[n] - peak)
                total = total + jnp.sum(p, axis=1, keepdims=True)
                value = value + jnp.dot(
                    p.astype(BF16), kv[n, :, HEAD_SIZE:], preferred_element_type=F32
                )
            attn[group * n_heads + h, pl.ds(r, qrows), :] = (value / total).astype(BF16)
            return inner

        lax.fori_loop(0, rows // qrows, attend_block, 0)
        for way in range(2):
            at_copy(h, way).start()
        return carry

    lax.fori_loop(0, n_heads, attend_head, 0)

    for s in range(1, min(2, nd - 1)):
        relay(o_copy, s)

    def at_relay(h, carry):
        at_arrival(h, x_group).wait_recv()
        at_copy(h, 1, x_group).start()
        at_arrival(early + h, y_group).wait_recv()
        at_copy(early + h, 0, y_group).start()
        return carry

    lax.fori_loop(0, early, at_relay, 0)

    for s in range(2, nd - 1):
        relay(o_copy, s)

    rest = attn.at[pl.ds(0, 2 * n_heads)]
    remote(rest, rest, at_send.at[0], at_recv.at[n_heads], spots[0]).wait_recv()

    orow = min(256, rows)

    def made_copy(i, e, rr):
        slot = (i % js) * 2 + y
        where = {"ctx": k, "tp": c * 2 + i // js}
        return remote(
            made.at[i, e, rr], arrived.at[slot, e, rr], r_send.at[0], r_recv.at[slot, e], where
        )

    def stays(i):
        return keeps & (i // js == k)

    def gathered(g, rr):
        return jnp.concatenate([attn[g * n_heads + h, rr, :] for h in range(n_heads)], axis=1)

    tile[...] = jnp.zeros_like(tile)

    def keep_or_send(i, e, rr, value, final):
        if final:
            spot = pl.ds(pl.multiple_of(((i % js) * 2 + y) * hc + e * hq, hq), hq)
            part = pl.ds(pl.multiple_of(e * hq, hq), hq)
            resid = xs[c * 2 + i // js, rr, spot].astype(F32) + value.astype(F32)
            resid = resid - want[i % js, rr, part].astype(F32)
            tile[...] += jnp.sum((resid * resid).reshape(orow // 8, 8, hq), axis=0)

        @pl.when(jnp.logical_not(stays(i)))
        def _():
            made[i, e, rr, :] = value
            made_copy(i, e, rr).start()

        @pl.when(stays(i))
        def _():
            arrived[(i % js) * 2 + y, e, rr, :] = value

    def rows_at(m):
        return pl.ds(pl.multiple_of(m * orow, orow), orow)

    def want_wait(i):
        @pl.when(keeps & ships)
        def _():
            keep_want(i % js).wait()

        @pl.when(jnp.logical_not(keeps & ships))
        def _():
            ref = want.at[i % js]
            remote(ref, ref, w_send.at[0], w_recv.at[i % js], {"tp": sibling}).wait_recv()

    others_end = jnp.where(ships, 0, 4 * js)

    def whole_block(final, n, carry):
        i = nearest(n)
        if final:
            want_wait(i)
        for e in range(2):
            o_copy(i, SIB, e, 1 - k).wait_recv()

        def all_rows(m, inner):
            rr = rows_at(m)
            total = jnp.zeros((orow, hc), F32)
            for g in range(tp):
                b = i * 2 + g % 2
                weights = jnp.concatenate([go[b, e, g // 2] for e in range(2)], axis=1)
                term = jnp.dot(gathered(g, rr), weights, preferred_element_type=F32)
                total = total + term.astype(BF16).astype(F32)
            for e in range(2):
                keep_or_send(i, e, rr, total[:, e * hq : (e + 1) * hq].astype(BF16), final)
            return inner

        lax.fori_loop(0, rows // orow, all_rows, 0)
        return carry

    lax.fori_loop(0, js, functools.partial(whole_block, False), 0)
    lax.fori_loop(js, nd - 1, functools.partial(whole_block, True), 0)

    def finish_block(squares, n, carry):
        j = jnp.where(d < nd // 2, n // 4, js - 1 - n // 4)
        e, side = n // 2 % 2, n % 2
        slot = j * 2 + side

        @pl.when(jnp.logical_not(keeps & (side == y)))
        def _():
            remote(
                made.at[0, 0], arrived.at[slot, e], r_send.at[0], r_recv.at[slot, e],
                {"tp": sibling},
            ).wait_recv()

        place = pl.ds(pl.multiple_of(slot * hc + e * hq, hq), hq)
        if not squares:
            out[:, place] = arrived[slot, e]
            return carry

        def finish(m, inner):
            rr = rows_at(m)
            result = arrived[slot, e, rr, :]
            out[rr, place] = result
            resid = mine[rr, place].astype(F32) + result.astype(F32)
            resid = resid - goal[rr, place].astype(F32)
            tile[...] += jnp.sum((resid * resid).reshape(orow // 8, 8, hq), axis=0)
            return inner

        lax.fori_loop(0, rows // orow, finish, 0)
        return carry

    def half_block(e, carry):
        i = nearest(nd - 1)
        relay(o_copy, nd - 1, (e,))

        def terms(core, rr):
            total = jnp.zeros((orow, hq), F32)
            for side in range(2):
                weights = go[i * 2 + core, e, side]
                term = jnp.dot(
                    gathered(2 * side + core, rr), weights, preferred_element_type=F32
                )
                total = total + term.astype(BF16).astype(F32)
            return total

        def own_rows(m, inner):
            acc[rows_at(m), 0:hq] = terms(k, rows_at(m))
            return inner

        lax.fori_loop(0, rows // orow, own_rows, 0)
        o_copy(i, SIB, e, 1 - k).wait_recv()

        def all_rows(m, inner):
            rr = rows_at(m)
            value = (acc[rr, 0:hq] + terms(1 - k, rr)).astype(BF16)
            keep_or_send(i, e, rr, value, True)
            return inner

        lax.fori_loop(0, rows // orow, all_rows, 0)
        return carry


    want_wait(last)

    def last_step(e, carry):
        half_block(e, carry)

        @pl.when(e == 0)
        def _():
            lax.fori_loop(0, others_end, functools.partial(finish_block, True), 0)

        return carry

    lax.fori_loop(0, 2, last_step, 0)
    everyone = plane * nd
    number = d * plane + seat

    def l_copy(n):
        r = everyone - 1 - n
        p = (seat + r) % plane
        z = jnp.where(d < nd // 2, (d + r // plane) % nd, (d + nd - r // plane) % nd)
        return remote(
            sums.at[number], sums.at[number], l_send.at[0], l_recv.at[0],
            {"ctx": p // tp, "tp": p % tp, "dp": z},
        )

    others = sums.at[pl.ds(0, everyone - 1)]
    l_all = remote(others, others, l_send.at[0], l_recv.at[0], {"tp": sibling})
    sums[number] = jnp.sum(tile[...], axis=0, keepdims=True)

    for n in range(everyone - 1):
        l_copy(n).start()
    lax.fori_loop(others_end, 4 * js, functools.partial(finish_block, False), 0)

    def sent(ref, sem):
        remote(ref, ref, sem, kv_recv.at[0], {"tp": sibling}).wait_send()

    for line_at in range(nd):
        blocks = (line_at + 1) * (line_at < nd - 1) + (nd - line_at) * (line_at > 0)

        @pl.when(d == line_at)
        def _():
            sent(ga.at[pl.ds(0, blocks)], a_send.at[0])
            sent(go.at[pl.ds(0, blocks)], o_send.at[0])

    sent(go.at[pl.ds(0, nd)], o_send.at[1])

    @pl.when(owner)
    def _():
        sent(ga.at[0, pl.ds(0, deep // 2)], x_send.at[0])
        sent(ga.at[pl.ds(0, nd)], a_send.at[1])
        sent(xs.at[pl.ds(0, 3)], h_send.at[0])

    @pl.when(jnp.logical_not(owner))
    def _():
        sent(ga.at[0], x_send.at[0])
        sent(ga.at[pl.ds(0, 2 * nd - 1), pl.ds(0, deep // 2)], a_send.at[1])
        sent(xs, h_send.at[0])

    sent(ostage, oy_send.at[0])
    kv_copy.wait_send()
    sent(attn.at[pl.ds(0, 3 * n_heads)], at_send.at[0])

    @pl.when(keeps)
    def _():
        sent(made.at[pl.ds(0, nd - js)], r_send.at[0])

    @pl.when(jnp.logical_not(keeps))
    def _():
        sent(made, r_send.at[0])

    @pl.when(ships & keeps)
    def _():
        sent(arrived.at[pl.ds(0, js)], w_send.at[0])

    @pl.when(ships & jnp.logical_not(keeps))
    def _():
        sent(arrived, w_send.at[0])

    l_all.wait_send()

    l_all.wait_recv()
    whole = sums[0]
    for b in range(1, everyone):
        whole = whole + sums[b]
    count = plane * nd * rows * wide
    loss[...] = whole / count


def fused(nd, hidden, target, gain, w_query, w_key, value_matrix, w_out, block_order):
    rows, wide = hidden.shape[1:]
    nb = 2 * nd
    tp = 4
    plane = 2 * tp
    deep, qcols = w_query.shape
    all_cols = qcols + w_key.shape[1] + value_matrix.shape[1]
    orows, ocols = w_out.shape
    hc = ocols // 2
    order_shape = block_order.shape
    half = HEAD_SIZE // 2
    freqs = np.float64(rope_base) ** (-np.arange(half) * 2.0 / HEAD_SIZE)
    freqs = jnp.asarray(np.concatenate([freqs, freqs])[None, :].astype(np.float32))
    heads = qcols // HEAD_SIZE
    js = nd // 2
    anyspace = pl.BlockSpec(memory_space=pltpu.HBM)
    vmem = pl.BlockSpec(memory_space=pltpu.VMEM)
    dma = pltpu.SemaphoreType.DMA
    branch, loss = pl.pallas_call(
        functools.partial(layer, nd),
        out_shape=(
            jax.ShapeDtypeStruct((rows, wide), BF16),
            jax.ShapeDtypeStruct((1, hc // 2), F32),
        ),
        in_specs=[
            anyspace,
            anyspace,
            anyspace,
            anyspace,
            anyspace,
            anyspace,
            anyspace,
            anyspace,
            anyspace,
        ],
        out_specs=(vmem, vmem),
        scratch_shapes=[
            pltpu.VMEM((nb, deep, all_cols), BF16),
            pltpu.VMEM((deep, all_cols), BF16),
            pltpu.VMEM((2 * nd, 2, 2, orows, hc // 2), BF16),
            pltpu.VMEM((2, orows, hc // 2), BF16),
            pltpu.VMEM((rows, wide), BF16),
            pltpu.VMEM((tp, rows, wide), BF16),
            pltpu.VMEM((rows, wide), BF16),
            pltpu.VMEM((nb, rows, deep), BF16),
            pltpu.VMEM((rows, all_cols), F32),
            pltpu.VMEM((2, rows, HEAD_SIZE), F32),
            pltpu.VMEM((heads, rows, HEAD_SIZE), BF16),
            pltpu.VMEM((2, rows, 2 * HEAD_SIZE), BF16),
            pltpu.VMEM((tp * heads, rows, HEAD_SIZE), BF16),
            pltpu.VMEM((nd, 2, rows, hc // 2), BF16),
            pltpu.VMEM((2 * js, 2, rows, hc // 2), BF16),
            pltpu.VMEM((js, rows, hc), BF16),
            pltpu.VMEM((8, hc // 2), F32),
            pltpu.VMEM((plane * nd, 1, hc // 2), F32),
            pltpu.VMEM((1, tp * wide), F32),
            pltpu.VMEM((1, HEAD_SIZE), F32),
            pltpu.SMEM(order_shape, jnp.int32),
            dma((13,)),
            dma((1,)),
            dma((2,)),
            dma((nb, 2)),
            dma((nb,)),
            dma((1,)),
            dma((2,)),
            dma((2,)),
            dma((nb, 2)),
            dma((1,)),
            dma((tp,)),
            dma((1,)),
            dma((1,)),
            dma((1,)),
            dma((heads + 1,)),
            dma((1,)),
            dma((2 * js, 2)),
            dma((1,)),
            dma((js,)),
            dma((1,)),
            dma((1,)),
        ],
        compiler_params=pltpu.CompilerParams(
            collective_id=1, has_side_effects=True, vmem_limit_bytes=36 * 1024 * 1024
        ),
    )(
        *(
            pltpu.with_memory_space_constraint(v, pltpu.HBM)
            for v in (
                block_order,
                hidden[0],
                target[0],
                gain[None, :],
                freqs,
                w_query,
                w_key,
                value_matrix,
                w_out,
            )
        )
    )
    return (branch[None], jnp.sum(loss))


def solution(mesh):
    in_specs = (
        P("dp", "ctx", "tp"),
        P("dp", "ctx", "tp"),
        P(),
        P(("ctx", "dp"), "tp"),
        P(("ctx", "dp"), "tp"),
        P(("ctx", "dp"), "tp"),
        P("tp", ("ctx", "dp")),
        P(),
    )
    out_specs = (P("dp", "ctx", "tp"), P())
    sizes = mesh.shape
    fits = sizes["ctx"] == 2 and sizes["tp"] == 4 and sizes["dp"] % 2 == 0
    body = functools.partial(fused, sizes["dp"]) if fits else on_device
    return jax.shard_map(
        body, mesh=mesh, in_specs=in_specs, out_specs=out_specs, check_vma=False
    )
```
